1024 devices in a mesh: dp: 8 (over x), mp: 128 (over z, y, core).
Axes of the slice: x: 8, y: 8, z: 8, core: 2. Of those that a mesh axis runs over, the one named last changes fastest.
Arguments:
- rewards: int32 [64], P('dp'), may hold values from 0 to 4096, as said below
- group_ids: int32 [64], P('dp'), may hold values from 0 to 3, as said below
- lengths: int32 [64], P('dp'), may hold values from 1 to 64
- token_mask: int32 [4096], P('dp'), may hold values from 0 to 1, as said below
- targets: int32 [4096], P('dp'), may hold values from 0 to 65535
- logits: bfloat16 [4096, 65536], P('dp', 'mp'), may hold values from -140 to 400
Outputs:
- advantage: float32 [64], P('dp')
- token_weight: float32 [4096], P('dp')
- token_logprob: float32 [4096], P('dp')
- token_entropy: float32 [4096], P('dp')
- objective: float32 [], replicated
The draws below stay inside these ranges and needn't reach their ends.
Inputs may be any that keep to these rules, and one draw needn't show every extreme that they name: rewards in units of 1/1024. `group_ids`: each of the 4 prompts has exactly 16 trajectories. `token_mask`: zeros come in aligned spans of 8 positions, except that the first position of each window is always 1.
All inputs are finite; a program needn't handle non-finite values.
Results may differ from the reference program's by a relative error of at most 0.00095.
Values may be sent and summed in bfloat16 or wider, within the bound.
No kernel may reach another device: no remote copies, remote signals or barrier semaphores. Data moves between devices by JAX's collectives and lax.ppermute only.
A program may use at most 32 MiB of HBM per device.

```python
import math
import jax
import jax.numpy as jnp
from jax import lax

VOCAB = 65536
GROUP = 16
WIN = 64
ROLLOUTS = 64
GROUPS = 4
TOKENS = 4096


def group_plan(key):
    shuffled = jax.random.permutation(jax.random.fold_in(key, 11), ROLLOUTS)
    return (shuffled // GROUP).astype(jnp.int32)


def draw_group_ids(key, part):
    return group_plan(key)


def draw_rewards(key, part):
    groups_of = group_plan(key)
    own_values = jax.random.randint(jax.random.fold_in(key, 12), (ROLLOUTS,), 0, 4097)
    shared_value = jax.random.randint(jax.random.fold_in(key, 13), (GROUPS,), 0, 4097)
    flat_group = jax.random.randint(jax.random.fold_in(key, 14), (GROUPS,), 0, 2)
    flat_group = flat_group * (jnp.arange(GROUPS, dtype=jnp.int32) > 0)
    return jnp.where(flat_group[groups_of] > 0, shared_value[groups_of], own_values).astype(jnp.int32)


def draw_lengths(key, part):
    rollout_index = jnp.arange(ROLLOUTS, dtype=jnp.int32)
    upper_bound = WIN // 3 + (WIN - WIN // 3) * rollout_index // max(ROLLOUTS - 1, 1)
    drawn_lengths = jax.random.randint(jax.random.fold_in(key, 21), (ROLLOUTS,), 1, upper_bound + 1)
    return jnp.where(rollout_index == ROLLOUTS - 1, WIN, drawn_lengths).astype(jnp.int32)


def draw_token_mask(key, part):
    span_bits = jax.random.randint(jax.random.fold_in(key, 31), (TOKENS // 8,), 0, 4)
    span_live = jnp.repeat(span_bits > 0, 8)
    opening = jnp.arange(TOKENS, dtype=jnp.int32) % WIN == 0
    return jnp.where(opening | span_live, 1, 0).astype(jnp.int32)


def target_plan(key):
    return jax.random.randint(jax.random.fold_in(key, 51), (TOKENS,), 0, VOCAB).astype(jnp.int32)


def draw_targets(key, part):
    return target_plan(key)


def draw_logits(key, part):
    row_scale = jnp.exp(jax.random.uniform(jax.random.fold_in(key, 61), (TOKENS, 1), jnp.float32, 0.0, math.log(10.0)))
    column_scale = jnp.exp(jax.random.uniform(jax.random.fold_in(key, 62), (1, VOCAB), jnp.float32, 0.0, math.log(10.0)))
    normal_part = jnp.clip(jax.random.normal(jax.random.fold_in(key, 63), (TOKENS, VOCAB), jnp.float32), -4.5, 4.5)
    base_logits = 0.3 * normal_part * row_scale * column_scale
    target_lift = jax.random.uniform(jax.random.fold_in(key, 65), (TOKENS, 1), jnp.float32, -3.0, 1.0)
    chosen = jnp.arange(VOCAB, dtype=jnp.int32)[None, :] == target_plan(key)[:, None]
    planted = jnp.where(chosen, jnp.max(base_logits, axis=1, keepdims=True) + target_lift, base_logits)
    return planted.astype(jnp.bfloat16)


def setup_inputs(seed: int = 0) -> dict:
    seeds = jax.random.split(jax.random.key(seed), 7)
    return {
        "rewards": draw_rewards(jax.random.fold_in(seeds[6], 71), 0),
        "group_ids": draw_group_ids(jax.random.fold_in(seeds[6], 71), 0),
        "lengths": draw_lengths(jax.random.fold_in(seeds[6], 71), 0),
        "token_mask": draw_token_mask(jax.random.fold_in(seeds[6], 71), 0),
        "targets": draw_targets(jax.random.fold_in(seeds[6], 71), 0),
        "logits": draw_logits(jax.random.fold_in(seeds[6], 71), 0),
    }


spread_floor = 0.25
reward_unit = 1024.0
highest = lax.Precision.HIGHEST

def window_statistics(inputs):
    logit_rows, row_targets = inputs
    values = logit_rows.astype(jnp.float32)
    row_peak = lax.optimization_barrier(jnp.max(values, axis=1))
    shifted = values - row_peak[:, None]
    weights = jnp.exp(shifted)
    totals = lax.optimization_barrier(jnp.sum(weights, axis=1))
    log_total = row_peak + jnp.log(totals)
    picked = jnp.take_along_axis(values, row_targets[:, None].astype(jnp.int32), axis=1)[:, 0]
    entropy = jnp.log(totals) - lax.optimization_barrier(jnp.sum(weights * shifted, axis=1)) / totals
    return (picked - log_total, entropy)

def reference(rewards, group_ids, lengths, token_mask, targets, logits):
    log_prob, entropy = lax.map(window_statistics, (logits.reshape(ROLLOUTS, WIN, VOCAB), targets.reshape(ROLLOUTS, WIN)))
    positions = jnp.arange(WIN, dtype=jnp.int32)
    live_mask = ((token_mask.reshape(ROLLOUTS, WIN) > 0) & (positions[None, :] < lengths[:, None])).astype(jnp.float32)
    token_logprob = live_mask * log_prob
    token_entropy = live_mask * entropy
    counts = lax.optimization_barrier(jnp.sum(live_mask, axis=1))
    reward_values = rewards.astype(jnp.float32) / reward_unit
    member = (group_ids[:, None] == jnp.arange(GROUPS, dtype=jnp.int32)[None, :]).astype(jnp.float32)
    group_mean = jnp.dot(reward_values, member, precision=highest) / GROUP
    centred = reward_values - jnp.dot(member, group_mean, precision=highest)
    group_var = jnp.dot(centred * centred, member, precision=highest) / GROUP
    group_spread = jnp.maximum(jnp.sqrt(group_var), spread_floor)
    group_tokens = jnp.dot(counts, member, precision=highest)
    advantage = centred / jnp.dot(member, group_spread, precision=highest)
    token_scale = GROUP * WIN / jnp.dot(member, group_tokens, precision=highest)
    token_weight = live_mask * (advantage * token_scale)[:, None]
    objective = -jnp.sum(token_weight * token_logprob) / (ROLLOUTS * WIN)
    return (advantage, token_weight.reshape(-1), token_logprob.reshape(-1), token_entropy.reshape(-1), objective)
```

```python
import jax
import jax.numpy as jnp
from jax import lax
from jax.experimental import pallas as pl
from jax.experimental.pallas import tpu as pltpu
from jax.sharding import Mesh
from jax.sharding import PartitionSpec as P

GROUP = 16
WIN = 64
LANES = 128
SUBLANES = 8
GROUPS = 4
MP = ("mp_0", "mp_1", "mp_2")

spread_floor = 0.25
reward_unit = 1024.0
highest = lax.Precision.HIGHEST


def lane_of(shape):
    return lax.broadcasted_iota(jnp.int32, shape, 1)


def row_of(shape):
    return lax.broadcasted_iota(jnp.int32, shape, 0)


def placed(contracted, block, precision=None):
    return lax.dot_general(
        contracted,
        block,
        (((1,), (1,)), ((), ())),
        precision=precision,
        preferred_element_type=jnp.float32,
    )


def local_kernel(
    rewards, group_ids, lengths, token_mask, targets, logits,
    send, token_info, own_info,
    tiles, target_rows, mask_rows, reward_of, group_of, length_of, sems,
):
    chunks = logits.shape[0] // LANES
    width = logits.shape[1]
    small = [
        pltpu.make_async_copy(targets, target_rows, sems.at[chunks]),
        pltpu.make_async_copy(token_mask, mask_rows, sems.at[chunks + 1]),
        pltpu.make_async_copy(rewards, reward_of, sems.at[chunks + 2]),
        pltpu.make_async_copy(group_ids, group_of, sems.at[chunks + 3]),
        pltpu.make_async_copy(lengths, length_of, sems.at[chunks + 4]),
    ]
    large = [
        pltpu.make_async_copy(
            logits.at[pl.ds(LANES * c, LANES)], tiles.at[pl.ds(LANES * c, LANES)], sems.at[c]
        )
        for c in range(chunks)
    ]
    small[0].start()
    for copy in large:
        copy.start()
    for copy in small[1:]:
        copy.start()
    column_start = (
        (lax.axis_index("mp_0") * lax.axis_size("mp_1") + lax.axis_index("mp_1"))
        * lax.axis_size("mp_2")
        + lax.axis_index("mp_2")
    ) * width
    for copy in small:
        copy.wait()

    shape = (SUBLANES, LANES)
    row, lane = row_of(shape), lane_of(shape)
    own_row = row == chunks
    reward_info = jnp.zeros(shape, jnp.float32)
    group_info = jnp.zeros(shape, jnp.int32)
    length_info = jnp.zeros(shape, jnp.int32)
    for i in range(2 * chunks):
        here = ((row == i // 2) & (lane // WIN == i % 2)) | (own_row & (lane == i))
        reward_info = jnp.where(here, reward_of[i].astype(jnp.float32), reward_info)
        group_info = jnp.where(here, group_of[i], group_info)
        length_info = jnp.where(here, length_of[i], length_info)
    reward_info = reward_info / reward_unit
    mask8 = jnp.concatenate([mask_rows[...], mask_rows[...]], axis=0)
    live = jnp.where((row < chunks) & (mask8 > 0) & (lane % WIN < length_info), 1.0, 0.0)
    token_info[0] = live
    token_info[1] = reward_info
    token_info[2] = group_info.astype(jnp.float32)
    even = jnp.sum(jnp.where(lane < WIN, live, 0.0), axis=1, keepdims=True)
    odd = jnp.sum(jnp.where(lane >= WIN, live, 0.0), axis=1, keepdims=True)
    spread_out = jnp.where((row == lane // 2) & (row < chunks), jnp.where(lane % 2 == 0, even, odd), 0.0)
    counts = jnp.sum(spread_out, axis=0, keepdims=True)
    own_reward = jnp.where(lane < 2 * chunks, reward_info[chunks : chunks + 1], 0.0)
    own_group = jnp.where(lane < 2 * chunks, group_info[chunks : chunks + 1].astype(jnp.float32), 0.0)
    own_info[...] = jnp.where(
        row == 1, counts, jnp.where(row == 2, own_reward, jnp.where(row == 3, own_group, 0.0))
    )

    block = (LANES, LANES)
    block_lane = lane_of(block)
    exact_tile = jnp.zeros(shape, jnp.float32)
    sum_tile = jnp.zeros(shape, jnp.float32)
    two_row, two_lane = row_of((SUBLANES, 2 * LANES)), lane_of((SUBLANES, 2 * LANES))
    for c in range(chunks):
        target_block = jnp.broadcast_to(target_rows[c : c + 1, :] - column_start, block).T
        large[c].wait()
        logit_block = tiles[LANES * c : LANES * (c + 1), :].astype(jnp.float32)
        row_peak = jnp.max(logit_block, axis=1, keepdims=True)
        totals = jnp.zeros(block, jnp.float32)
        moments = jnp.zeros(block, jnp.float32)
        picked = jnp.zeros(block, jnp.float32)
        for k in range(width // LANES):
            part = logit_block[:, LANES * k : LANES * (k + 1)]
            shifted = part - row_peak
            weights = jnp.exp(shifted)
            totals += weights
            moments += weights * shifted
            picked += jnp.where(target_block == block_lane + LANES * k, part, 0.0)
        peaks = jnp.broadcast_to(row_peak, block)
        exact_pick = jnp.where(
            ((two_row == c) & (two_lane == 0)) | ((two_row == chunks + c) & (two_lane >= LANES)), 1.0, 0.0
        )
        sum_pick = jnp.where(
            ((two_row == c) & (two_lane < LANES)) | ((two_row == chunks + c) & (two_lane >= LANES)), 1.0, 0.0
        )
        exact_tile += placed(
            exact_pick.astype(jnp.bfloat16),
            jnp.concatenate([peaks, picked], axis=1).astype(jnp.bfloat16),
        )
        sum_tile += placed(sum_pick, jnp.concatenate([totals, moments], axis=1), highest)
    for n in range(send.shape[0]):
        send[n, :SUBLANES] = exact_tile
        send[n, SUBLANES:] = sum_tile


def merged(received):
    shape = (SUBLANES, LANES)
    half = SUBLANES // 2
    upper = row_of(shape) < half
    heads = [received[n, :SUBLANES] for n in range(received.shape[0])]
    peaks = [jnp.where(upper, head, pltpu.roll(head, half, 0)) for head in heads]
    picked = sum(heads[1:], heads[0])
    joint = peaks[0]
    for peak in peaks[1:]:
        joint = jnp.maximum(joint, peak)
    sums = jnp.zeros(shape, jnp.float32)
    extra = jnp.zeros(shape, jnp.float32)
    for n, peak in enumerate(peaks):
        shift = peak - joint
        scaled = jnp.exp(shift) * received[n, SUBLANES:]
        sums += scaled
        extra += shift * scaled
    sums += jnp.where(upper, 0.0, pltpu.roll(extra, half, 0))
    return joint, picked, sums


def merge_kernel(received, send):
    joint, picked, sums = merged(received)
    upper = row_of((SUBLANES, LANES)) < SUBLANES // 2
    head = jnp.where(upper, joint, picked)
    for n in range(send.shape[0]):
        send[n, :SUBLANES] = head
        send[n, SUBLANES:] = sums


def token_kernel(received, token_info, own_info, send, token_values):
    half = SUBLANES // 2
    shape = (SUBLANES, LANES)
    row, lane = row_of(shape), lane_of(shape)
    upper = row < half
    joint, picked, sums = merged(received)
    target = pltpu.roll(picked, half, 0)
    moment = pltpu.roll(sums, half, 0)
    total = jnp.where(upper, sums, 1.0)
    log_sum = jnp.log(total)
    live = token_info[0]
    logprob = live * (target - (joint + log_sum))
    entropy = live * (log_sum - moment / total)
    token_values[:half] = logprob[:half]
    token_values[half:] = entropy[:half]
    logprob = jnp.where(upper, logprob, 0.0)
    even = jnp.sum(jnp.where(lane < WIN, logprob, 0.0), axis=1, keepdims=True)
    odd = jnp.sum(jnp.where(lane >= WIN, logprob, 0.0), axis=1, keepdims=True)
    spread_out = jnp.where((row == lane // 2) & upper, jnp.where(lane % 2 == 0, even, odd), 0.0)
    packed = jnp.where(row == 0, jnp.sum(spread_out, axis=0, keepdims=True), own_info[...])
    for n in range(send.shape[0]):
        send[n] = packed


def final_kernel(
    received, token_info, token_values,
    advantage, token_weight, token_logprob, token_entropy, objective,
    advantage_row, weight_rows, objective_row, sems,
):
    half = SUBLANES // 2
    copies = [
        pltpu.make_async_copy(token_values.at[pl.ds(0, half)], token_logprob, sems.at[0]),
        pltpu.make_async_copy(token_values.at[pl.ds(half, half)], token_entropy, sems.at[1]),
        pltpu.make_async_copy(weight_rows, token_weight, sems.at[2]),
        pltpu.make_async_copy(advantage_row, advantage, sems.at[3]),
        pltpu.make_async_copy(objective_row, objective, sems.at[4]),
    ]
    copies[0].start()
    copies[1].start()
    shape = (SUBLANES, LANES)
    row, lane = row_of(shape), lane_of(shape)
    own = received.shape[0]
    gathered = received[0]
    for d in range(1, own):
        gathered += pltpu.roll(received[d], SUBLANES * d, 1)
    logprob_sums, counts = gathered[0:1], gathered[1:2]
    reward_values, groups = gathered[2:3], gathered[3:4]
    slot = row % GROUPS
    first = row < GROUPS
    member = (groups == slot.astype(jnp.float32)) & (lane < SUBLANES * own)
    sums = jnp.sum(
        jnp.where(member, jnp.where(first, reward_values, counts), 0.0), axis=1, keepdims=True
    )
    group_mean = sums / GROUP

    def spread_over(chosen, values):
        return jnp.sum(jnp.where(member & chosen, values, 0.0), axis=0, keepdims=True)

    centred = reward_values - spread_over(first, group_mean)
    group_var = (
        jnp.sum(jnp.where(member & first, centred * centred, 0.0), axis=1, keepdims=True) / GROUP
    )
    group_spread = jnp.maximum(jnp.sqrt(group_var), spread_floor)
    live_rollouts = lane[0:1] < SUBLANES * own
    spread_row = jnp.where(live_rollouts, spread_over(first, group_spread), 1.0)
    tokens_row = jnp.where(live_rollouts, spread_over(~first, sums), 1.0)
    weights = centred / spread_row * (GROUP * WIN / tokens_row)
    products = jnp.where(live_rollouts, weights * logprob_sums, 0.0)
    total_rows = GROUPS * GROUP * WIN
    objective_row[...] = -jnp.sum(products, axis=1, keepdims=True) / total_rows
    copies[4].start()

    info_reward, info_group = token_info[1], token_info[2]
    mean, spread, tokens = group_mean[0:1], group_spread[0:1], sums[GROUPS : GROUPS + 1]
    for g in range(1, GROUPS):
        here = info_group == float(g)
        mean = jnp.where(here, group_mean[g : g + 1], mean)
        spread = jnp.where(here, group_spread[g : g + 1], spread)
        tokens = jnp.where(here, sums[GROUPS + g : GROUPS + g + 1], tokens)
    info_advantage = (info_reward - mean) / spread
    weight = token_info[0] * (info_advantage * (GROUP * WIN / tokens))
    advantage_row[...] = info_advantage[half : half + 1, :SUBLANES]
    copies[3].start()
    weight_rows[...] = weight[:half]
    copies[2].start()
    for copy in copies:
        copy.wait()


def shards(rewards, group_ids, lengths, token_mask, targets, logits):
    rows = logits.shape[0]
    chunks = rows // LANES
    f32, i32 = jnp.float32, jnp.int32
    any_spec = pl.BlockSpec(memory_space=pl.ANY)
    vmem = pl.BlockSpec(memory_space=pltpu.VMEM)
    stat_shape = (2 * SUBLANES, LANES)
    first_axes = ("mp_0", "mp_2")
    first_size = lax.axis_size("mp_0") * lax.axis_size("mp_2")
    sent, token_info, own_info = pl.pallas_call(
        local_kernel,
        name="local_stats",
        in_specs=[any_spec] * 6,
        out_specs=[vmem] * 3,
        out_shape=[
            jax.ShapeDtypeStruct((first_size, *stat_shape), f32),
            jax.ShapeDtypeStruct((3, SUBLANES, LANES), f32),
            jax.ShapeDtypeStruct((SUBLANES, LANES), f32),
        ],
        scratch_shapes=[
            pltpu.VMEM(logits.shape, logits.dtype),
            pltpu.VMEM((chunks, LANES), i32),
            pltpu.VMEM((chunks, LANES), i32),
            pltpu.SMEM(rewards.shape, i32),
            pltpu.SMEM(rewards.shape, i32),
            pltpu.SMEM(rewards.shape, i32),
            pltpu.SemaphoreType.DMA((chunks + 5,)),
        ],
    )(
        rewards,
        group_ids,
        lengths,
        token_mask.reshape(chunks, LANES),
        targets.reshape(chunks, LANES),
        logits,
    )
    received = lax.all_to_all(sent, first_axes, 0, 0, tiled=True)
    sent = pl.pallas_call(
        merge_kernel,
        name="merge_stats",
        in_specs=[vmem],
        out_specs=vmem,
        out_shape=jax.ShapeDtypeStruct((lax.axis_size("mp_1"), *stat_shape), f32),
    )(received)
    received = lax.all_to_all(sent, "mp_1", 0, 0, tiled=True)
    sent, token_values = pl.pallas_call(
        token_kernel,
        name="token_values",
        in_specs=[vmem] * 3,
        out_specs=[vmem] * 2,
        out_shape=[
            jax.ShapeDtypeStruct((lax.axis_size("dp"), SUBLANES, LANES), f32),
            jax.ShapeDtypeStruct((2 * chunks, LANES), f32),
        ],
    )(received, token_info, own_info)
    received = lax.all_to_all(sent, "dp", 0, 0, tiled=True)
    advantage, token_weight, token_logprob, token_entropy, objective = pl.pallas_call(
        final_kernel,
        name="group_values",
        in_specs=[vmem] * 3,
        out_specs=[any_spec] * 5,
        out_shape=[
            jax.ShapeDtypeStruct((1, SUBLANES), f32),
            jax.ShapeDtypeStruct((chunks, LANES), f32),
            jax.ShapeDtypeStruct((chunks, LANES), f32),
            jax.ShapeDtypeStruct((chunks, LANES), f32),
            jax.ShapeDtypeStruct((1, 1), f32),
        ],
        scratch_shapes=[
            pltpu.VMEM((1, SUBLANES), f32),
            pltpu.VMEM((chunks, LANES), f32),
            pltpu.VMEM((1, 1), f32),
            pltpu.SemaphoreType.DMA((5,)),
        ],
    )(received, token_info, token_values)
    return (
        advantage.reshape(-1),
        token_weight.reshape(-1),
        token_logprob.reshape(-1),
        token_entropy.reshape(-1),
        objective.reshape(()),
    )


def solution(mesh):
    split = Mesh(mesh.devices.reshape(mesh.shape["dp"], 8, 8, 2), ("dp", "mp_0", "mp_1", "mp_2"))
    in_specs = (P("dp"), P("dp"), P("dp"), P("dp"), P("dp"), P("dp", MP))
    out_specs = (P("dp"), P("dp"), P("dp"), P("dp"), P())
    return jax.shard_map(
        shards, mesh=split, in_specs=in_specs, out_specs=out_specs, check_vma=False
    )
```

```python
import jax
import jax.numpy as jnp
from jax import lax
from jax.experimental import pallas as pl
from jax.experimental.pallas import tpu as pltpu
from jax.sharding import Mesh
from jax.sharding import PartitionSpec as P

GROUP = 16
WIN = 64
LANES = 128
SUBLANES = 8
GROUPS = 4
MP = ("mp_0", "mp_1", "mp_2")

spread_floor = 0.25
reward_unit = 1024.0
highest = lax.Precision.HIGHEST


def lane_of(shape):
    return lax.broadcasted_iota(jnp.int32, shape, 1)


def row_of(shape):
    return lax.broadcasted_iota(jnp.int32, shape, 0)


def placed(contracted, block, precision=None):
    return lax.dot_general(
        contracted,
        block,
        (((1,), (1,)), ((), ())),
        precision=precision,
        preferred_element_type=jnp.float32,
    )


def local_kernel(
    rewards, group_ids, lengths, token_mask, targets, logits,
    send, token_info, own_info,
    tiles, target_rows, mask_rows, reward_of, group_of, length_of, sems,
):
    chunks = logits.shape[0] // LANES
    width = logits.shape[1]
    small = [
        pltpu.make_async_copy(targets, target_rows, sems.at[chunks]),
        pltpu.make_async_copy(token_mask, mask_rows, sems.at[chunks + 1]),
        pltpu.make_async_copy(rewards, reward_of, sems.at[chunks + 2]),
        pltpu.make_async_copy(group_ids, group_of, sems.at[chunks + 3]),
        pltpu.make_async_copy(lengths, length_of, sems.at[chunks + 4]),
    ]
    large = [
        pltpu.make_async_copy(
            logits.at[pl.ds(LANES * c, LANES)], tiles.at[pl.ds(LANES * c, LANES)], sems.at[c]
        )
        for c in range(chunks)
    ]
    small[0].start()
    for copy in large:
        copy.start()
    for copy in small[1:]:
        copy.start()
    column_start = (
        (lax.axis_index("mp_0") * lax.axis_size("mp_1") + lax.axis_index("mp_1"))
        * lax.axis_size("mp_2")
        + lax.axis_index("mp_2")
    ) * width
    for copy in small:
        copy.wait()

    shape = (SUBLANES, LANES)
    row, lane = row_of(shape), lane_of(shape)
    own_row = row == chunks
    reward_info = jnp.zeros(shape, jnp.float32)
    group_info = jnp.zeros(shape, jnp.int32)
    length_info = jnp.zeros(shape, jnp.int32)
    for i in range(2 * chunks):
        here = ((row == i // 2) & (lane // WIN == i % 2)) | (own_row & (lane == i))
        reward_info = jnp.where(here, reward_of[i].astype(jnp.float32), reward_info)
        group_info = jnp.where(here, group_of[i], group_info)
        length_info = jnp.where(here, length_of[i], length_info)
    reward_info = reward_info / reward_unit
    mask8 = jnp.concatenate([mask_rows[...], mask_rows[...]], axis=0)
    live = jnp.where((row < chunks) & (mask8 > 0) & (lane % WIN < length_info), 1.0, 0.0)
    token_info[0] = live
    token_info[1] = reward_info
    token_info[2] = group_info.astype(jnp.float32)
    even = jnp.sum(jnp.where(lane < WIN, live, 0.0), axis=1, keepdims=True)
    odd = jnp.sum(jnp.where(lane >= WIN, live, 0.0), axis=1, keepdims=True)
    spread_out = jnp.where((row == lane // 2) & (row < chunks), jnp.where(lane % 2 == 0, even, odd), 0.0)
    counts = jnp.sum(spread_out, axis=0, keepdims=True)
    own_reward = jnp.where(lane < 2 * chunks, reward_info[chunks : chunks + 1], 0.0)
    own_group = jnp.where(lane < 2 * chunks, group_info[chunks : chunks + 1].astype(jnp.float32), 0.0)
    own_info[...] = jnp.where(
        row == 1, counts, jnp.where(row == 2, own_reward, jnp.where(row == 3, own_group, 0.0))
    )

    block = (LANES, LANES)
    block_lane = lane_of(block)
    exact_tile = jnp.zeros(shape, jnp.float32)
    sum_tile = jnp.zeros(shape, jnp.float32)
    two_row, two_lane = row_of((SUBLANES, 2 * LANES)), lane_of((SUBLANES, 2 * LANES))
    for c in range(chunks):
        target_block = jnp.broadcast_to(target_rows[c : c + 1, :] - column_start, block).T
        large[c].wait()
        logit_block = tiles[LANES * c : LANES * (c + 1), :].astype(jnp.float32)
        row_peak = jnp.max(logit_block, axis=1, keepdims=True)
        totals = jnp.zeros(block, jnp.float32)
        moments = jnp.zeros(block, jnp.float32)
        picked = jnp.zeros(block, jnp.float32)
        for k in range(width // LANES):
            part = logit_block[:, LANES * k : LANES * (k + 1)]
            shifted = part - row_peak
            weights = jnp.exp(shifted)
            totals += weights
            moments += weights * shifted
            picked += jnp.where(target_block == block_lane + LANES * k, part, 0.0)
        peaks = jnp.broadcast_to(row_peak, block)
        exact_pick = jnp.where(
            ((two_row == c) & (two_lane == 0)) | ((two_row == chunks + c) & (two_lane >= LANES)), 1.0, 0.0
        )
        sum_pick = jnp.where(
            ((two_row == c) & (two_lane < LANES)) | ((two_row == chunks + c) & (two_lane >= LANES)), 1.0, 0.0
        )
        exact_tile += placed(
            exact_pick.astype(jnp.bfloat16),
            jnp.concatenate([peaks, picked], axis=1).astype(jnp.bfloat16),
        )
        sum_tile += placed(sum_pick, jnp.concatenate([totals, moments], axis=1), highest)
    for n in range(send.shape[0]):
        send[n, :SUBLANES] = exact_tile
        send[n, SUBLANES:] = sum_tile


def merged(received):
    shape = (SUBLANES, LANES)
    half = SUBLANES // 2
    upper = row_of(shape) < half
    heads = [received[n, :SUBLANES] for n in range(received.shape[0])]
    peaks = [jnp.where(upper, head, pltpu.roll(head, half, 0)) for head in heads]
    picked = sum(heads[1:], heads[0])
    joint = peaks[0]
    for peak in peaks[1:]:
        joint = jnp.maximum(joint, peak)
    sums = jnp.zeros(shape, jnp.float32)
    extra = jnp.zeros(shape, jnp.float32)
    for n, peak in enumerate(peaks):
        shift = peak - joint
        scaled = jnp.exp(shift) * received[n, SUBLANES:]
        sums += scaled
        extra += shift * scaled
    sums += jnp.where(upper, 0.0, pltpu.roll(extra, half, 0))
    return joint, picked, sums


def merge_kernel(received, send):
    joint, picked, sums = merged(received)
    upper = row_of((SUBLANES, LANES)) < SUBLANES // 2
    head = jnp.where(upper, joint, picked)
    for n in range(send.shape[0]):
        send[n, :SUBLANES] = head
        send[n, SUBLANES:] = sums


def token_kernel(received, token_info, own_info, send, token_values):
    half = SUBLANES // 2
    shape = (SUBLANES, LANES)
    row, lane = row_of(shape), lane_of(shape)
    upper = row < half
    joint, picked, sums = merged(received)
    target = pltpu.roll(picked, half, 0)
    moment = pltpu.roll(sums, half, 0)
    total = jnp.where(upper, sums, 1.0)
    log_sum = jnp.log(total)
    live = token_info[0]
    logprob = live * (target - (joint + log_sum))
    entropy = live * (log_sum - moment / total)
    token_values[:half] = logprob[:half]
    token_values[half:] = entropy[:half]
    logprob = jnp.where(upper, logprob, 0.0)
    even = jnp.sum(jnp.where(lane < WIN, logprob, 0.0), axis=1, keepdims=True)
    odd = jnp.sum(jnp.where(lane >= WIN, logprob, 0.0), axis=1, keepdims=True)
    spread_out = jnp.where((row == lane // 2) & upper, jnp.where(lane % 2 == 0, even, odd), 0.0)
    packed = jnp.where(row == 0, jnp.sum(spread_out, axis=0, keepdims=True), own_info[...])
    for n in range(send.shape[0]):
        send[n] = packed


def final_kernel(
    received, token_info, token_values,
    advantage, token_weight, token_logprob, token_entropy, objective,
    advantage_row, weight_rows, objective_row, sems,
):
    half = SUBLANES // 2
    copies = [
        pltpu.make_async_copy(token_values.at[pl.ds(0, half)], token_logprob, sems.at[0]),
        pltpu.make_async_copy(token_values.at[pl.ds(half, half)], token_entropy, sems.at[1]),
        pltpu.make_async_copy(weight_rows, token_weight, sems.at[2]),
        pltpu.make_async_copy(advantage_row, advantage, sems.at[3]),
        pltpu.make_async_copy(objective_row, objective, sems.at[4]),
    ]
    copies[0].start()
    copies[1].start()
    shape = (SUBLANES, LANES)
    row, lane = row_of(shape), lane_of(shape)
    own = received.shape[0]
    gathered = received[0]
    for d in range(1, own):
        gathered += pltpu.roll(received[d], SUBLANES * d, 1)
    logprob_sums, counts = gathered[0:1], gathered[1:2]
    reward_values, groups = gathered[2:3], gathered[3:4]
    slot = row % GROUPS
    first = row < GROUPS
    member = (groups == slot.astype(jnp.float32)) & (lane < SUBLANES * own)
    sums = jnp.sum(
        jnp.where(member, jnp.where(first, reward_values, counts), 0.0), axis=1, keepdims=True
    )
    group_mean = sums / GROUP

    def spread_over(chosen, values):
        return jnp.sum(jnp.where(member & chosen, values, 0.0), axis=0, keepdims=True)

    centred = reward_values - spread_over(first, group_mean)
    group_var = (
        jnp.sum(jnp.where(member & first, centred * centred, 0.0), axis=1, keepdims=True) / GROUP
    )
    group_spread = jnp.maximum(jnp.sqrt(group_var), spread_floor)
    live_rollouts = lane[0:1] < SUBLANES * own
    spread_row = jnp.where(live_rollouts, spread_over(first, group_spread), 1.0)
    tokens_row = jnp.where(live_rollouts, spread_over(~first, sums), 1.0)
    weights = centred / spread_row * (GROUP * WIN / tokens_row)
    products = jnp.where(live_rollouts, weights * logprob_sums, 0.0)
    total_rows = GROUPS * GROUP * WIN
    objective_row[...] = -jnp.sum(products, axis=1, keepdims=True) / total_rows
    copies[4].start()

    info_reward, info_group = token_info[1], token_info[2]
    mean, spread, tokens = group_mean[0:1], group_spread[0:1], sums[GROUPS : GROUPS + 1]
    for g in range(1, GROUPS):
        here = info_group == float(g)
        mean = jnp.where(here, group_mean[g : g + 1], mean)
        spread = jnp.where(here, group_spread[g : g + 1], spread)
        tokens = jnp.where(here, sums[GROUPS + g : GROUPS + g + 1], tokens)
    info_advantage = (info_reward - mean) / spread
    weight = token_info[0] * (info_advantage * (GROUP * WIN / tokens))
    advantage_row[...] = info_advantage[half : half + 1, :SUBLANES]
    copies[3].start()
    weight_rows[...] = weight[:half]
    copies[2].start()
    for copy in copies:
        copy.wait()


def shards(rewards, group_ids, lengths, token_mask, targets, logits):
    rows = logits.shape[0]
    chunks = rows // LANES
    f32, i32 = jnp.float32, jnp.int32
    any_spec = pl.BlockSpec(memory_space=pl.ANY)

    def kept(shape):
        return pltpu.VMEM(shape, f32)

    def near(array):
        return pltpu.with_memory_space_constraint(array, pltpu.VMEM)

    vmem = pl.BlockSpec(memory_space=pltpu.VMEM)
    stat_shape = (2 * SUBLANES, LANES)
    first_axes = ("mp_0", "mp_2")
    first_size = lax.axis_size("mp_0") * lax.axis_size("mp_2")
    sent, token_info, own_info = pl.pallas_call(
        local_kernel,
        name="local_stats",
        in_specs=[any_spec] * 6,
        out_specs=[vmem] * 3,
        out_shape=[
            kept((first_size, *stat_shape)),
            kept((3, SUBLANES, LANES)),
            kept((SUBLANES, LANES)),
        ],
        scratch_shapes=[
            pltpu.VMEM(logits.shape, logits.dtype),
            pltpu.VMEM((chunks, LANES), i32),
            pltpu.VMEM((chunks, LANES), i32),
            pltpu.SMEM(rewards.shape, i32),
            pltpu.SMEM(rewards.shape, i32),
            pltpu.SMEM(rewards.shape, i32),
            pltpu.SemaphoreType.DMA((chunks + 5,)),
        ],
    )(
        rewards,
        group_ids,
        lengths,
        token_mask.reshape(chunks, LANES),
        targets.reshape(chunks, LANES),
        logits,
    )
    received = lax.all_to_all(sent, first_axes, 0, 0, tiled=True)
    sent = pl.pallas_call(
        merge_kernel,
        name="merge_stats",
        in_specs=[vmem],
        out_specs=vmem,
        out_shape=kept((lax.axis_size("mp_1"), *stat_shape)),
    )(near(received))
    received = lax.all_to_all(sent, "mp_1", 0, 0, tiled=True)
    sent, token_values = pl.pallas_call(
        token_kernel,
        name="token_values",
        in_specs=[vmem] * 3,
        out_specs=[vmem] * 2,
        out_shape=[
            kept((lax.axis_size("dp"), SUBLANES, LANES)),
            kept((2 * chunks, LANES)),
        ],
    )(near(received), near(token_info), near(own_info))
    received = lax.all_to_all(sent, "dp", 0, 0, tiled=True)
    advantage, token_weight, token_logprob, token_entropy, objective = pl.pallas_call(
        final_kernel,
        name="group_values",
        in_specs=[vmem] * 3,
        out_specs=[any_spec] * 5,
        out_shape=[
            jax.ShapeDtypeStruct((1, SUBLANES), f32),
            jax.ShapeDtypeStruct((chunks, LANES), f32),
            jax.ShapeDtypeStruct((chunks, LANES), f32),
            jax.ShapeDtypeStruct((chunks, LANES), f32),
            jax.ShapeDtypeStruct((1, 1), f32),
        ],
        scratch_shapes=[
            pltpu.VMEM((1, SUBLANES), f32),
            pltpu.VMEM((chunks, LANES), f32),
            pltpu.VMEM((1, 1), f32),
            pltpu.SemaphoreType.DMA((5,)),
        ],
    )(near(received), near(token_info), near(token_values))
    return (
        advantage.reshape(-1),
        token_weight.reshape(-1),
        token_logprob.reshape(-1),
        token_entropy.reshape(-1),
        objective.reshape(()),
    )


def solution(mesh):
    split = Mesh(mesh.devices.reshape(mesh.shape["dp"], 8, 8, 2), ("dp", "mp_0", "mp_1", "mp_2"))
    in_specs = (P("dp"), P("dp"), P("dp"), P("dp"), P("dp"), P("dp", MP))
    out_specs = (P("dp"), P("dp"), P("dp"), P("dp"), P())
    return jax.shard_map(
        shards, mesh=split, in_specs=in_specs, out_specs=out_specs, check_vma=False
    )
```

```python
import jax
import jax.numpy as jnp
from jax import lax
from jax.experimental import pallas as pl
from jax.experimental.pallas import tpu as pltpu
from jax.sharding import Mesh
from jax.sharding import PartitionSpec as P

GROUP = 16
WIN = 64
LANES = 128
SUBLANES = 8
GROUPS = 4
MP = ("mp_0", "mp_1", "mp_2")

spread_floor = 0.25
reward_unit = 1024.0
highest = lax.Precision.HIGHEST


def lane_of(shape):
    return lax.broadcasted_iota(jnp.int32, shape, 1)


def row_of(shape):
    return lax.broadcasted_iota(jnp.int32, shape, 0)


def placed(contracted, block, precision=None):
    return lax.dot_general(
        contracted,
        block,
        (((1,), (1,)), ((), ())),
        precision=precision,
        preferred_element_type=jnp.float32,
    )


def local_kernel(
    rewards, group_ids, lengths, token_mask, targets, logits,
    send, token_info, own_info,
    tiles, target_rows, mask_rows, reward_of, group_of, length_of, sems,
):
    chunks = logits.shape[0] // LANES
    width = logits.shape[1]
    cores = lax.axis_size("mp_2")
    core = lax.axis_index("mp_2")
    part = chunks // cores
    small = [
        pltpu.make_async_copy(targets, target_rows, sems.at[chunks]),
        pltpu.make_async_copy(token_mask, mask_rows, sems.at[chunks + 1]),
        pltpu.make_async_copy(rewards, reward_of, sems.at[chunks + 2]),
        pltpu.make_async_copy(group_ids, group_of, sems.at[chunks + 3]),
        pltpu.make_async_copy(lengths, length_of, sems.at[chunks + 4]),
    ]
    large = [
        pltpu.make_async_copy(
            logits.at[pl.ds(LANES * c, LANES)], tiles.at[pl.ds(LANES * c, LANES)], sems.at[c]
        )
        for c in range(chunks)
    ]
    small[0].start()
    for copy in large:
        copy.start()
    for copy in small[1:]:
        copy.start()
    column_start = (
        (lax.axis_index("mp_0") * lax.axis_size("mp_1") + lax.axis_index("mp_1")) * cores + core
    ) * width
    small[0].wait()

    shape = (SUBLANES, LANES)
    block = (LANES, LANES)
    block_lane = lane_of(block)
    exact_row, exact_lane = row_of((SUBLANES, 2 * LANES)), lane_of((SUBLANES, 2 * LANES))
    packed = []
    for c in range(chunks):
        k_row = c % part
        target_block = jnp.broadcast_to(target_rows[c : c + 1, :] - column_start, block).T
        large[c].wait()
        logit_block = tiles[LANES * c : LANES * (c + 1), :].astype(jnp.float32)
        row_peak = jnp.max(logit_block, axis=1, keepdims=True)
        totals = jnp.zeros(block, jnp.float32)
        moments = jnp.zeros(block, jnp.float32)
        picked = jnp.zeros(block, jnp.float32)
        for k in range(width // LANES):
            segment = logit_block[:, LANES * k : LANES * (k + 1)]
            shifted = segment - row_peak
            weights = jnp.exp(shifted)
            totals += weights
            moments += weights * shifted
            picked += jnp.where(target_block == block_lane + LANES * k, segment, 0.0)
        peaks = jnp.broadcast_to(row_peak, block)
        exact_pick = jnp.where(
            ((exact_row == k_row) & (exact_lane == 0))
            | ((exact_row == part + k_row) & (exact_lane >= LANES)),
            1.0,
            0.0,
        )
        sum_pick = jnp.where(
            ((exact_row == 2 * part + k_row) & (exact_lane < LANES))
            | ((exact_row == 3 * part + k_row) & (exact_lane >= LANES)),
            1.0,
            0.0,
        )
        tile = placed(
            exact_pick.astype(jnp.bfloat16),
            jnp.concatenate([peaks, picked], axis=1).astype(jnp.bfloat16),
        ) + placed(sum_pick, jnp.concatenate([totals, moments], axis=1), highest)
        if k_row == 0:
            packed.append(tile)
        else:
            packed[-1] += tile
    for n in range(send.shape[0]):
        send[n] = packed[n % cores]

    for copy in small[1:]:
        copy.wait()
    row, lane = row_of(shape), lane_of(shape)
    own_row = row == chunks
    reward_info = jnp.zeros(shape, jnp.float32)
    group_info = jnp.zeros(shape, jnp.int32)
    length_info = jnp.zeros(shape, jnp.int32)
    for i in range(2 * chunks):
        here = ((row == i // 2) & (lane // WIN == i % 2)) | (own_row & (lane == i))
        reward_info = jnp.where(here, reward_of[i].astype(jnp.float32), reward_info)
        group_info = jnp.where(here, group_of[i], group_info)
        length_info = jnp.where(here, length_of[i], length_info)
    reward_info = reward_info / reward_unit
    mask8 = jnp.concatenate([mask_rows[...], mask_rows[...]], axis=0)
    live = jnp.where((row < chunks) & (mask8 > 0) & (lane % WIN < length_info), 1.0, 0.0)
    token_info[0] = live
    token_info[1] = reward_info
    token_info[2] = group_info.astype(jnp.float32)
    token_info[3] = jnp.where(core == 0, live, pltpu.roll(live, SUBLANES - part, 0))
    even = jnp.sum(jnp.where(lane < WIN, live, 0.0), axis=1, keepdims=True)
    odd = jnp.sum(jnp.where(lane >= WIN, live, 0.0), axis=1, keepdims=True)
    spread_out = jnp.where(
        (row == lane // 2) & (row < chunks), jnp.where(lane % 2 == 0, even, odd), 0.0
    )
    counts = jnp.sum(spread_out, axis=0, keepdims=True)
    own_reward = jnp.where(lane < 2 * chunks, reward_info[chunks : chunks + 1], 0.0)
    own_group = jnp.where(
        lane < 2 * chunks, group_info[chunks : chunks + 1].astype(jnp.float32), 0.0
    )
    own_info[...] = jnp.where(
        row == 5, counts, jnp.where(row == 6, own_reward, jnp.where(row == 7, own_group, 0.0))
    )


def merged(received):
    shape = (SUBLANES, LANES)
    row = row_of(shape)
    tiles = [received[n] for n in range(received.shape[0])]
    peaks = [
        jnp.where(
            row < 2,
            tile,
            jnp.where(
                row < 4,
                pltpu.roll(tile, 2, 0),
                jnp.where(row < 6, pltpu.roll(tile, 4, 0), pltpu.roll(tile, 6, 0)),
            ),
        )
        for tile in tiles
    ]
    joint = peaks[0]
    for peak in peaks[1:]:
        joint = jnp.maximum(joint, peak)
    sums = jnp.zeros(shape, jnp.float32)
    extra = jnp.zeros(shape, jnp.float32)
    for tile, peak in zip(tiles, peaks):
        shift = peak - joint
        scaled = jnp.exp(shift) * tile
        sums += jnp.where(row < 4, tile, scaled)
        extra += shift * scaled
    sums += jnp.where(row < 6, 0.0, pltpu.roll(extra, 2, 0))
    return jnp.where(row < 2, joint, sums)


def merge_kernel(received, send):
    tile = merged(received)
    for n in range(send.shape[0]):
        send[n] = tile


def token_kernel(received, token_info, own_info, send):
    shape = (SUBLANES, LANES)
    row, lane = row_of(shape), lane_of(shape)
    part = token_info.shape[1] // 2 // lax.axis_size("mp_2")
    first = 2 * part * lax.axis_index("mp_2")
    tile = merged(received)
    upper = row < part
    target = pltpu.roll(tile, 6, 0)
    total = jnp.where(upper, pltpu.roll(tile, 4, 0), 1.0)
    moment = pltpu.roll(tile, 2, 0)
    log_sum = jnp.log(total)
    live = token_info[3]
    logprob = jnp.where(upper, live * (target - (tile + log_sum)), 0.0)
    entropy = jnp.where(upper, live * (log_sum - moment / total), 0.0)
    even = jnp.sum(jnp.where(lane < WIN, logprob, 0.0), axis=1, keepdims=True)
    odd = jnp.sum(jnp.where(lane >= WIN, logprob, 0.0), axis=1, keepdims=True)
    own_lane = lane - first
    spread_out = jnp.where(
        (own_lane >= 0) & (row == own_lane // 2) & upper,
        jnp.where(lane % 2 == 0, even, odd),
        0.0,
    )
    packed = jnp.where(
        upper,
        logprob,
        jnp.where(
            row < 4,
            pltpu.roll(entropy, 2, 0),
            jnp.where(row == 4, jnp.sum(spread_out, axis=0, keepdims=True), own_info[...]),
        ),
    )
    for n in range(send.shape[0]):
        send[n] = packed


def final_kernel(
    received, token_info,
    advantage, token_weight, token_logprob, token_entropy, objective,
    advantage_row, weight_rows, logprob_rows, entropy_rows, objective_row, sems,
):
    chunks = token_weight.shape[0]
    copies = [
        pltpu.make_async_copy(logprob_rows, token_logprob, sems.at[0]),
        pltpu.make_async_copy(entropy_rows, token_entropy, sems.at[1]),
        pltpu.make_async_copy(weight_rows, token_weight, sems.at[2]),
        pltpu.make_async_copy(advantage_row, advantage, sems.at[3]),
        pltpu.make_async_copy(objective_row, objective, sems.at[4]),
    ]
    shape = (SUBLANES, LANES)
    row, lane = row_of(shape), lane_of(shape)
    shards = lax.axis_size("dp")
    here = 2 * lax.axis_index("dp")
    low, high = received[here], received[here + 1]
    logprob_rows[...] = jnp.where(row < 2, low, pltpu.roll(high, 2, 0))[:chunks]
    copies[0].start()
    entropy_rows[...] = jnp.where(row < 2, pltpu.roll(low, 6, 0), high)[:chunks]
    copies[1].start()
    gathered = jnp.zeros(shape, jnp.float32)
    for d in range(shards):
        pair = received[2 * d] + jnp.where(row == 4, received[2 * d + 1], 0.0)
        gathered += pltpu.roll(pair, SUBLANES * d, 1) if d else pair
    valid = lane < SUBLANES * shards
    logprob_sums, counts = gathered[4:5], gathered[5:6]
    reward_values, groups = gathered[6:7], gathered[7:8]
    slot = row % GROUPS
    first = row < GROUPS
    member = (groups == slot.astype(jnp.float32)) & valid
    sums = jnp.sum(
        jnp.where(member, jnp.where(first, reward_values, counts), 0.0), axis=1, keepdims=True
    )
    group_mean = sums / GROUP

    def spread_over(chosen, values):
        return jnp.sum(jnp.where(member & chosen, values, 0.0), axis=0, keepdims=True)

    centred = reward_values - spread_over(first, group_mean)
    group_var = (
        jnp.sum(jnp.where(member & first, centred * centred, 0.0), axis=1, keepdims=True) / GROUP
    )
    group_spread = jnp.maximum(jnp.sqrt(group_var), spread_floor)
    spread_row = jnp.where(valid[:1], spread_over(first, group_spread), 1.0)
    tokens_row = jnp.where(valid[:1], spread_over(~first, sums), 1.0)
    weights = centred / spread_row * (GROUP * WIN / tokens_row)
    products = jnp.where(valid[:1], weights * logprob_sums, 0.0)
    total_rows = GROUPS * GROUP * WIN
    objective_row[...] = -jnp.sum(products, axis=1, keepdims=True) / total_rows
    copies[4].start()

    info_reward, info_group = token_info[1], token_info[2]
    mean, spread, tokens = group_mean[0:1], group_spread[0:1], sums[GROUPS : GROUPS + 1]
    for g in range(1, GROUPS):
        chosen = info_group == float(g)
        mean = jnp.where(chosen, group_mean[g : g + 1], mean)
        spread = jnp.where(chosen, group_spread[g : g + 1], spread)
        tokens = jnp.where(chosen, sums[GROUPS + g : GROUPS + g + 1], tokens)
    info_advantage = (info_reward - mean) / spread
    weight = token_info[0] * (info_advantage * (GROUP * WIN / tokens))
    advantage_row[...] = info_advantage[chunks : chunks + 1, :SUBLANES]
    copies[3].start()
    weight_rows[...] = weight[:chunks]
    copies[2].start()
    for copy in copies:
        copy.wait()


def shards(rewards, group_ids, lengths, token_mask, targets, logits):
    rows = logits.shape[0]
    chunks = rows // LANES
    f32, i32 = jnp.float32, jnp.int32
    any_spec = pl.BlockSpec(memory_space=pl.ANY)

    def kept(shape):
        return pltpu.VMEM(shape, f32)

    def near(array):
        return pltpu.with_memory_space_constraint(array, pltpu.VMEM)

    vmem = pl.BlockSpec(memory_space=pltpu.VMEM)
    stat_shape = (SUBLANES, LANES)
    first_axes = ("mp_0", "mp_2")
    first_size = lax.axis_size("mp_0") * lax.axis_size("mp_2")
    sent, token_info, own_info = pl.pallas_call(
        local_kernel,
        name="local_stats",
        in_specs=[any_spec] * 6,
        out_specs=[vmem] * 3,
        out_shape=[
            kept((first_size, *stat_shape)),
            kept((4, SUBLANES, LANES)),
            kept((SUBLANES, LANES)),
        ],
        scratch_shapes=[
            pltpu.VMEM(logits.shape, logits.dtype),
            pltpu.VMEM((chunks, LANES), i32),
            pltpu.VMEM((chunks, LANES), i32),
            pltpu.SMEM(rewards.shape, i32),
            pltpu.SMEM(rewards.shape, i32),
            pltpu.SMEM(rewards.shape, i32),
            pltpu.SemaphoreType.DMA((chunks + 5,)),
        ],
    )(
        rewards,
        group_ids,
        lengths,
        token_mask.reshape(chunks, LANES),
        targets.reshape(chunks, LANES),
        logits,
    )
    received = lax.all_to_all(sent, first_axes, 0, 0, tiled=True)
    sent = pl.pallas_call(
        merge_kernel,
        name="merge_stats",
        in_specs=[vmem],
        out_specs=vmem,
        out_shape=kept((lax.axis_size("mp_1"), *stat_shape)),
    )(near(received))
    received = lax.all_to_all(sent, "mp_1", 0, 0, tiled=True)
    last_axes = ("dp", "mp_2")
    last_size = lax.axis_size("dp") * lax.axis_size("mp_2")
    sent = pl.pallas_call(
        token_kernel,
        name="token_values",
        in_specs=[vmem] * 3,
        out_specs=vmem,
        out_shape=kept((last_size, *stat_shape)),
    )(near(received), near(token_info), near(own_info))
    received = lax.all_to_all(sent, last_axes, 0, 0, tiled=True)
    advantage, token_weight, token_logprob, token_entropy, objective = pl.pallas_call(
        final_kernel,
        name="group_values",
        in_specs=[vmem] * 2,
        out_specs=[any_spec] * 5,
        out_shape=[
            jax.ShapeDtypeStruct((1, SUBLANES), f32),
            jax.ShapeDtypeStruct((chunks, LANES), f32),
            jax.ShapeDtypeStruct((chunks, LANES), f32),
            jax.ShapeDtypeStruct((chunks, LANES), f32),
            jax.ShapeDtypeStruct((1, 1), f32),
        ],
        scratch_shapes=[
            pltpu.VMEM((1, SUBLANES), f32),
            pltpu.VMEM((chunks, LANES), f32),
            pltpu.VMEM((chunks, LANES), f32),
            pltpu.VMEM((chunks, LANES), f32),
            pltpu.VMEM((1, 1), f32),
            pltpu.SemaphoreType.DMA((5,)),
        ],
    )(near(received), near(token_info))
    return (
        advantage.reshape(-1),
        token_weight.reshape(-1),
        token_logprob.reshape(-1),
        token_entropy.reshape(-1),
        objective.reshape(()),
    )


def solution(mesh):
    split = Mesh(mesh.devices.reshape(mesh.shape["dp"], 8, 8, 2), ("dp", "mp_0", "mp_1", "mp_2"))
    in_specs = (P("dp"), P("dp"), P("dp"), P("dp"), P("dp"), P("dp", MP))
    out_specs = (P("dp"), P("dp"), P("dp"), P("dp"), P())
    return jax.shard_map(
        shards, mesh=split, in_specs=in_specs, out_specs=out_specs, check_vma=False
    )
```

```python
import jax
import jax.numpy as jnp
from jax import lax
from jax.experimental import pallas as pl
from jax.experimental.pallas import tpu as pltpu
from jax.sharding import Mesh
from jax.sharding import PartitionSpec as P

GROUP = 16
WIN = 64
LANES = 128
SUBLANES = 8
GROUPS = 4
STEP = 16
MP = ("mp_0", "mp_1", "mp_2")

spread_floor = 0.25
reward_unit = 1024.0


def lane_of(shape):
    return lax.broadcasted_iota(jnp.int32, shape, 1)


def row_of(shape):
    return lax.broadcasted_iota(jnp.int32, shape, 0)


def lines_to_lanes(pick, block):
    return lax.dot_general(
        pick, block, (((1,), (1,)), ((), ())), preferred_element_type=jnp.float32
    )


def local_kernel(
    rewards, group_ids, lengths, token_mask, targets, logits,
    send, token_info, own_info,
    tiles, target_rows, mask_rows, reward_of, group_of, length_of, peak_rows, columns, sems,
):
    chunks = logits.shape[0] // LANES
    width = logits.shape[1]
    targets_copy = pltpu.make_async_copy(targets, target_rows, sems.at[0])
    small = [
        pltpu.make_async_copy(token_mask, mask_rows, sems.at[1]),
        pltpu.make_async_copy(rewards, reward_of, sems.at[2]),
        pltpu.make_async_copy(group_ids, group_of, sems.at[3]),
        pltpu.make_async_copy(lengths, length_of, sems.at[4]),
    ]
    logits_copy = pltpu.make_async_copy(logits, tiles, sems.at[5])
    targets_copy.start()
    for copy in small:
        copy.start()
    logits_copy.start()
    shard = (
        lax.axis_index("mp_0") * lax.axis_size("mp_1") + lax.axis_index("mp_1")
    ) * lax.axis_size("mp_2") + lax.axis_index("mp_2")
    targets_copy.wait()

    block = (LANES, LANES)
    diagonal = row_of(block) == lane_of(block)
    digit_row = row_of((2 * LANES, LANES))
    digits = jnp.where(digit_row < LANES, 1.0, float(LANES)).astype(jnp.bfloat16)
    local = target_rows[...] - shard * width
    inside = (local >= 0) & (local < width)
    low_digit = jnp.where(inside, local % LANES, -1).astype(jnp.float32)
    high_digit = jnp.where(inside, local // LANES, 0).astype(jnp.float32)
    for c in range(chunks):
        spread = jnp.concatenate(
            [
                jnp.where(diagonal, low_digit[c : c + 1], 0.0),
                jnp.where(diagonal, high_digit[c : c + 1], 0.0),
            ],
            axis=1,
        ).astype(jnp.bfloat16)
        columns[LANES * c : LANES * (c + 1), :] = jnp.dot(
            spread, digits, preferred_element_type=jnp.float32
        )

    for copy in small:
        copy.wait()
    shape = (SUBLANES, LANES)
    row, lane = row_of(shape), lane_of(shape)
    reward_info = jnp.zeros(shape, jnp.float32)
    group_info = jnp.zeros(shape, jnp.float32)
    length_info = jnp.zeros(shape, jnp.int32)
    own = jnp.zeros(shape, jnp.float32)
    for i in range(2 * chunks):
        here = ((row == i // 2) & (lane // WIN == i % 2)) | ((row == chunks) & (lane == i))
        reward = reward_of[i].astype(jnp.float32) / reward_unit
        group = group_of[i].astype(jnp.float32)
        reward_info = jnp.where(here, reward, reward_info)
        group_info = jnp.where(here, group, group_info)
        length_info = jnp.where(here, length_of[i], length_info)
        own = jnp.where(lane == 2 * SUBLANES + i, reward, own)
        own = jnp.where(lane == 3 * SUBLANES + i, group, own)
    mask8 = jnp.concatenate([mask_rows[...], mask_rows[...]], axis=0)
    live = jnp.where((row < chunks) & (mask8 > 0) & (lane % WIN < length_info), 1.0, 0.0)
    token_info[0] = live
    token_info[1] = reward_info
    token_info[2] = group_info
    own_info[...] = own + rollout_sums(live, SUBLANES)

    segments = width // LANES
    step_shape = (STEP, LANES)
    lane_value = lane_of(step_shape).astype(jnp.float32)
    lane_values = [lane_value + float(LANES * k) for k in range(segments)]
    pick_shape = (4 * chunks, 6 * LANES)
    pick_row, pick_lane = row_of(pick_shape), lane_of(pick_shape)
    pick_slot = pick_lane // LANES
    pick_kind = jnp.where(pick_slot < 2, pick_slot, pick_slot // 2 + 1)

    def find_peaks(c):
        for r in range(LANES * c, LANES * (c + 1), STEP):
            best = tiles[r : r + STEP, :LANES]
            for k in range(1, segments):
                best = jnp.maximum(best, tiles[r : r + STEP, LANES * k : LANES * (k + 1)])
            peak_rows[r : r + STEP, :] = jnp.broadcast_to(
                jnp.max(best.astype(jnp.float32), axis=1, keepdims=True), step_shape
            )

    def add_sums(c):
        lines = []
        for r in range(LANES * c, LANES * (c + 1), STEP):
            peak = peak_rows[r : r + STEP, :]
            column = columns[r : r + STEP, :]
            total = moment = picked = 0.0
            for k in range(segments):
                segment = tiles[r : r + STEP, LANES * k : LANES * (k + 1)].astype(jnp.float32)
                shifted = segment - peak
                weight = jnp.exp(shifted)
                product = weight * shifted
                total = weight if k == 0 else total + weight
                moment = product if k == 0 else moment + product
                picked = jnp.where(column == lane_values[k], segment, picked)
            total_high = total.astype(jnp.bfloat16)
            moment_high = moment.astype(jnp.bfloat16)
            lines.append(
                jnp.concatenate(
                    [
                        peak.astype(jnp.bfloat16),
                        picked.astype(jnp.bfloat16),
                        total_high,
                        (total - total_high.astype(jnp.float32)).astype(jnp.bfloat16),
                        moment_high,
                        (moment - moment_high.astype(jnp.float32)).astype(jnp.bfloat16),
                    ],
                    axis=1,
                )
            )
        pick = (pick_row == chunks * pick_kind + c) & ((pick_slot > 0) | (pick_lane == 0))
        return lines_to_lanes(
            jnp.where(pick, 1.0, 0.0).astype(jnp.bfloat16), jnp.concatenate(lines, axis=0)
        )

    logits_copy.wait()
    find_peaks(0)
    gathered = jnp.zeros((4 * chunks, LANES), jnp.float32)
    for c in range(chunks):
        if c + 1 < chunks:
            find_peaks(c + 1)
        gathered += add_sums(c)
    total = gathered[2 * chunks : 3 * chunks]
    log_total = jnp.log(total)
    log_sum = gathered[:chunks] + log_total
    entropy = log_total - gathered[3 * chunks :] / total
    picked = gathered[chunks : 2 * chunks]
    for n in range(send.shape[0]):
        send[n, 0] = log_sum
        send[n, 1] = entropy
        send[n, 2] = picked


def rollout_sums(values, start):
    shape = values.shape
    row, lane = row_of(shape), lane_of(shape)
    even = jnp.sum(jnp.where(lane < WIN, values, 0.0), axis=1, keepdims=True)
    odd = jnp.sum(jnp.where(lane >= WIN, values, 0.0), axis=1, keepdims=True)
    placed = (lane >= start) & (row == (lane - start) // 2)
    spread = jnp.where(placed, jnp.where(lane % 2 == 0, even, odd), 0.0)
    return jnp.broadcast_to(jnp.sum(spread, axis=0, keepdims=True), shape)


def merged(received):
    count = received.shape[0]
    joint = received[0, 0]
    picked = received[0, 2]
    for n in range(1, count):
        joint = jnp.maximum(joint, received[n, 0])
        picked += received[n, 2]
    total = jnp.zeros_like(joint)
    mixed = jnp.zeros_like(joint)
    for n in range(count):
        shift = received[n, 0] - joint
        factor = jnp.exp(shift)
        total += factor
        mixed += factor * (received[n, 1] - shift)
    log_total = jnp.log(total)
    return joint + log_total, mixed / total + log_total, picked


def merge_kernel(received, send):
    log_sum, entropy, picked = merged(received)
    for n in range(send.shape[0]):
        send[n, 0] = log_sum
        send[n, 1] = entropy
        send[n, 2] = picked


def token_kernel(received, token_info, own_info, send, token_values):
    log_sum, entropy, picked = merged(received)
    chunks = log_sum.shape[0]
    live = token_info[0][:chunks]
    logprob = live * (picked - log_sum)
    token_values[:chunks] = logprob
    token_values[chunks:] = live * entropy
    padded = jnp.concatenate([logprob, jnp.zeros_like(logprob)], axis=0)
    send[...] = own_info[...] + rollout_sums(padded, 0)


def final_kernel(
    received, token_info, token_values,
    advantage, token_weight, token_logprob, token_entropy, objective,
    advantage_row, weight_rows, objective_row, sems,
):
    chunks = token_weight.shape[0]
    copies = [
        pltpu.make_async_copy(token_values.at[pl.ds(0, chunks)], token_logprob, sems.at[0]),
        pltpu.make_async_copy(token_values.at[pl.ds(chunks, chunks)], token_entropy, sems.at[1]),
        pltpu.make_async_copy(weight_rows, token_weight, sems.at[2]),
        pltpu.make_async_copy(advantage_row, advantage, sems.at[3]),
        pltpu.make_async_copy(objective_row, objective, sems.at[4]),
    ]
    copies[0].start()
    copies[1].start()
    shape = (SUBLANES, LANES)
    row, lane = row_of(shape), lane_of(shape)
    valid = lane < SUBLANES * received.shape[0]
    shards = pltpu.roll(received[...], 0, 1, stride=SUBLANES, stride_axis=0)

    def field(f):
        shifted = pltpu.roll(shards, LANES - SUBLANES * f, 1) if f else shards
        return jnp.sum(
            jnp.where(lane // SUBLANES == row, shifted, 0.0), axis=0, keepdims=True
        )

    logprob_sums, counts, reward_values, groups = (field(f) for f in range(4))
    first = row < GROUPS
    member = (groups == (row % GROUPS).astype(jnp.float32)) & valid
    sums = jnp.sum(
        jnp.where(member, jnp.where(first, reward_values, counts), 0.0), axis=1, keepdims=True
    )
    group_mean = sums / GROUP

    def spread_over(chosen, values):
        return jnp.sum(jnp.where(member & chosen, values, 0.0), axis=0, keepdims=True)

    centred = reward_values - spread_over(first, group_mean)
    group_var = (
        jnp.sum(jnp.where(member & first, centred * centred, 0.0), axis=1, keepdims=True) / GROUP
    )
    group_spread = jnp.maximum(jnp.sqrt(group_var), spread_floor)

    info_reward, info_group = token_info[1], token_info[2]
    mean, spread, tokens = group_mean[0:1], group_spread[0:1], sums[GROUPS : GROUPS + 1]
    for g in range(1, GROUPS):
        chosen = info_group == float(g)
        mean = jnp.where(chosen, group_mean[g : g + 1], mean)
        spread = jnp.where(chosen, group_spread[g : g + 1], spread)
        tokens = jnp.where(chosen, sums[GROUPS + g : GROUPS + g + 1], tokens)
    info_advantage = (info_reward - mean) / spread
    weight = token_info[0] * (info_advantage * (GROUP * WIN / tokens))
    advantage_row[...] = info_advantage[chunks : chunks + 1, :SUBLANES]
    copies[3].start()
    weight_rows[...] = weight[:chunks]
    copies[2].start()

    spread_row = jnp.where(valid[:1], spread_over(first, group_spread), 1.0)
    tokens_row = jnp.where(valid[:1], spread_over(~first, sums), 1.0)
    weights = centred / spread_row * (GROUP * WIN / tokens_row)
    products = jnp.where(valid[:1], weights * logprob_sums, 0.0)
    total_rows = GROUPS * GROUP * WIN
    objective_row[...] = -jnp.sum(products, axis=1, keepdims=True) / total_rows
    copies[4].start()
    for copy in copies:
        copy.wait()


def shards(rewards, group_ids, lengths, token_mask, targets, logits):
    rows = logits.shape[0]
    chunks = rows // LANES
    f32, i32 = jnp.float32, jnp.int32
    any_spec = pl.BlockSpec(memory_space=pl.ANY)
    vmem = pl.BlockSpec(memory_space=pltpu.VMEM)

    def kept(*shape):
        return pltpu.VMEM(shape, f32)

    def near(array):
        return pltpu.with_memory_space_constraint(array, pltpu.VMEM)

    first_axes = ("mp_0", "mp_2")
    first_size = lax.axis_size("mp_0") * lax.axis_size("mp_2")
    sent, token_info, own_info = pl.pallas_call(
        local_kernel,
        name="local_stats",
        in_specs=[any_spec] * 6,
        out_specs=[vmem] * 3,
        out_shape=[
            kept(first_size, 3, chunks, LANES),
            kept(3, SUBLANES, LANES),
            kept(SUBLANES, LANES),
        ],
        scratch_shapes=[
            pltpu.VMEM(logits.shape, logits.dtype),
            pltpu.VMEM((chunks, LANES), i32),
            pltpu.VMEM((chunks, LANES), i32),
            pltpu.SMEM(rewards.shape, i32),
            pltpu.SMEM(rewards.shape, i32),
            pltpu.SMEM(rewards.shape, i32),
            pltpu.VMEM((rows, LANES), f32),
            pltpu.VMEM((rows, LANES), f32),
            pltpu.SemaphoreType.DMA((6,)),
        ],
    )(
        rewards,
        group_ids,
        lengths,
        token_mask.reshape(chunks, LANES),
        targets.reshape(chunks, LANES),
        logits,
    )
    received = lax.all_to_all(sent, first_axes, 0, 0, tiled=True)
    sent = pl.pallas_call(
        merge_kernel,
        name="merge_stats",
        in_specs=[vmem],
        out_specs=vmem,
        out_shape=kept(lax.axis_size("mp_1"), 3, chunks, LANES),
    )(near(received))
    received = lax.all_to_all(sent, "mp_1", 0, 0, tiled=True)
    shard_count = lax.axis_size("dp")
    sent, token_values = pl.pallas_call(
        token_kernel,
        name="token_values",
        in_specs=[vmem] * 3,
        out_specs=[vmem] * 2,
        out_shape=[kept(SUBLANES, LANES), kept(2 * chunks, LANES)],
    )(near(received), near(token_info), near(own_info))
    received = lax.all_to_all(sent.reshape(shard_count, 1, LANES), "dp", 0, 0, tiled=True)
    advantage, token_weight, token_logprob, token_entropy, objective = pl.pallas_call(
        final_kernel,
        name="group_values",
        in_specs=[vmem] * 3,
        out_specs=[any_spec] * 5,
        out_shape=[
            jax.ShapeDtypeStruct((1, SUBLANES), f32),
            jax.ShapeDtypeStruct((chunks, LANES), f32),
            jax.ShapeDtypeStruct((chunks, LANES), f32),
            jax.ShapeDtypeStruct((chunks, LANES), f32),
            jax.ShapeDtypeStruct((1, 1), f32),
        ],
        scratch_shapes=[
            pltpu.VMEM((1, SUBLANES), f32),
            pltpu.VMEM((chunks, LANES), f32),
            pltpu.VMEM((1, 1), f32),
            pltpu.SemaphoreType.DMA((5,)),
        ],
    )(near(received.reshape(shard_count, LANES)), near(token_info), near(token_values))
    return (
        advantage.reshape(-1),
        token_weight.reshape(-1),
        token_logprob.reshape(-1),
        token_entropy.reshape(-1),
        objective.reshape(()),
    )


def solution(mesh):
    split = Mesh(mesh.devices.reshape(mesh.shape["dp"], 8, 8, 2), ("dp", "mp_0", "mp_1", "mp_2"))
    in_specs = (P("dp"), P("dp"), P("dp"), P("dp"), P("dp"), P("dp", MP))
    out_specs = (P("dp"), P("dp"), P("dp"), P("dp"), P())
    return jax.shard_map(
        shards, mesh=split, in_specs=in_specs, out_specs=out_specs, check_vma=False
    )
```

```python
import jax
import jax.numpy as jnp
from jax import lax
from jax.experimental import pallas as pl
from jax.experimental.pallas import tpu as pltpu
from jax.sharding import Mesh
from jax.sharding import PartitionSpec as P

GROUP = 16
WIN = 64
LANES = 128
SUBLANES = 8
GROUPS = 4
STEP = 16
MP = ("mp_0", "mp_1", "mp_2")

spread_floor = 0.25
reward_unit = 1024.0


def lane_of(shape):
    return lax.broadcasted_iota(jnp.int32, shape, 1)


def row_of(shape):
    return lax.broadcasted_iota(jnp.int32, shape, 0)


def lines_to_lanes(pick, block):
    return lax.dot_general(
        pick, block, (((1,), (1,)), ((), ())), preferred_element_type=jnp.float32
    )


def local_kernel(
    rewards, group_ids, lengths, token_mask, targets, logits,
    send, token_info, own_info,
    tiles, target_rows, mask_rows, reward_of, group_of, length_of, peak_rows, columns, sems,
):
    chunks = logits.shape[0] // LANES
    width = logits.shape[1]
    targets_copy = pltpu.make_async_copy(targets, target_rows, sems.at[0])
    small = [
        pltpu.make_async_copy(token_mask, mask_rows, sems.at[1]),
        pltpu.make_async_copy(rewards, reward_of, sems.at[2]),
        pltpu.make_async_copy(group_ids, group_of, sems.at[3]),
        pltpu.make_async_copy(lengths, length_of, sems.at[4]),
    ]
    logits_copy = pltpu.make_async_copy(logits, tiles, sems.at[5])
    targets_copy.start()
    for copy in small:
        copy.start()
    logits_copy.start()
    shard = (
        lax.axis_index("mp_0") * lax.axis_size("mp_1") + lax.axis_index("mp_1")
    ) * lax.axis_size("mp_2") + lax.axis_index("mp_2")
    targets_copy.wait()

    block = (LANES, LANES)
    diagonal = row_of(block) == lane_of(block)
    digit_row = row_of((2 * LANES, LANES))
    digits = jnp.where(digit_row < LANES, 1.0, float(LANES)).astype(jnp.bfloat16)
    local = target_rows[...] - shard * width
    inside = (local >= 0) & (local < width)
    low_digit = jnp.where(inside, local % LANES, -1).astype(jnp.float32)
    high_digit = jnp.where(inside, local // LANES, 0).astype(jnp.float32)
    for c in range(chunks):
        spread = jnp.concatenate(
            [
                jnp.where(diagonal, low_digit[c : c + 1], 0.0),
                jnp.where(diagonal, high_digit[c : c + 1], 0.0),
            ],
            axis=1,
        ).astype(jnp.bfloat16)
        columns[LANES * c : LANES * (c + 1), :] = jnp.dot(
            spread, digits, preferred_element_type=jnp.float32
        )

    for copy in small:
        copy.wait()
    shape = (SUBLANES, LANES)
    row, lane = row_of(shape), lane_of(shape)
    reward_info = jnp.zeros(shape, jnp.float32)
    group_info = jnp.zeros(shape, jnp.float32)
    length_info = jnp.zeros(shape, jnp.int32)
    own_reward = jnp.zeros(shape, jnp.float32)
    own_group = jnp.zeros(shape, jnp.int32)
    for i in range(2 * chunks):
        here = ((row == i // 2) & (lane // WIN == i % 2)) | ((row == chunks) & (lane == i))
        reward = reward_of[i].astype(jnp.float32) / reward_unit
        reward_info = jnp.where(here, reward, reward_info)
        group_info = jnp.where(here, group_of[i].astype(jnp.float32), group_info)
        length_info = jnp.where(here, length_of[i], length_info)
        own_reward = jnp.where(lane % SUBLANES == i, reward, own_reward)
        own_group = jnp.where(lane % SUBLANES == i, group_of[i], own_group)
    mask8 = jnp.concatenate([mask_rows[...], mask_rows[...]], axis=0)
    live = jnp.where((row < chunks) & (mask8 > 0) & (lane % WIN < length_info), 1.0, 0.0)
    token_info[0] = live
    token_info[1] = reward_info
    token_info[2] = group_info
    slot = lane // SUBLANES
    field = slot // GROUPS
    values = jnp.where(
        field == 0, own_reward, jnp.where(field == 1, rollout_sums(live), 1.0)
    )
    mine = own_group == slot % GROUPS
    own_info[0] = jnp.where(mine & (field != 2), values, 0.0)
    own_info[1] = jnp.where(mine & (field == 2), 1.0, 0.0)

    segments = width // LANES
    step_shape = (STEP, LANES)
    lane_value = lane_of(step_shape).astype(jnp.float32)
    lane_values = [lane_value + float(LANES * k) for k in range(segments)]
    pick_shape = (4 * chunks, 6 * LANES)
    pick_row, pick_lane = row_of(pick_shape), lane_of(pick_shape)
    pick_slot = pick_lane // LANES
    pick_kind = jnp.where(pick_slot < 2, pick_slot, pick_slot // 2 + 1)

    def find_peaks(c):
        for r in range(LANES * c, LANES * (c + 1), STEP):
            best = tiles[r : r + STEP, :LANES]
            for k in range(1, segments):
                best = jnp.maximum(best, tiles[r : r + STEP, LANES * k : LANES * (k + 1)])
            peak_rows[r : r + STEP, :] = jnp.broadcast_to(
                jnp.max(best.astype(jnp.float32), axis=1, keepdims=True), step_shape
            )

    def add_sums(c):
        lines = []
        for r in range(LANES * c, LANES * (c + 1), STEP):
            peak = peak_rows[r : r + STEP, :]
            column = columns[r : r + STEP, :]
            total = moment = picked = 0.0
            for k in range(segments):
                segment = tiles[r : r + STEP, LANES * k : LANES * (k + 1)].astype(jnp.float32)
                shifted = segment - peak
                weight = jnp.exp(shifted)
                product = weight * shifted
                total = weight if k == 0 else total + weight
                moment = product if k == 0 else moment + product
                picked = jnp.where(column == lane_values[k], segment, picked)
            total_high = total.astype(jnp.bfloat16)
            moment_high = moment.astype(jnp.bfloat16)
            lines.append(
                jnp.concatenate(
                    [
                        peak.astype(jnp.bfloat16),
                        picked.astype(jnp.bfloat16),
                        total_high,
                        (total - total_high.astype(jnp.float32)).astype(jnp.bfloat16),
                        moment_high,
                        (moment - moment_high.astype(jnp.float32)).astype(jnp.bfloat16),
                    ],
                    axis=1,
                )
            )
        pick = (pick_row == chunks * pick_kind + c) & ((pick_slot > 0) | (pick_lane == 0))
        return lines_to_lanes(
            jnp.where(pick, 1.0, 0.0).astype(jnp.bfloat16), jnp.concatenate(lines, axis=0)
        )

    logits_copy.wait()
    find_peaks(0)
    gathered = jnp.zeros((4 * chunks, LANES), jnp.float32)
    for c in range(chunks):
        if c + 1 < chunks:
            find_peaks(c + 1)
        gathered += add_sums(c)
    total = gathered[2 * chunks : 3 * chunks]
    log_total = jnp.log(total)
    log_sum = gathered[:chunks] + log_total
    entropy = log_total - gathered[3 * chunks :] / total
    picked = gathered[chunks : 2 * chunks]
    for n in range(send.shape[0]):
        send[n, 0] = log_sum
        send[n, 1] = entropy
        send[n, 2] = picked


def rollout_sums(values):
    shape = values.shape
    row, lane = row_of(shape), lane_of(shape)
    even = jnp.sum(jnp.where(lane < WIN, values, 0.0), axis=1, keepdims=True)
    odd = jnp.sum(jnp.where(lane >= WIN, values, 0.0), axis=1, keepdims=True)
    spread = jnp.where(
        row == lane % SUBLANES // 2, jnp.where(lane % 2 == 0, even, odd), 0.0
    )
    return jnp.broadcast_to(jnp.sum(spread, axis=0, keepdims=True), shape)


def merged(received):
    count = received.shape[0]
    joint = received[0, 0]
    picked = received[0, 2]
    for n in range(1, count):
        joint = jnp.maximum(joint, received[n, 0])
        picked += received[n, 2]
    total = jnp.zeros_like(joint)
    mixed = jnp.zeros_like(joint)
    for n in range(count):
        shift = received[n, 0] - joint
        factor = jnp.exp(shift)
        total += factor
        mixed += factor * (received[n, 1] - shift)
    log_total = jnp.log(total)
    return joint + log_total, mixed / total + log_total, picked


def merge_kernel(received, send):
    log_sum, entropy, picked = merged(received)
    for n in range(send.shape[0]):
        send[n, 0] = log_sum
        send[n, 1] = entropy
        send[n, 2] = picked


def token_kernel(received, token_info, own_info, send, token_values):
    log_sum, entropy, picked = merged(received)
    chunks = log_sum.shape[0]
    live = token_info[0][:chunks]
    logprob = live * (picked - log_sum)
    token_values[:chunks] = logprob
    token_values[chunks:] = live * entropy
    padded = jnp.concatenate([logprob, jnp.zeros_like(logprob)], axis=0)
    send[...] = own_info[0] + own_info[1] * rollout_sums(padded)


def final_kernel(
    received, token_info, token_values,
    advantage, token_weight, token_logprob, token_entropy, objective,
    advantage_row, weight_rows, objective_row, sems,
):
    chunks = token_weight.shape[0]
    copies = [
        pltpu.make_async_copy(token_values.at[pl.ds(0, chunks)], token_logprob, sems.at[0]),
        pltpu.make_async_copy(token_values.at[pl.ds(chunks, chunks)], token_entropy, sems.at[1]),
        pltpu.make_async_copy(weight_rows, token_weight, sems.at[2]),
        pltpu.make_async_copy(advantage_row, advantage, sems.at[3]),
        pltpu.make_async_copy(objective_row, objective, sems.at[4]),
    ]
    copies[0].start()
    copies[1].start()
    shape = (SUBLANES, LANES)
    row, lane = row_of(shape), lane_of(shape)
    slot = lane // SUBLANES
    first = row < GROUPS
    own_slot = slot == row
    rewards = received[...]
    logprob_sums = pltpu.roll(rewards, LANES // 2, 1)
    member = pltpu.roll(rewards, LANES // 4, 1)

    def row_sums(upper, lower):
        upper = jnp.sum(upper, axis=0, keepdims=True)
        lower = jnp.sum(lower, axis=0, keepdims=True)
        chosen = jnp.where(
            first, jnp.where(own_slot, upper, 0.0), jnp.where(slot == row - GROUPS, lower, 0.0)
        )
        return jnp.sum(chosen, axis=1, keepdims=True)

    total = jnp.sum(rewards, axis=0, keepdims=True)
    sums = jnp.sum(jnp.where(own_slot, total, 0.0), axis=1, keepdims=True)
    group_mean = sums / GROUP
    mean_row = jnp.sum(jnp.where(own_slot & first, group_mean, 0.0), axis=0, keepdims=True)
    centred = rewards - member * mean_row
    spreads = row_sums(centred * centred, centred * logprob_sums)
    group_spread = jnp.maximum(jnp.sqrt(spreads / GROUP), spread_floor)
    info_reward, info_group = token_info[1], token_info[2]
    mean, spread, tokens = group_mean[0:1], group_spread[0:1], sums[GROUPS : GROUPS + 1]
    terms = spreads[GROUPS : GROUPS + 1] * (GROUP * WIN / tokens) / spread
    for g in range(1, GROUPS):
        chosen = info_group == float(g)
        one_tokens = sums[GROUPS + g : GROUPS + g + 1]
        one_spread = group_spread[g : g + 1]
        terms += spreads[GROUPS + g : GROUPS + g + 1] * (GROUP * WIN / one_tokens) / one_spread
        mean = jnp.where(chosen, group_mean[g : g + 1], mean)
        spread = jnp.where(chosen, one_spread, spread)
        tokens = jnp.where(chosen, one_tokens, tokens)
    total_rows = GROUPS * GROUP * WIN
    objective_row[...] = -terms / total_rows
    copies[4].start()
    info_advantage = (info_reward - mean) / spread
    weight = token_info[0] * (info_advantage * (GROUP * WIN / tokens))
    advantage_row[...] = info_advantage[chunks : chunks + 1, :SUBLANES]
    copies[3].start()
    weight_rows[...] = weight[:chunks]
    copies[2].start()
    for copy in copies:
        copy.wait()


def shards(rewards, group_ids, lengths, token_mask, targets, logits):
    rows = logits.shape[0]
    chunks = rows // LANES
    f32, i32 = jnp.float32, jnp.int32
    any_spec = pl.BlockSpec(memory_space=pl.ANY)
    vmem = pl.BlockSpec(memory_space=pltpu.VMEM)

    def kept(*shape):
        return pltpu.VMEM(shape, f32)

    def near(array):
        return pltpu.with_memory_space_constraint(array, pltpu.VMEM)

    first_axes = ("mp_1", "mp_2")
    first_size = lax.axis_size("mp_1") * lax.axis_size("mp_2")
    sent, token_info, own_info = pl.pallas_call(
        local_kernel,
        name="local_stats",
        in_specs=[any_spec] * 6,
        out_specs=[vmem] * 3,
        out_shape=[
            kept(first_size, 3, chunks, LANES),
            kept(3, SUBLANES, LANES),
            kept(2, SUBLANES, LANES),
        ],
        scratch_shapes=[
            pltpu.VMEM(logits.shape, logits.dtype),
            pltpu.VMEM((chunks, LANES), i32),
            pltpu.VMEM((chunks, LANES), i32),
            pltpu.SMEM(rewards.shape, i32),
            pltpu.SMEM(rewards.shape, i32),
            pltpu.SMEM(rewards.shape, i32),
            pltpu.VMEM((rows, LANES), f32),
            pltpu.VMEM((rows, LANES), f32),
            pltpu.SemaphoreType.DMA((6,)),
        ],
    )(
        rewards,
        group_ids,
        lengths,
        token_mask.reshape(chunks, LANES),
        targets.reshape(chunks, LANES),
        logits,
    )
    received = lax.all_to_all(sent, first_axes, 0, 0, tiled=True)
    sent = pl.pallas_call(
        merge_kernel,
        name="merge_stats",
        in_specs=[vmem],
        out_specs=vmem,
        out_shape=kept(lax.axis_size("mp_0"), 3, chunks, LANES),
    )(near(received))
    received = lax.all_to_all(sent, "mp_0", 0, 0, tiled=True)
    shard_count = lax.axis_size("dp")
    sent, token_values = pl.pallas_call(
        token_kernel,
        name="token_values",
        in_specs=[vmem] * 3,
        out_specs=[vmem] * 2,
        out_shape=[kept(SUBLANES, LANES), kept(2 * chunks, LANES)],
    )(near(received), near(token_info), near(own_info))
    received = lax.all_to_all(sent.reshape(shard_count, 1, LANES), "dp", 0, 0, tiled=True)
    advantage, token_weight, token_logprob, token_entropy, objective = pl.pallas_call(
        final_kernel,
        name="group_values",
        in_specs=[vmem] * 3,
        out_specs=[any_spec] * 5,
        out_shape=[
            jax.ShapeDtypeStruct((1, SUBLANES), f32),
            jax.ShapeDtypeStruct((chunks, LANES), f32),
            jax.ShapeDtypeStruct((chunks, LANES), f32),
            jax.ShapeDtypeStruct((chunks, LANES), f32),
            jax.ShapeDtypeStruct((1, 1), f32),
        ],
        scratch_shapes=[
            pltpu.VMEM((1, SUBLANES), f32),
            pltpu.VMEM((chunks, LANES), f32),
            pltpu.VMEM((1, 1), f32),
            pltpu.SemaphoreType.DMA((5,)),
        ],
    )(near(received.reshape(shard_count, LANES)), near(token_info), near(token_values))
    return (
        advantage.reshape(-1),
        token_weight.reshape(-1),
        token_logprob.reshape(-1),
        token_entropy.reshape(-1),
        objective.reshape(()),
    )


def solution(mesh):
    split = Mesh(mesh.devices.reshape(mesh.shape["dp"], 8, 8, 2), ("dp", "mp_0", "mp_1", "mp_2"))
    in_specs = (P("dp"), P("dp"), P("dp"), P("dp"), P("dp"), P("dp", MP))
    out_specs = (P("dp"), P("dp"), P("dp"), P("dp"), P())
    return jax.shard_map(
        shards, mesh=split, in_specs=in_specs, out_specs=out_specs, check_vma=False
    )
```

```python
import jax
import jax.numpy as jnp
from jax import lax
from jax.experimental import pallas as pl
from jax.experimental.pallas import tpu as pltpu
from jax.sharding import Mesh
from jax.sharding import PartitionSpec as P

GROUP = 16
WIN = 64
LANES = 128
SUBLANES = 8
GROUPS = 4
STEP = 16
MP = ("mp_0", "mp_1", "mp_2")

spread_floor = 0.25
reward_unit = 1024.0


def lane_of(shape):
    return lax.broadcasted_iota(jnp.int32, shape, 1)


def row_of(shape):
    return lax.broadcasted_iota(jnp.int32, shape, 0)


def lines_to_lanes(pick, block):
    return lax.dot_general(
        pick, block, (((1,), (1,)), ((), ())), preferred_element_type=jnp.float32
    )


def local_kernel(
    rewards, group_ids, lengths, token_mask, targets, logits,
    send, token_info, own_info,
    tiles, target_rows, mask_rows, reward_of, group_of, length_of, peak_rows, columns, sems,
):
    chunks = logits.shape[0] // LANES
    width = logits.shape[1]
    targets_copy = pltpu.make_async_copy(targets, target_rows, sems.at[0])
    small = [
        pltpu.make_async_copy(token_mask, mask_rows, sems.at[1]),
        pltpu.make_async_copy(rewards, reward_of, sems.at[2]),
        pltpu.make_async_copy(group_ids, group_of, sems.at[3]),
        pltpu.make_async_copy(lengths, length_of, sems.at[4]),
    ]
    logits_copy = pltpu.make_async_copy(logits, tiles, sems.at[5])
    targets_copy.start()
    for copy in small:
        copy.start()
    logits_copy.start()
    shard = (
        lax.axis_index("mp_0") * lax.axis_size("mp_1") + lax.axis_index("mp_1")
    ) * lax.axis_size("mp_2") + lax.axis_index("mp_2")
    targets_copy.wait()

    block = (LANES, LANES)
    diagonal = row_of(block) == lane_of(block)
    digit_row = row_of((2 * LANES, LANES))
    digits = jnp.where(digit_row < LANES, 1.0, float(LANES)).astype(jnp.bfloat16)
    local = target_rows[...] - shard * width
    inside = (local >= 0) & (local < width)
    low_digit = jnp.where(inside, local % LANES, -1).astype(jnp.float32)
    high_digit = jnp.where(inside, local // LANES, 0).astype(jnp.float32)
    for c in range(chunks):
        spread = jnp.concatenate(
            [
                jnp.where(diagonal, low_digit[c : c + 1], 0.0),
                jnp.where(diagonal, high_digit[c : c + 1], 0.0),
            ],
            axis=1,
        ).astype(jnp.bfloat16)
        columns[LANES * c : LANES * (c + 1), :] = jnp.dot(
            spread, digits, preferred_element_type=jnp.float32
        )

    for copy in small:
        copy.wait()
    shape = (SUBLANES, LANES)
    row, lane = row_of(shape), lane_of(shape)
    reward_info = jnp.zeros(shape, jnp.float32)
    group_info = jnp.zeros(shape, jnp.float32)
    length_info = jnp.zeros(shape, jnp.int32)
    own_reward = jnp.zeros(shape, jnp.float32)
    own_group = jnp.zeros(shape, jnp.int32)
    for i in range(2 * chunks):
        here = ((row == i // 2) & (lane // WIN == i % 2)) | ((row == chunks) & (lane == i))
        reward = reward_of[i].astype(jnp.float32) / reward_unit
        reward_info = jnp.where(here, reward, reward_info)
        group_info = jnp.where(here, group_of[i].astype(jnp.float32), group_info)
        length_info = jnp.where(here, length_of[i], length_info)
        own_reward = jnp.where(lane % SUBLANES == i, reward, own_reward)
        own_group = jnp.where(lane % SUBLANES == i, group_of[i], own_group)
    mask8 = jnp.concatenate([mask_rows[...], mask_rows[...]], axis=0)
    live = jnp.where((row < chunks) & (mask8 > 0) & (lane % WIN < length_info), 1.0, 0.0)
    token_info[0] = live
    token_info[1] = reward_info
    token_info[2] = group_info
    slot = lane // SUBLANES
    field = slot // GROUPS
    values = jnp.where(
        field == 0, own_reward, jnp.where(field == 1, rollout_sums(live), 1.0)
    )
    mine = own_group == slot % GROUPS
    own_info[0] = jnp.where(mine & (field != 2), values, 0.0)
    own_info[1] = jnp.where(mine & (field == 2), 1.0, 0.0)

    segments = width // LANES
    step_shape = (STEP, LANES)
    lane_value = lane_of(step_shape).astype(jnp.float32)
    lane_values = [lane_value + float(LANES * k) for k in range(segments)]
    pick_shape = (4 * chunks, 6 * LANES)
    pick_row, pick_lane = row_of(pick_shape), lane_of(pick_shape)
    pick_slot = pick_lane // LANES
    pick_kind = jnp.where(pick_slot < 2, pick_slot, pick_slot // 2 + 1)

    def find_peaks(c):
        for r in range(LANES * c, LANES * (c + 1), STEP):
            best = tiles[r : r + STEP, :LANES]
            for k in range(1, segments):
                best = jnp.maximum(best, tiles[r : r + STEP, LANES * k : LANES * (k + 1)])
            peak_rows[r : r + STEP, :] = jnp.broadcast_to(
                jnp.max(best.astype(jnp.float32), axis=1, keepdims=True), step_shape
            )

    def add_sums(c):
        lines = []
        for r in range(LANES * c, LANES * (c + 1), STEP):
            peak = peak_rows[r : r + STEP, :]
            column = columns[r : r + STEP, :]
            total = moment = picked = 0.0
            for k in range(segments):
                segment = tiles[r : r + STEP, LANES * k : LANES * (k + 1)].astype(jnp.float32)
                shifted = segment - peak
                weight = jnp.exp(shifted)
                product = weight * shifted
                total = weight if k == 0 else total + weight
                moment = product if k == 0 else moment + product
                picked = jnp.where(column == lane_values[k], segment, picked)
            total_high = total.astype(jnp.bfloat16)
            moment_high = moment.astype(jnp.bfloat16)
            lines.append(
                jnp.concatenate(
                    [
                        peak.astype(jnp.bfloat16),
                        picked.astype(jnp.bfloat16),
                        total_high,
                        (total - total_high.astype(jnp.float32)).astype(jnp.bfloat16),
                        moment_high,
                        (moment - moment_high.astype(jnp.float32)).astype(jnp.bfloat16),
                    ],
                    axis=1,
                )
            )
        pick = (pick_row == chunks * pick_kind + c) & ((pick_slot > 0) | (pick_lane == 0))
        return lines_to_lanes(
            jnp.where(pick, 1.0, 0.0).astype(jnp.bfloat16), jnp.concatenate(lines, axis=0)
        )

    logits_copy.wait()
    find_peaks(0)
    gathered = jnp.zeros((4 * chunks, LANES), jnp.float32)
    for c in range(chunks):
        if c + 1 < chunks:
            find_peaks(c + 1)
        gathered += add_sums(c)
    total = gathered[2 * chunks : 3 * chunks]
    log_total = jnp.log(total)
    log_sum = gathered[:chunks] + log_total
    entropy = log_total - gathered[3 * chunks :] / total
    picked = gathered[chunks : 2 * chunks]
    for n in range(send.shape[0]):
        send[n, 0] = log_sum
        send[n, 1] = entropy
        send[n, 2] = picked


def rollout_sums(values):
    shape = values.shape
    row, lane = row_of(shape), lane_of(shape)
    even = jnp.sum(jnp.where(lane < WIN, values, 0.0), axis=1, keepdims=True)
    odd = jnp.sum(jnp.where(lane >= WIN, values, 0.0), axis=1, keepdims=True)
    spread = jnp.where(
        row == lane % SUBLANES // 2, jnp.where(lane % 2 == 0, even, odd), 0.0
    )
    return jnp.broadcast_to(jnp.sum(spread, axis=0, keepdims=True), shape)


def merged(received):
    count = received.shape[0]
    joint = received[0, 0]
    picked = received[0, 2]
    for n in range(1, count):
        joint = jnp.maximum(joint, received[n, 0])
        picked += received[n, 2]
    total = jnp.zeros_like(joint)
    mixed = jnp.zeros_like(joint)
    for n in range(count):
        shift = received[n, 0] - joint
        factor = jnp.exp(shift)
        total += factor
        mixed += factor * (received[n, 1] - shift)
    log_total = jnp.log(total)
    return joint + log_total, mixed / total + log_total, picked


def merge_kernel(received, send):
    log_sum, entropy, picked = merged(received)
    for n in range(send.shape[0]):
        send[n, 0] = log_sum
        send[n, 1] = entropy
        send[n, 2] = picked


def token_kernel(received, token_info, own_info, send, token_values):
    log_sum, entropy, picked = merged(received)
    chunks = log_sum.shape[0]
    live = token_info[0][:chunks]
    logprob = live * (picked - log_sum)
    token_values[:chunks] = logprob
    token_values[chunks:] = live * entropy
    padded = jnp.concatenate([logprob, jnp.zeros_like(logprob)], axis=0)
    send[...] = own_info[0] + own_info[1] * rollout_sums(padded)


def final_kernel(
    received, token_info, token_values,
    advantage, token_weight, token_logprob, token_entropy, objective,
    advantage_row, weight_rows, objective_row, sems,
):
    chunks = token_weight.shape[0]
    copies = [
        pltpu.make_async_copy(token_values.at[pl.ds(0, chunks)], token_logprob, sems.at[0]),
        pltpu.make_async_copy(token_values.at[pl.ds(chunks, chunks)], token_entropy, sems.at[1]),
        pltpu.make_async_copy(weight_rows, token_weight, sems.at[2]),
        pltpu.make_async_copy(advantage_row, advantage, sems.at[3]),
        pltpu.make_async_copy(objective_row, objective, sems.at[4]),
    ]
    copies[0].start()
    copies[1].start()
    shape = (SUBLANES, LANES)
    row, lane = row_of(shape), lane_of(shape)
    slot = lane // SUBLANES
    first = row < GROUPS
    own_slot = slot == row
    rewards = received[...]
    logprob_sums = pltpu.roll(rewards, LANES // 2, 1)
    member = pltpu.roll(rewards, LANES // 4, 1)

    def row_sums(upper, lower):
        upper = jnp.sum(upper, axis=0, keepdims=True)
        lower = jnp.sum(lower, axis=0, keepdims=True)
        chosen = jnp.where(
            first, jnp.where(own_slot, upper, 0.0), jnp.where(slot == row - GROUPS, lower, 0.0)
        )
        return jnp.sum(chosen, axis=1, keepdims=True)

    total = jnp.sum(rewards, axis=0, keepdims=True)
    sums = jnp.sum(jnp.where(own_slot, total, 0.0), axis=1, keepdims=True)
    group_mean = sums / GROUP
    mean_row = jnp.sum(jnp.where(own_slot & first, group_mean, 0.0), axis=0, keepdims=True)
    centred = rewards - member * mean_row
    spreads = row_sums(centred * centred, centred * logprob_sums)
    group_spread = jnp.maximum(jnp.sqrt(spreads / GROUP), spread_floor)
    info_reward, info_group = token_info[1], token_info[2]
    mean, spread, tokens = group_mean[0:1], group_spread[0:1], sums[GROUPS : GROUPS + 1]
    terms = spreads[GROUPS : GROUPS + 1] * (GROUP * WIN / tokens) / spread
    for g in range(1, GROUPS):
        chosen = info_group == float(g)
        one_tokens = sums[GROUPS + g : GROUPS + g + 1]
        one_spread = group_spread[g : g + 1]
        terms += spreads[GROUPS + g : GROUPS + g + 1] * (GROUP * WIN / one_tokens) / one_spread
        mean = jnp.where(chosen, group_mean[g : g + 1], mean)
        spread = jnp.where(chosen, one_spread, spread)
        tokens = jnp.where(chosen, one_tokens, tokens)
    total_rows = GROUPS * GROUP * WIN
    objective_row[...] = -terms / total_rows
    copies[4].start()
    info_advantage = (info_reward - mean) / spread
    weight = token_info[0] * (info_advantage * (GROUP * WIN / tokens))
    advantage_row[...] = info_advantage[chunks : chunks + 1, :SUBLANES]
    copies[3].start()
    weight_rows[...] = weight[:chunks]
    copies[2].start()
    for copy in copies:
        copy.wait()


def shards(rewards, group_ids, lengths, token_mask, targets, logits):
    rows = logits.shape[0]
    chunks = rows // LANES
    f32, i32 = jnp.float32, jnp.int32
    any_spec = pl.BlockSpec(memory_space=pl.ANY)
    vmem = pl.BlockSpec(memory_space=pltpu.VMEM)

    def kept(*shape):
        return pltpu.VMEM(shape, f32)

    def near(array):
        return pltpu.with_memory_space_constraint(array, pltpu.VMEM)

    first_axes = ("mp_2", "mp_0")
    first_size = lax.axis_size("mp_2") * lax.axis_size("mp_0")
    sent, token_info, own_info = pl.pallas_call(
        local_kernel,
        name="local_stats",
        in_specs=[any_spec] * 6,
        out_specs=[vmem] * 3,
        out_shape=[
            kept(first_size, 3, chunks, LANES),
            kept(3, SUBLANES, LANES),
            kept(2, SUBLANES, LANES),
        ],
        scratch_shapes=[
            pltpu.VMEM(logits.shape, logits.dtype),
            pltpu.VMEM((chunks, LANES), i32),
            pltpu.VMEM((chunks, LANES), i32),
            pltpu.SMEM(rewards.shape, i32),
            pltpu.SMEM(rewards.shape, i32),
            pltpu.SMEM(rewards.shape, i32),
            pltpu.VMEM((rows, LANES), f32),
            pltpu.VMEM((rows, LANES), f32),
            pltpu.SemaphoreType.DMA((6,)),
        ],
    )(
        rewards,
        group_ids,
        lengths,
        token_mask.reshape(chunks, LANES),
        targets.reshape(chunks, LANES),
        logits,
    )
    received = lax.all_to_all(sent, first_axes, 0, 0, tiled=True)
    sent = pl.pallas_call(
        merge_kernel,
        name="merge_stats",
        in_specs=[vmem],
        out_specs=vmem,
        out_shape=kept(lax.axis_size("mp_1"), 3, chunks, LANES),
    )(near(received))
    received = lax.all_to_all(sent, "mp_1", 0, 0, tiled=True)
    shard_count = lax.axis_size("dp")
    sent, token_values = pl.pallas_call(
        token_kernel,
        name="token_values",
        in_specs=[vmem] * 3,
        out_specs=[vmem] * 2,
        out_shape=[kept(SUBLANES, LANES), kept(2 * chunks, LANES)],
    )(near(received), near(token_info), near(own_info))
    received = lax.all_to_all(sent.reshape(shard_count, 1, LANES), "dp", 0, 0, tiled=True)
    advantage, token_weight, token_logprob, token_entropy, objective = pl.pallas_call(
        final_kernel,
        name="group_values",
        in_specs=[vmem] * 3,
        out_specs=[any_spec] * 5,
        out_shape=[
            jax.ShapeDtypeStruct((1, SUBLANES), f32),
            jax.ShapeDtypeStruct((chunks, LANES), f32),
            jax.ShapeDtypeStruct((chunks, LANES), f32),
            jax.ShapeDtypeStruct((chunks, LANES), f32),
            jax.ShapeDtypeStruct((1, 1), f32),
        ],
        scratch_shapes=[
            pltpu.VMEM((1, SUBLANES), f32),
            pltpu.VMEM((chunks, LANES), f32),
            pltpu.VMEM((1, 1), f32),
            pltpu.SemaphoreType.DMA((5,)),
        ],
    )(near(received.reshape(shard_count, LANES)), near(token_info), near(token_values))
    return (
        advantage.reshape(-1),
        token_weight.reshape(-1),
        token_logprob.reshape(-1),
        token_entropy.reshape(-1),
        objective.reshape(()),
    )


def solution(mesh):
    split = Mesh(mesh.devices.reshape(mesh.shape["dp"], 8, 8, 2), ("dp", "mp_0", "mp_1", "mp_2"))
    in_specs = (P("dp"), P("dp"), P("dp"), P("dp"), P("dp"), P("dp", MP))
    out_specs = (P("dp"), P("dp"), P("dp"), P("dp"), P())
    return jax.shard_map(
        shards, mesh=split, in_specs=in_specs, out_specs=out_specs, check_vma=False
    )
```

```python
import jax
import jax.numpy as jnp
from jax import lax
from jax.experimental import pallas as pl
from jax.experimental.pallas import tpu as pltpu
from jax.sharding import Mesh
from jax.sharding import PartitionSpec as P

GROUP = 16
WIN = 64
LANES = 128
SUBLANES = 8
GROUPS = 4
STEP = 16
X_AXES = ("x2", "x1", "x0")
Z_AXES = ("z2", "z1", "z0")
Y_AXES = ("y2", "y1", "y0")
MP = Z_AXES + Y_AXES + ("core",)
FIRST = ("z0", "z1", "z2", "core")
SECOND = ("y0", "y1", "y2")
THIRD = ("x0", "x1", "x2")

spread_floor = 0.25
reward_unit = 1024.0


def lane_of(shape):
    return lax.broadcasted_iota(jnp.int32, shape, 1)


def row_of(shape):
    return lax.broadcasted_iota(jnp.int32, shape, 0)


def lines_to_lanes(pick, block):
    return lax.dot_general(
        pick, block, (((1,), (1,)), ((), ())), preferred_element_type=jnp.float32
    )


def local_kernel(
    rewards, group_ids, lengths, token_mask, targets, logits,
    send, token_info, own_info,
    tiles, target_rows, mask_rows, reward_of, group_of, length_of, peak_rows, columns, sems,
):
    chunks = logits.shape[0] // LANES
    width = logits.shape[1]
    targets_copy = pltpu.make_async_copy(targets, target_rows, sems.at[0])
    small = [
        pltpu.make_async_copy(token_mask, mask_rows, sems.at[1]),
        pltpu.make_async_copy(rewards, reward_of, sems.at[2]),
        pltpu.make_async_copy(group_ids, group_of, sems.at[3]),
        pltpu.make_async_copy(lengths, length_of, sems.at[4]),
    ]
    logits_copy = pltpu.make_async_copy(logits, tiles, sems.at[5])
    targets_copy.start()
    for copy in small:
        copy.start()
    logits_copy.start()
    shard = 0
    for name in MP:
        shard = shard * 2 + lax.axis_index(name)
    targets_copy.wait()

    block = (LANES, LANES)
    diagonal = row_of(block) == lane_of(block)
    digit_row = row_of((2 * LANES, LANES))
    digits = jnp.where(digit_row < LANES, 1.0, float(LANES)).astype(jnp.bfloat16)
    local = target_rows[...] - shard * width
    inside = (local >= 0) & (local < width)
    low_digit = jnp.where(inside, local % LANES, -1).astype(jnp.float32)
    high_digit = jnp.where(inside, local // LANES, 0).astype(jnp.float32)
    for c in range(chunks):
        spread = jnp.concatenate(
            [
                jnp.where(diagonal, low_digit[c : c + 1], 0.0),
                jnp.where(diagonal, high_digit[c : c + 1], 0.0),
            ],
            axis=1,
        ).astype(jnp.bfloat16)
        columns[LANES * c : LANES * (c + 1), :] = jnp.dot(
            spread, digits, preferred_element_type=jnp.float32
        )

    for copy in small:
        copy.wait()
    shape = (SUBLANES, LANES)
    row, lane = row_of(shape), lane_of(shape)
    reward_info = jnp.zeros(shape, jnp.float32)
    group_info = jnp.zeros(shape, jnp.float32)
    length_info = jnp.zeros(shape, jnp.int32)
    own_reward = jnp.zeros(shape, jnp.float32)
    own_group = jnp.zeros(shape, jnp.int32)
    for i in range(2 * chunks):
        here = ((row == i // 2) & (lane // WIN == i % 2)) | ((row == chunks) & (lane == i))
        reward = reward_of[i].astype(jnp.float32) / reward_unit
        reward_info = jnp.where(here, reward, reward_info)
        group_info = jnp.where(here, group_of[i].astype(jnp.float32), group_info)
        length_info = jnp.where(here, length_of[i], length_info)
        own_reward = jnp.where(lane % SUBLANES == i, reward, own_reward)
        own_group = jnp.where(lane % SUBLANES == i, group_of[i], own_group)
    mask8 = jnp.concatenate([mask_rows[...], mask_rows[...]], axis=0)
    live = jnp.where((row < chunks) & (mask8 > 0) & (lane % WIN < length_info), 1.0, 0.0)
    token_info[0] = live
    token_info[1] = reward_info
    token_info[2] = group_info
    slot = lane // SUBLANES
    field = slot // GROUPS
    values = jnp.where(
        field == 0, own_reward, jnp.where(field == 1, rollout_sums(live), 1.0)
    )
    mine = own_group == slot % GROUPS
    own_info[0] = jnp.where(mine & (field != 2), values, 0.0)
    own_info[1] = jnp.where(mine & (field == 2), 1.0, 0.0)

    segments = width // LANES
    step_shape = (STEP, LANES)
    lane_value = lane_of(step_shape).astype(jnp.float32)
    lane_values = [lane_value + float(LANES * k) for k in range(segments)]
    pick_shape = (4 * chunks, 6 * LANES)
    pick_row, pick_lane = row_of(pick_shape), lane_of(pick_shape)
    pick_slot = pick_lane // LANES
    pick_kind = jnp.where(pick_slot < 2, pick_slot, pick_slot // 2 + 1)

    def find_peaks(c):
        for r in range(LANES * c, LANES * (c + 1), STEP):
            best = tiles[r : r + STEP, :LANES]
            for k in range(1, segments):
                best = jnp.maximum(best, tiles[r : r + STEP, LANES * k : LANES * (k + 1)])
            peak_rows[r : r + STEP, :] = jnp.broadcast_to(
                jnp.max(best.astype(jnp.float32), axis=1, keepdims=True), step_shape
            )

    def add_sums(c):
        lines = []
        for r in range(LANES * c, LANES * (c + 1), STEP):
            peak = peak_rows[r : r + STEP, :]
            column = columns[r : r + STEP, :]
            total = moment = picked = 0.0
            for k in range(segments):
                segment = tiles[r : r + STEP, LANES * k : LANES * (k + 1)].astype(jnp.float32)
                shifted = segment - peak
                weight = jnp.exp(shifted)
                product = weight * shifted
                total = weight if k == 0 else total + weight
                moment = product if k == 0 else moment + product
                picked = jnp.where(column == lane_values[k], segment, picked)
            total_high = total.astype(jnp.bfloat16)
            moment_high = moment.astype(jnp.bfloat16)
            lines.append(
                jnp.concatenate(
                    [
                        peak.astype(jnp.bfloat16),
                        picked.astype(jnp.bfloat16),
                        total_high,
                        (total - total_high.astype(jnp.float32)).astype(jnp.bfloat16),
                        moment_high,
                        (moment - moment_high.astype(jnp.float32)).astype(jnp.bfloat16),
                    ],
                    axis=1,
                )
            )
        pick = (pick_row == chunks * pick_kind + c) & ((pick_slot > 0) | (pick_lane == 0))
        return lines_to_lanes(
            jnp.where(pick, 1.0, 0.0).astype(jnp.bfloat16), jnp.concatenate(lines, axis=0)
        )

    logits_copy.wait()
    find_peaks(0)
    gathered = jnp.zeros((4 * chunks, LANES), jnp.float32)
    for c in range(chunks):
        if c + 1 < chunks:
            find_peaks(c + 1)
        gathered += add_sums(c)
    total = gathered[2 * chunks : 3 * chunks]
    log_total = jnp.log(total)
    log_sum = gathered[:chunks] + log_total
    entropy = log_total - gathered[3 * chunks :] / total
    picked = gathered[chunks : 2 * chunks]
    for n in range(send.shape[0]):
        send[n, 0] = log_sum
        send[n, 1] = entropy
        send[n, 2] = picked


def rollout_sums(values):
    shape = values.shape
    row, lane = row_of(shape), lane_of(shape)
    even = jnp.sum(jnp.where(lane < WIN, values, 0.0), axis=1, keepdims=True)
    odd = jnp.sum(jnp.where(lane >= WIN, values, 0.0), axis=1, keepdims=True)
    spread = jnp.where(
        row == lane % SUBLANES // 2, jnp.where(lane % 2 == 0, even, odd), 0.0
    )
    return jnp.broadcast_to(jnp.sum(spread, axis=0, keepdims=True), shape)


def merged(received):
    count = received.shape[0]
    joint = received[0, 0]
    picked = received[0, 2]
    for n in range(1, count):
        joint = jnp.maximum(joint, received[n, 0])
        picked += received[n, 2]
    total = jnp.zeros_like(joint)
    mixed = jnp.zeros_like(joint)
    for n in range(count):
        shift = received[n, 0] - joint
        factor = jnp.exp(shift)
        total += factor
        mixed += factor * (received[n, 1] - shift)
    log_total = jnp.log(total)
    return joint + log_total, mixed / total + log_total, picked


def merge_kernel(received, send):
    log_sum, entropy, picked = merged(received)
    for n in range(send.shape[0]):
        send[n, 0] = log_sum
        send[n, 1] = entropy
        send[n, 2] = picked


def token_kernel(received, token_info, own_info, send, token_values):
    log_sum, entropy, picked = merged(received)
    chunks = log_sum.shape[0]
    live = token_info[0][:chunks]
    logprob = live * (picked - log_sum)
    token_values[:chunks] = logprob
    token_values[chunks:] = live * entropy
    padded = jnp.concatenate([logprob, jnp.zeros_like(logprob)], axis=0)
    send[...] = own_info[0] + own_info[1] * rollout_sums(padded)


def final_kernel(
    received, token_info, token_values,
    advantage, token_weight, token_logprob, token_entropy, objective,
    advantage_row, weight_rows, objective_row, sems,
):
    chunks = token_weight.shape[0]
    copies = [
        pltpu.make_async_copy(token_values.at[pl.ds(0, chunks)], token_logprob, sems.at[0]),
        pltpu.make_async_copy(token_values.at[pl.ds(chunks, chunks)], token_entropy, sems.at[1]),
        pltpu.make_async_copy(weight_rows, token_weight, sems.at[2]),
        pltpu.make_async_copy(advantage_row, advantage, sems.at[3]),
        pltpu.make_async_copy(objective_row, objective, sems.at[4]),
    ]
    copies[0].start()
    copies[1].start()
    shape = (SUBLANES, LANES)
    row, lane = row_of(shape), lane_of(shape)
    slot = lane // SUBLANES
    first = row < GROUPS
    own_slot = slot == row
    rewards = received[...]
    logprob_sums = pltpu.roll(rewards, LANES // 2, 1)
    member = pltpu.roll(rewards, LANES // 4, 1)

    def row_sums(upper, lower):
        upper = jnp.sum(upper, axis=0, keepdims=True)
        lower = jnp.sum(lower, axis=0, keepdims=True)
        chosen = jnp.where(
            first, jnp.where(own_slot, upper, 0.0), jnp.where(slot == row - GROUPS, lower, 0.0)
        )
        return jnp.sum(chosen, axis=1, keepdims=True)

    total = jnp.sum(rewards, axis=0, keepdims=True)
    sums = jnp.sum(jnp.where(own_slot, total, 0.0), axis=1, keepdims=True)
    group_mean = sums / GROUP
    mean_row = jnp.sum(jnp.where(own_slot & first, group_mean, 0.0), axis=0, keepdims=True)
    centred = rewards - member * mean_row
    spreads = row_sums(centred * centred, centred * logprob_sums)
    group_spread = jnp.maximum(jnp.sqrt(spreads / GROUP), spread_floor)
    info_reward, info_group = token_info[1], token_info[2]
    mean, spread, tokens = group_mean[0:1], group_spread[0:1], sums[GROUPS : GROUPS + 1]
    terms = spreads[GROUPS : GROUPS + 1] * (GROUP * WIN / tokens) / spread
    for g in range(1, GROUPS):
        chosen = info_group == float(g)
        one_tokens = sums[GROUPS + g : GROUPS + g + 1]
        one_spread = group_spread[g : g + 1]
        terms += spreads[GROUPS + g : GROUPS + g + 1] * (GROUP * WIN / one_tokens) / one_spread
        mean = jnp.where(chosen, group_mean[g : g + 1], mean)
        spread = jnp.where(chosen, one_spread, spread)
        tokens = jnp.where(chosen, one_tokens, tokens)
    total_rows = GROUPS * GROUP * WIN
    objective_row[...] = -terms / total_rows
    copies[4].start()
    info_advantage = (info_reward - mean) / spread
    weight = token_info[0] * (info_advantage * (GROUP * WIN / tokens))
    advantage_row[...] = info_advantage[chunks : chunks + 1, :SUBLANES]
    copies[3].start()
    weight_rows[...] = weight[:chunks]
    copies[2].start()
    for copy in copies:
        copy.wait()


def shards(rewards, group_ids, lengths, token_mask, targets, logits):
    rows = logits.shape[0]
    chunks = rows // LANES
    f32, i32 = jnp.float32, jnp.int32
    any_spec = pl.BlockSpec(memory_space=pl.ANY)
    vmem = pl.BlockSpec(memory_space=pltpu.VMEM)

    def kept(*shape):
        return pltpu.VMEM(shape, f32)

    def near(array):
        return pltpu.with_memory_space_constraint(array, pltpu.VMEM)

    sent, token_info, own_info = pl.pallas_call(
        local_kernel,
        name="local_stats",
        in_specs=[any_spec] * 6,
        out_specs=[vmem] * 3,
        out_shape=[
            kept(2 ** len(FIRST), 3, chunks, LANES),
            kept(3, SUBLANES, LANES),
            kept(2, SUBLANES, LANES),
        ],
        scratch_shapes=[
            pltpu.VMEM(logits.shape, logits.dtype),
            pltpu.VMEM((chunks, LANES), i32),
            pltpu.VMEM((chunks, LANES), i32),
            pltpu.SMEM(rewards.shape, i32),
            pltpu.SMEM(rewards.shape, i32),
            pltpu.SMEM(rewards.shape, i32),
            pltpu.VMEM((rows, LANES), f32),
            pltpu.VMEM((rows, LANES), f32),
            pltpu.SemaphoreType.DMA((6,)),
        ],
    )(
        rewards,
        group_ids,
        lengths,
        token_mask.reshape(chunks, LANES),
        targets.reshape(chunks, LANES),
        logits,
    )
    received = lax.all_to_all(sent, FIRST, 0, 0, tiled=True)
    sent = pl.pallas_call(
        merge_kernel,
        name="merge_stats",
        in_specs=[vmem],
        out_specs=vmem,
        out_shape=kept(2 ** len(SECOND), 3, chunks, LANES),
    )(near(received))
    received = lax.all_to_all(sent, SECOND, 0, 0, tiled=True)
    shard_count = 2 ** len(THIRD)
    sent, token_values = pl.pallas_call(
        token_kernel,
        name="token_values",
        in_specs=[vmem] * 3,
        out_specs=[vmem] * 2,
        out_shape=[kept(SUBLANES, LANES), kept(2 * chunks, LANES)],
    )(near(received), near(token_info), near(own_info))
    received = lax.all_to_all(sent.reshape(shard_count, 1, LANES), THIRD, 0, 0, tiled=True)
    advantage, token_weight, token_logprob, token_entropy, objective = pl.pallas_call(
        final_kernel,
        name="group_values",
        in_specs=[vmem] * 3,
        out_specs=[any_spec] * 5,
        out_shape=[
            jax.ShapeDtypeStruct((1, SUBLANES), f32),
            jax.ShapeDtypeStruct((chunks, LANES), f32),
            jax.ShapeDtypeStruct((chunks, LANES), f32),
            jax.ShapeDtypeStruct((chunks, LANES), f32),
            jax.ShapeDtypeStruct((1, 1), f32),
        ],
        scratch_shapes=[
            pltpu.VMEM((1, SUBLANES), f32),
            pltpu.VMEM((chunks, LANES), f32),
            pltpu.VMEM((1, 1), f32),
            pltpu.SemaphoreType.DMA((5,)),
        ],
    )(near(received.reshape(shard_count, LANES)), near(token_info), near(token_values))
    return (
        advantage.reshape(-1),
        token_weight.reshape(-1),
        token_logprob.reshape(-1),
        token_entropy.reshape(-1),
        objective.reshape(()),
    )


def solution(mesh):
    names = X_AXES + MP
    split = Mesh(mesh.devices.reshape((2,) * len(names)), names)
    rows = P(X_AXES)
    in_specs = (rows, rows, rows, rows, rows, P(X_AXES, MP))
    out_specs = (rows, rows, rows, rows, P())
    return jax.shard_map(
        shards, mesh=split, in_specs=in_specs, out_specs=out_specs, check_vma=False
    )
```

```python
import jax
import jax.numpy as jnp
from jax import lax
from jax.experimental import pallas as pl
from jax.experimental.pallas import tpu as pltpu
from jax.sharding import Mesh
from jax.sharding import PartitionSpec as P

GROUP = 16
WIN = 64
LANES = 128
SUBLANES = 8
GROUPS = 4
STEP = 16
X_AXES = ("x2", "x1", "x0")
Z_AXES = ("z2", "z1", "z0")
Y_AXES = ("y2", "y1", "y0")
MP = Z_AXES + Y_AXES + ("core",)
FIRST = Z_AXES + ("core",)
SECOND = Y_AXES

spread_floor = 0.25
reward_unit = 1024.0


def dp_groups():
    groups = []
    for z in range(8):
        for y in range(8):
            swapped = 1 if y == z == 0 else 0
            for core in range(2):
                groups.append(
                    [
                        ((x * 8 + z) * 8 + y) * 2 + (1 - core if x == swapped else core)
                        for x in range(8)
                    ]
                )
    return groups


def lane_of(shape):
    return lax.broadcasted_iota(jnp.int32, shape, 1)


def row_of(shape):
    return lax.broadcasted_iota(jnp.int32, shape, 0)


def lines_to_lanes(pick, block):
    return lax.dot_general(
        pick, block, (((1,), (1,)), ((), ())), preferred_element_type=jnp.float32
    )


def local_kernel(
    rewards, group_ids, lengths, token_mask, targets, logits,
    send, token_info, own_info,
    tiles, target_rows, mask_rows, reward_of, group_of, length_of, peak_rows, columns, sems,
):
    chunks = logits.shape[0] // LANES
    width = logits.shape[1]
    targets_copy = pltpu.make_async_copy(targets, target_rows, sems.at[0])
    small = [
        pltpu.make_async_copy(token_mask, mask_rows, sems.at[1]),
        pltpu.make_async_copy(rewards, reward_of, sems.at[2]),
        pltpu.make_async_copy(group_ids, group_of, sems.at[3]),
        pltpu.make_async_copy(lengths, length_of, sems.at[4]),
    ]
    logits_copy = pltpu.make_async_copy(logits, tiles, sems.at[5])
    targets_copy.start()
    for copy in small:
        copy.start()
    logits_copy.start()
    shard = 0
    for name in MP:
        shard = shard * 2 + lax.axis_index(name)
    targets_copy.wait()

    block = (LANES, LANES)
    diagonal = row_of(block) == lane_of(block)
    digit_row = row_of((2 * LANES, LANES))
    digits = jnp.where(digit_row < LANES, 1.0, float(LANES)).astype(jnp.bfloat16)
    local = target_rows[...] - shard * width
    inside = (local >= 0) & (local < width)
    low_digit = jnp.where(inside, local % LANES, -1).astype(jnp.float32)
    high_digit = jnp.where(inside, local // LANES, 0).astype(jnp.float32)
    for c in range(chunks):
        spread = jnp.concatenate(
            [
                jnp.where(diagonal, low_digit[c : c + 1], 0.0),
                jnp.where(diagonal, high_digit[c : c + 1], 0.0),
            ],
            axis=1,
        ).astype(jnp.bfloat16)
        columns[LANES * c : LANES * (c + 1), :] = jnp.dot(
            spread, digits, preferred_element_type=jnp.float32
        )

    for copy in small:
        copy.wait()
    shape = (SUBLANES, LANES)
    row, lane = row_of(shape), lane_of(shape)
    reward_info = jnp.zeros(shape, jnp.float32)
    group_info = jnp.zeros(shape, jnp.float32)
    length_info = jnp.zeros(shape, jnp.int32)
    own_reward = jnp.zeros(shape, jnp.float32)
    own_group = jnp.zeros(shape, jnp.int32)
    for i in range(2 * chunks):
        here = ((row == i // 2) & (lane // WIN == i % 2)) | ((row == chunks) & (lane == i))
        reward = reward_of[i].astype(jnp.float32) / reward_unit
        reward_info = jnp.where(here, reward, reward_info)
        group_info = jnp.where(here, group_of[i].astype(jnp.float32), group_info)
        length_info = jnp.where(here, length_of[i], length_info)
        own_reward = jnp.where(lane % SUBLANES == i, reward, own_reward)
        own_group = jnp.where(lane % SUBLANES == i, group_of[i], own_group)
    mask8 = jnp.concatenate([mask_rows[...], mask_rows[...]], axis=0)
    live = jnp.where((row < chunks) & (mask8 > 0) & (lane % WIN < length_info), 1.0, 0.0)
    token_info[0] = live
    token_info[1] = reward_info
    token_info[2] = group_info
    slot = lane // SUBLANES
    field = slot // GROUPS
    values = jnp.where(
        field == 0, own_reward, jnp.where(field == 1, rollout_sums(live), 1.0)
    )
    mine = own_group == slot % GROUPS
    own_info[0] = jnp.where(mine & (field != 2), values, 0.0)
    own_info[1] = jnp.where(mine & (field == 2), 1.0, 0.0)

    segments = width // LANES
    step_shape = (STEP, LANES)
    lane_value = lane_of(step_shape).astype(jnp.float32)
    lane_values = [lane_value + float(LANES * k) for k in range(segments)]
    pick_shape = (4 * chunks, 6 * LANES)
    pick_row, pick_lane = row_of(pick_shape), lane_of(pick_shape)
    pick_slot = pick_lane // LANES
    pick_kind = jnp.where(pick_slot < 2, pick_slot, pick_slot // 2 + 1)

    def find_peaks(c):
        for r in range(LANES * c, LANES * (c + 1), STEP):
            best = tiles[r : r + STEP, :LANES]
            for k in range(1, segments):
                best = jnp.maximum(best, tiles[r : r + STEP, LANES * k : LANES * (k + 1)])
            peak_rows[r : r + STEP, :] = jnp.broadcast_to(
                jnp.max(best.astype(jnp.float32), axis=1, keepdims=True), step_shape
            )

    def add_sums(c):
        lines = []
        for r in range(LANES * c, LANES * (c + 1), STEP):
            peak = peak_rows[r : r + STEP, :]
            column = columns[r : r + STEP, :]
            total = moment = picked = 0.0
            for k in range(segments):
                segment = tiles[r : r + STEP, LANES * k : LANES * (k + 1)].astype(jnp.float32)
                shifted = segment - peak
                weight = jnp.exp(shifted)
                product = weight * shifted
                total = weight if k == 0 else total + weight
                moment = product if k == 0 else moment + product
                picked = jnp.where(column == lane_values[k], segment, picked)
            total_high = total.astype(jnp.bfloat16)
            moment_high = moment.astype(jnp.bfloat16)
            lines.append(
                jnp.concatenate(
                    [
                        peak.astype(jnp.bfloat16),
                        picked.astype(jnp.bfloat16),
                        total_high,
                        (total - total_high.astype(jnp.float32)).astype(jnp.bfloat16),
                        moment_high,
                        (moment - moment_high.astype(jnp.float32)).astype(jnp.bfloat16),
                    ],
                    axis=1,
                )
            )
        pick = (pick_row == chunks * pick_kind + c) & ((pick_slot > 0) | (pick_lane == 0))
        return lines_to_lanes(
            jnp.where(pick, 1.0, 0.0).astype(jnp.bfloat16), jnp.concatenate(lines, axis=0)
        )

    logits_copy.wait()
    find_peaks(0)
    gathered = jnp.zeros((4 * chunks, LANES), jnp.float32)
    for c in range(chunks):
        if c + 1 < chunks:
            find_peaks(c + 1)
        gathered += add_sums(c)
    total = gathered[2 * chunks : 3 * chunks]
    log_total = jnp.log(total)
    log_sum = gathered[:chunks] + log_total
    entropy = log_total - gathered[3 * chunks :] / total
    picked = gathered[chunks : 2 * chunks]
    for n in range(send.shape[0]):
        send[n, 0] = log_sum
        send[n, 1] = entropy
        send[n, 2] = picked


def rollout_sums(values):
    shape = values.shape
    row, lane = row_of(shape), lane_of(shape)
    even = jnp.sum(jnp.where(lane < WIN, values, 0.0), axis=1, keepdims=True)
    odd = jnp.sum(jnp.where(lane >= WIN, values, 0.0), axis=1, keepdims=True)
    spread = jnp.where(
        row == lane % SUBLANES // 2, jnp.where(lane % 2 == 0, even, odd), 0.0
    )
    return jnp.broadcast_to(jnp.sum(spread, axis=0, keepdims=True), shape)


def merged(received):
    count = received.shape[0]
    joint = received[0, 0]
    picked = received[0, 2]
    for n in range(1, count):
        joint = jnp.maximum(joint, received[n, 0])
        picked += received[n, 2]
    total = jnp.zeros_like(joint)
    mixed = jnp.zeros_like(joint)
    for n in range(count):
        shift = received[n, 0] - joint
        factor = jnp.exp(shift)
        total += factor
        mixed += factor * (received[n, 1] - shift)
    log_total = jnp.log(total)
    return joint + log_total, mixed / total + log_total, picked


def merge_kernel(received, send):
    log_sum, entropy, picked = merged(received)
    for n in range(send.shape[0]):
        send[n, 0] = log_sum
        send[n, 1] = entropy
        send[n, 2] = picked


def token_kernel(received, token_info, own_info, send, token_values):
    log_sum, entropy, picked = merged(received)
    chunks = log_sum.shape[0]
    live = token_info[0][:chunks]
    logprob = live * (picked - log_sum)
    token_values[:chunks] = logprob
    token_values[chunks:] = live * entropy
    padded = jnp.concatenate([logprob, jnp.zeros_like(logprob)], axis=0)
    send[...] = own_info[0] + own_info[1] * rollout_sums(padded)


def final_kernel(
    received, token_info, token_values,
    advantage, token_weight, token_logprob, token_entropy, objective,
    advantage_row, weight_rows, objective_row, sems,
):
    chunks = token_weight.shape[0]
    copies = [
        pltpu.make_async_copy(token_values.at[pl.ds(0, chunks)], token_logprob, sems.at[0]),
        pltpu.make_async_copy(token_values.at[pl.ds(chunks, chunks)], token_entropy, sems.at[1]),
        pltpu.make_async_copy(weight_rows, token_weight, sems.at[2]),
        pltpu.make_async_copy(advantage_row, advantage, sems.at[3]),
        pltpu.make_async_copy(objective_row, objective, sems.at[4]),
    ]
    copies[0].start()
    copies[1].start()
    shape = (SUBLANES, LANES)
    row, lane = row_of(shape), lane_of(shape)
    slot = lane // SUBLANES
    first = row < GROUPS
    own_slot = slot == row
    rewards = received[...]
    logprob_sums = pltpu.roll(rewards, LANES // 2, 1)
    member = pltpu.roll(rewards, LANES // 4, 1)

    def row_sums(upper, lower):
        upper = jnp.sum(upper, axis=0, keepdims=True)
        lower = jnp.sum(lower, axis=0, keepdims=True)
        chosen = jnp.where(
            first, jnp.where(own_slot, upper, 0.0), jnp.where(slot == row - GROUPS, lower, 0.0)
        )
        return jnp.sum(chosen, axis=1, keepdims=True)

    total = jnp.sum(rewards, axis=0, keepdims=True)
    sums = jnp.sum(jnp.where(own_slot, total, 0.0), axis=1, keepdims=True)
    group_mean = sums / GROUP
    mean_row = jnp.sum(jnp.where(own_slot & first, group_mean, 0.0), axis=0, keepdims=True)
    centred = rewards - member * mean_row
    spreads = row_sums(centred * centred, centred * logprob_sums)
    group_spread = jnp.maximum(jnp.sqrt(spreads / GROUP), spread_floor)
    info_reward, info_group = token_info[1], token_info[2]
    mean, spread, tokens = group_mean[0:1], group_spread[0:1], sums[GROUPS : GROUPS + 1]
    terms = spreads[GROUPS : GROUPS + 1] * (GROUP * WIN / tokens) / spread
    for g in range(1, GROUPS):
        chosen = info_group == float(g)
        one_tokens = sums[GROUPS + g : GROUPS + g + 1]
        one_spread = group_spread[g : g + 1]
        terms += spreads[GROUPS + g : GROUPS + g + 1] * (GROUP * WIN / one_tokens) / one_spread
        mean = jnp.where(chosen, group_mean[g : g + 1], mean)
        spread = jnp.where(chosen, one_spread, spread)
        tokens = jnp.where(chosen, one_tokens, tokens)
    total_rows = GROUPS * GROUP * WIN
    objective_row[...] = -terms / total_rows
    copies[4].start()
    info_advantage = (info_reward - mean) / spread
    weight = token_info[0] * (info_advantage * (GROUP * WIN / tokens))
    advantage_row[...] = info_advantage[chunks : chunks + 1, :SUBLANES]
    copies[3].start()
    weight_rows[...] = weight[:chunks]
    copies[2].start()
    for copy in copies:
        copy.wait()


def shards(rewards, group_ids, lengths, token_mask, targets, logits):
    rows = logits.shape[0]
    chunks = rows // LANES
    f32, i32 = jnp.float32, jnp.int32
    any_spec = pl.BlockSpec(memory_space=pl.ANY)
    vmem = pl.BlockSpec(memory_space=pltpu.VMEM)

    def kept(*shape):
        return pltpu.VMEM(shape, f32)

    def near(array):
        return pltpu.with_memory_space_constraint(array, pltpu.VMEM)

    sent, token_info, own_info = pl.pallas_call(
        local_kernel,
        name="local_stats",
        in_specs=[any_spec] * 6,
        out_specs=[vmem] * 3,
        out_shape=[
            kept(2 ** len(FIRST), 3, chunks, LANES),
            kept(3, SUBLANES, LANES),
            kept(2, SUBLANES, LANES),
        ],
        scratch_shapes=[
            pltpu.VMEM(logits.shape, logits.dtype),
            pltpu.VMEM((chunks, LANES), i32),
            pltpu.VMEM((chunks, LANES), i32),
            pltpu.SMEM(rewards.shape, i32),
            pltpu.SMEM(rewards.shape, i32),
            pltpu.SMEM(rewards.shape, i32),
            pltpu.VMEM((rows, LANES), f32),
            pltpu.VMEM((rows, LANES), f32),
            pltpu.SemaphoreType.DMA((6,)),
        ],
    )(
        rewards,
        group_ids,
        lengths,
        token_mask.reshape(chunks, LANES),
        targets.reshape(chunks, LANES),
        logits,
    )
    received = lax.all_to_all(sent, FIRST, 0, 0, tiled=True)
    sent = pl.pallas_call(
        merge_kernel,
        name="merge_stats",
        in_specs=[vmem],
        out_specs=vmem,
        out_shape=kept(2 ** len(SECOND), 3, chunks, LANES),
    )(near(received))
    received = lax.all_to_all(sent, SECOND, 0, 0, tiled=True)
    shard_count = 2 ** len(X_AXES)
    sent, token_values = pl.pallas_call(
        token_kernel,
        name="token_values",
        in_specs=[vmem] * 3,
        out_specs=[vmem] * 2,
        out_shape=[kept(SUBLANES, LANES), kept(2 * chunks, LANES)],
    )(near(received), near(token_info), near(own_info))
    received = lax.all_to_all(
        sent.reshape(shard_count, 1, LANES),
        X_AXES + MP,
        0,
        0,
        axis_index_groups=dp_groups(),
        tiled=True,
    )
    advantage, token_weight, token_logprob, token_entropy, objective = pl.pallas_call(
        final_kernel,
        name="group_values",
        in_specs=[vmem] * 3,
        out_specs=[any_spec] * 5,
        out_shape=[
            jax.ShapeDtypeStruct((1, SUBLANES), f32),
            jax.ShapeDtypeStruct((chunks, LANES), f32),
            jax.ShapeDtypeStruct((chunks, LANES), f32),
            jax.ShapeDtypeStruct((chunks, LANES), f32),
            jax.ShapeDtypeStruct((1, 1), f32),
        ],
        scratch_shapes=[
            pltpu.VMEM((1, SUBLANES), f32),
            pltpu.VMEM((chunks, LANES), f32),
            pltpu.VMEM((1, 1), f32),
            pltpu.SemaphoreType.DMA((5,)),
        ],
    )(near(received.reshape(shard_count, LANES)), near(token_info), near(token_values))
    return (
        advantage.reshape(-1),
        token_weight.reshape(-1),
        token_logprob.reshape(-1),
        token_entropy.reshape(-1),
        objective.reshape(()),
    )


def solution(mesh):
    names = X_AXES + MP
    split = Mesh(mesh.devices.reshape((2,) * len(names)), names)
    rows = P(X_AXES)
    in_specs = (rows, rows, rows, rows, rows, P(X_AXES, MP))
    out_specs = (rows, rows, rows, rows, P())
    return jax.shard_map(
        shards, mesh=split, in_specs=in_specs, out_specs=out_specs, check_vma=False
    )
```

```python
import jax
import jax.numpy as jnp
from jax import lax
from jax.experimental import pallas as pl
from jax.experimental.pallas import tpu as pltpu
from jax.sharding import Mesh
from jax.sharding import PartitionSpec as P

GROUP = 16
WIN = 64
LANES = 128
SUBLANES = 8
GROUPS = 4
STEP = 16
X_AXES = ("x2", "x1", "x0")
Z_AXES = ("z2", "z1", "z0")
Y_AXES = ("y2", "y1", "y0")
MP = Z_AXES + Y_AXES + ("core",)
FIRST = ("core",) + Z_AXES

spread_floor = 0.25
reward_unit = 1024.0


def position(x, z, y, core):
    return ((x * 8 + z) * 8 + y) * 2 + core


def y_groups():
    return [
        [position(x, z, y, core if y < 4 else 1 - core) for y in range(8)]
        for x in range(8)
        for z in range(8)
        for core in range(2)
    ]


def x_groups():
    groups = []
    for z in range(8):
        for y in range(8):
            swapped = (1,) if y == z == 0 else (4, 5, 6, 7)
            for core in range(2):
                groups.append(
                    [position(x, z, y, 1 - core if x in swapped else core) for x in range(8)]
                )
    return groups


def lane_of(shape):
    return lax.broadcasted_iota(jnp.int32, shape, 1)


def row_of(shape):
    return lax.broadcasted_iota(jnp.int32, shape, 0)


def lines_to_lanes(pick, block):
    return lax.dot_general(
        pick, block, (((1,), (1,)), ((), ())), preferred_element_type=jnp.float32
    )


def local_kernel(
    rewards, group_ids, lengths, token_mask, targets, logits,
    send, token_info, own_info,
    tiles, target_rows, mask_rows, reward_of, group_of, length_of, peak_rows, columns, sems,
):
    chunks = logits.shape[0] // LANES
    width = logits.shape[1]
    targets_copy = pltpu.make_async_copy(targets, target_rows, sems.at[0])
    small = [
        pltpu.make_async_copy(token_mask, mask_rows, sems.at[1]),
        pltpu.make_async_copy(rewards, reward_of, sems.at[2]),
        pltpu.make_async_copy(group_ids, group_of, sems.at[3]),
        pltpu.make_async_copy(lengths, length_of, sems.at[4]),
    ]
    logits_copy = pltpu.make_async_copy(logits, tiles, sems.at[5])
    targets_copy.start()
    for copy in small:
        copy.start()
    logits_copy.start()
    shard = 0
    for name in MP:
        shard = shard * 2 + lax.axis_index(name)
    targets_copy.wait()

    block = (LANES, LANES)
    diagonal = row_of(block) == lane_of(block)
    digit_row = row_of((2 * LANES, LANES))
    digits = jnp.where(digit_row < LANES, 1.0, float(LANES)).astype(jnp.bfloat16)
    local = target_rows[...] - shard * width
    inside = (local >= 0) & (local < width)
    low_digit = jnp.where(inside, local % LANES, -1).astype(jnp.float32)
    high_digit = jnp.where(inside, local // LANES, 0).astype(jnp.float32)
    for c in range(chunks):
        spread = jnp.concatenate(
            [
                jnp.where(diagonal, low_digit[c : c + 1], 0.0),
                jnp.where(diagonal, high_digit[c : c + 1], 0.0),
            ],
            axis=1,
        ).astype(jnp.bfloat16)
        columns[LANES * c : LANES * (c + 1), :] = jnp.dot(
            spread, digits, preferred_element_type=jnp.float32
        )

    for copy in small:
        copy.wait()
    shape = (SUBLANES, LANES)
    row, lane = row_of(shape), lane_of(shape)
    reward_info = jnp.zeros(shape, jnp.float32)
    group_info = jnp.zeros(shape, jnp.float32)
    length_info = jnp.zeros(shape, jnp.int32)
    own_reward = jnp.zeros(shape, jnp.float32)
    own_group = jnp.zeros(shape, jnp.int32)
    for i in range(2 * chunks):
        here = ((row == i // 2) & (lane // WIN == i % 2)) | ((row == chunks) & (lane == i))
        reward = reward_of[i].astype(jnp.float32) / reward_unit
        reward_info = jnp.where(here, reward, reward_info)
        group_info = jnp.where(here, group_of[i].astype(jnp.float32), group_info)
        length_info = jnp.where(here, length_of[i], length_info)
        own_reward = jnp.where(lane % SUBLANES == i, reward, own_reward)
        own_group = jnp.where(lane % SUBLANES == i, group_of[i], own_group)
    mask8 = jnp.concatenate([mask_rows[...], mask_rows[...]], axis=0)
    live = jnp.where((row < chunks) & (mask8 > 0) & (lane % WIN < length_info), 1.0, 0.0)
    token_info[0] = live
    token_info[1] = reward_info
    token_info[2] = group_info
    slot = lane // SUBLANES
    field = slot // GROUPS
    values = jnp.where(
        field == 0, own_reward, jnp.where(field == 1, rollout_sums(live), 1.0)
    )
    mine = own_group == slot % GROUPS
    own_info[0] = jnp.where(mine & (field != 2), values, 0.0)
    own_info[1] = jnp.where(mine & (field == 2), 1.0, 0.0)

    segments = width // LANES
    step_shape = (STEP, LANES)
    lane_value = lane_of(step_shape).astype(jnp.float32)
    lane_values = [lane_value + float(LANES * k) for k in range(segments)]
    pick_shape = (4 * chunks, 6 * LANES)
    pick_row, pick_lane = row_of(pick_shape), lane_of(pick_shape)
    pick_slot = pick_lane // LANES
    pick_kind = jnp.where(pick_slot < 2, pick_slot, pick_slot // 2 + 1)

    def find_peaks(c):
        for r in range(LANES * c, LANES * (c + 1), STEP):
            best = tiles[r : r + STEP, :LANES]
            for k in range(1, segments):
                best = jnp.maximum(best, tiles[r : r + STEP, LANES * k : LANES * (k + 1)])
            peak_rows[r : r + STEP, :] = jnp.broadcast_to(
                jnp.max(best.astype(jnp.float32), axis=1, keepdims=True), step_shape
            )

    def add_sums(c):
        lines = []
        for r in range(LANES * c, LANES * (c + 1), STEP):
            peak = peak_rows[r : r + STEP, :]
            column = columns[r : r + STEP, :]
            total = moment = picked = 0.0
            for k in range(segments):
                segment = tiles[r : r + STEP, LANES * k : LANES * (k + 1)].astype(jnp.float32)
                shifted = segment - peak
                weight = jnp.exp(shifted)
                product = weight * shifted
                total = weight if k == 0 else total + weight
                moment = product if k == 0 else moment + product
                picked = jnp.where(column == lane_values[k], segment, picked)
            total_high = total.astype(jnp.bfloat16)
            moment_high = moment.astype(jnp.bfloat16)
            lines.append(
                jnp.concatenate(
                    [
                        peak.astype(jnp.bfloat16),
                        picked.astype(jnp.bfloat16),
                        total_high,
                        (total - total_high.astype(jnp.float32)).astype(jnp.bfloat16),
                        moment_high,
                        (moment - moment_high.astype(jnp.float32)).astype(jnp.bfloat16),
                    ],
                    axis=1,
                )
            )
        pick = (pick_row == chunks * pick_kind + c) & ((pick_slot > 0) | (pick_lane == 0))
        return lines_to_lanes(
            jnp.where(pick, 1.0, 0.0).astype(jnp.bfloat16), jnp.concatenate(lines, axis=0)
        )

    logits_copy.wait()
    find_peaks(0)
    gathered = jnp.zeros((4 * chunks, LANES), jnp.float32)
    for c in range(chunks):
        if c + 1 < chunks:
            find_peaks(c + 1)
        gathered += add_sums(c)
    total = gathered[2 * chunks : 3 * chunks]
    log_total = jnp.log(total)
    log_sum = gathered[:chunks] + log_total
    entropy = log_total - gathered[3 * chunks :] / total
    picked = gathered[chunks : 2 * chunks]
    for n in range(send.shape[0]):
        send[n, 0] = log_sum
        send[n, 1] = entropy
        send[n, 2] = picked


def rollout_sums(values):
    shape = values.shape
    row, lane = row_of(shape), lane_of(shape)
    even = jnp.sum(jnp.where(lane < WIN, values, 0.0), axis=1, keepdims=True)
    odd = jnp.sum(jnp.where(lane >= WIN, values, 0.0), axis=1, keepdims=True)
    spread = jnp.where(
        row == lane % SUBLANES // 2, jnp.where(lane % 2 == 0, even, odd), 0.0
    )
    return jnp.broadcast_to(jnp.sum(spread, axis=0, keepdims=True), shape)


def merged(received):
    count = received.shape[0]
    joint = received[0, 0]
    picked = received[0, 2]
    for n in range(1, count):
        joint = jnp.maximum(joint, received[n, 0])
        picked += received[n, 2]
    total = jnp.zeros_like(joint)
    mixed = jnp.zeros_like(joint)
    for n in range(count):
        shift = received[n, 0] - joint
        factor = jnp.exp(shift)
        total += factor
        mixed += factor * (received[n, 1] - shift)
    log_total = jnp.log(total)
    return joint + log_total, mixed / total + log_total, picked


def merge_kernel(received, send):
    log_sum, entropy, picked = merged(received)
    for n in range(send.shape[0]):
        send[n, 0] = log_sum
        send[n, 1] = entropy
        send[n, 2] = picked


def token_kernel(received, token_info, own_info, send, token_values):
    log_sum, entropy, picked = merged(received)
    chunks = log_sum.shape[0]
    live = token_info[0][:chunks]
    logprob = live * (picked - log_sum)
    token_values[:chunks] = logprob
    token_values[chunks:] = live * entropy
    padded = jnp.concatenate([logprob, jnp.zeros_like(logprob)], axis=0)
    send[...] = own_info[0] + own_info[1] * rollout_sums(padded)


def final_kernel(
    received, token_info, token_values,
    advantage, token_weight, token_logprob, token_entropy, objective,
    advantage_row, weight_rows, objective_row, sems,
):
    chunks = token_weight.shape[0]
    copies = [
        pltpu.make_async_copy(token_values.at[pl.ds(0, chunks)], token_logprob, sems.at[0]),
        pltpu.make_async_copy(token_values.at[pl.ds(chunks, chunks)], token_entropy, sems.at[1]),
        pltpu.make_async_copy(weight_rows, token_weight, sems.at[2]),
        pltpu.make_async_copy(advantage_row, advantage, sems.at[3]),
        pltpu.make_async_copy(objective_row, objective, sems.at[4]),
    ]
    copies[0].start()
    copies[1].start()
    shape = (SUBLANES, LANES)
    row, lane = row_of(shape), lane_of(shape)
    slot = lane // SUBLANES
    first = row < GROUPS
    own_slot = slot == row
    rewards = received[...]
    logprob_sums = pltpu.roll(rewards, LANES // 2, 1)
    member = pltpu.roll(rewards, LANES // 4, 1)

    def row_sums(upper, lower):
        upper = jnp.sum(upper, axis=0, keepdims=True)
        lower = jnp.sum(lower, axis=0, keepdims=True)
        chosen = jnp.where(
            first, jnp.where(own_slot, upper, 0.0), jnp.where(slot == row - GROUPS, lower, 0.0)
        )
        return jnp.sum(chosen, axis=1, keepdims=True)

    total = jnp.sum(rewards, axis=0, keepdims=True)
    sums = jnp.sum(jnp.where(own_slot, total, 0.0), axis=1, keepdims=True)
    group_mean = sums / GROUP
    mean_row = jnp.sum(jnp.where(own_slot & first, group_mean, 0.0), axis=0, keepdims=True)
    centred = rewards - member * mean_row
    spreads = row_sums(centred * centred, centred * logprob_sums)
    group_spread = jnp.maximum(jnp.sqrt(spreads / GROUP), spread_floor)
    info_reward, info_group = token_info[1], token_info[2]
    mean, spread, tokens = group_mean[0:1], group_spread[0:1], sums[GROUPS : GROUPS + 1]
    terms = spreads[GROUPS : GROUPS + 1] * (GROUP * WIN / tokens) / spread
    for g in range(1, GROUPS):
        chosen = info_group == float(g)
        one_tokens = sums[GROUPS + g : GROUPS + g + 1]
        one_spread = group_spread[g : g + 1]
        terms += spreads[GROUPS + g : GROUPS + g + 1] * (GROUP * WIN / one_tokens) / one_spread
        mean = jnp.where(chosen, group_mean[g : g + 1], mean)
        spread = jnp.where(chosen, one_spread, spread)
        tokens = jnp.where(chosen, one_tokens, tokens)
    total_rows = GROUPS * GROUP * WIN
    objective_row[...] = -terms / total_rows
    copies[4].start()
    info_advantage = (info_reward - mean) / spread
    weight = token_info[0] * (info_advantage * (GROUP * WIN / tokens))
    advantage_row[...] = info_advantage[chunks : chunks + 1, :SUBLANES]
    copies[3].start()
    weight_rows[...] = weight[:chunks]
    copies[2].start()
    for copy in copies:
        copy.wait()


def shards(rewards, group_ids, lengths, token_mask, targets, logits):
    rows = logits.shape[0]
    chunks = rows // LANES
    f32, i32 = jnp.float32, jnp.int32
    any_spec = pl.BlockSpec(memory_space=pl.ANY)
    vmem = pl.BlockSpec(memory_space=pltpu.VMEM)

    def kept(*shape):
        return pltpu.VMEM(shape, f32)

    def near(array):
        return pltpu.with_memory_space_constraint(array, pltpu.VMEM)

    sent, token_info, own_info = pl.pallas_call(
        local_kernel,
        name="local_stats",
        in_specs=[any_spec] * 6,
        out_specs=[vmem] * 3,
        out_shape=[
            kept(2 ** len(FIRST), 3, chunks, LANES),
            kept(3, SUBLANES, LANES),
            kept(2, SUBLANES, LANES),
        ],
        scratch_shapes=[
            pltpu.VMEM(logits.shape, logits.dtype),
            pltpu.VMEM((chunks, LANES), i32),
            pltpu.VMEM((chunks, LANES), i32),
            pltpu.SMEM(rewards.shape, i32),
            pltpu.SMEM(rewards.shape, i32),
            pltpu.SMEM(rewards.shape, i32),
            pltpu.VMEM((rows, LANES), f32),
            pltpu.VMEM((rows, LANES), f32),
            pltpu.SemaphoreType.DMA((6,)),
        ],
    )(
        rewards,
        group_ids,
        lengths,
        token_mask.reshape(chunks, LANES),
        targets.reshape(chunks, LANES),
        logits,
    )
    received = lax.all_to_all(sent, FIRST, 0, 0, tiled=True)
    sent = pl.pallas_call(
        merge_kernel,
        name="merge_stats",
        in_specs=[vmem],
        out_specs=vmem,
        out_shape=kept(2 ** len(Y_AXES), 3, chunks, LANES),
    )(near(received))
    received = lax.all_to_all(
        sent, X_AXES + MP, 0, 0, axis_index_groups=y_groups(), tiled=True
    )
    shard_count = 2 ** len(X_AXES)
    sent, token_values = pl.pallas_call(
        token_kernel,
        name="token_values",
        in_specs=[vmem] * 3,
        out_specs=[vmem] * 2,
        out_shape=[kept(SUBLANES, LANES), kept(2 * chunks, LANES)],
    )(near(received), near(token_info), near(own_info))
    received = lax.all_to_all(
        sent.reshape(shard_count, 1, LANES),
        X_AXES + MP,
        0,
        0,
        axis_index_groups=x_groups(),
        tiled=True,
    )
    advantage, token_weight, token_logprob, token_entropy, objective = pl.pallas_call(
        final_kernel,
        name="group_values",
        in_specs=[vmem] * 3,
        out_specs=[any_spec] * 5,
        out_shape=[
            jax.ShapeDtypeStruct((1, SUBLANES), f32),
            jax.ShapeDtypeStruct((chunks, LANES), f32),
            jax.ShapeDtypeStruct((chunks, LANES), f32),
            jax.ShapeDtypeStruct((chunks, LANES), f32),
            jax.ShapeDtypeStruct((1, 1), f32),
        ],
        scratch_shapes=[
            pltpu.VMEM((1, SUBLANES), f32),
            pltpu.VMEM((chunks, LANES), f32),
            pltpu.VMEM((1, 1), f32),
            pltpu.SemaphoreType.DMA((5,)),
        ],
    )(near(received.reshape(shard_count, LANES)), near(token_info), near(token_values))
    return (
        advantage.reshape(-1),
        token_weight.reshape(-1),
        token_logprob.reshape(-1),
        token_entropy.reshape(-1),
        objective.reshape(()),
    )


def solution(mesh):
    names = X_AXES + MP
    split = Mesh(mesh.devices.reshape((2,) * len(names)), names)
    rows = P(X_AXES)
    in_specs = (rows, rows, rows, rows, rows, P(X_AXES, MP))
    out_specs = (rows, rows, rows, rows, P())
    return jax.shard_map(
        shards, mesh=split, in_specs=in_specs, out_specs=out_specs, check_vma=False
    )
```

```python
import jax
import jax.numpy as jnp
from jax import lax
from jax.experimental import pallas as pl
from jax.experimental.pallas import tpu as pltpu
from jax.sharding import Mesh
from jax.sharding import PartitionSpec as P

GROUP = 16
WIN = 64
LANES = 128
SUBLANES = 8
GROUPS = 4
STEP = 16
X_AXES = ("x2", "x1", "x0")
Z_AXES = ("z2", "z1", "z0")
Y_AXES = ("y2", "y1", "y0")
MP = Z_AXES + Y_AXES + ("core",)
FIRST = ("core",) + Z_AXES

spread_floor = 0.25
reward_unit = 1024.0


def position(x, z, y, core):
    return ((x * 8 + z) * 8 + y) * 2 + core


def y_groups():
    return [
        [position(x, z, y, core if y < 4 else 1 - core) for y in range(8)]
        for x in range(8)
        for z in range(8)
        for core in range(2)
    ]


def x_groups():
    groups = []
    for z in range(8):
        for y in range(8):
            swapped = () if y == z == 0 else (4, 5, 6, 7)
            for core in range(2):
                groups.append(
                    [position(x, z, y, 1 - core if x in swapped else core) for x in range(8)]
                )
    return groups


def lane_of(shape):
    return lax.broadcasted_iota(jnp.int32, shape, 1)


def row_of(shape):
    return lax.broadcasted_iota(jnp.int32, shape, 0)


def lines_to_lanes(pick, block):
    return lax.dot_general(
        pick, block, (((1,), (1,)), ((), ())), preferred_element_type=jnp.float32
    )


def local_kernel(
    rewards, group_ids, lengths, token_mask, targets, logits,
    send, token_info, own_info,
    tiles, target_rows, mask_rows, reward_of, group_of, length_of, peak_rows, columns, sems,
):
    chunks = logits.shape[0] // LANES
    width = logits.shape[1]
    targets_copy = pltpu.make_async_copy(targets, target_rows, sems.at[0])
    small = [
        pltpu.make_async_copy(token_mask, mask_rows, sems.at[1]),
        pltpu.make_async_copy(rewards, reward_of, sems.at[2]),
        pltpu.make_async_copy(group_ids, group_of, sems.at[3]),
        pltpu.make_async_copy(lengths, length_of, sems.at[4]),
    ]
    logits_copy = pltpu.make_async_copy(logits, tiles, sems.at[5])
    targets_copy.start()
    for copy in small:
        copy.start()
    logits_copy.start()
    shard = 0
    for name in MP:
        shard = shard * 2 + lax.axis_index(name)
    targets_copy.wait()

    block = (LANES, LANES)
    diagonal = row_of(block) == lane_of(block)
    digit_row = row_of((2 * LANES, LANES))
    digits = jnp.where(digit_row < LANES, 1.0, float(LANES)).astype(jnp.bfloat16)
    local = target_rows[...] - shard * width
    inside = (local >= 0) & (local < width)
    low_digit = jnp.where(inside, local % LANES, -1).astype(jnp.float32)
    high_digit = jnp.where(inside, local // LANES, 0).astype(jnp.float32)
    for c in range(chunks):
        spread = jnp.concatenate(
            [
                jnp.where(diagonal, low_digit[c : c + 1], 0.0),
                jnp.where(diagonal, high_digit[c : c + 1], 0.0),
            ],
            axis=1,
        ).astype(jnp.bfloat16)
        columns[LANES * c : LANES * (c + 1), :] = jnp.dot(
            spread, digits, preferred_element_type=jnp.float32
        )

    for copy in small:
        copy.wait()
    shape = (SUBLANES, LANES)
    row, lane = row_of(shape), lane_of(shape)
    reward_info = jnp.zeros(shape, jnp.float32)
    group_info = jnp.zeros(shape, jnp.float32)
    length_info = jnp.zeros(shape, jnp.int32)
    own_reward = jnp.zeros(shape, jnp.float32)
    own_group = jnp.zeros(shape, jnp.int32)
    for i in range(2 * chunks):
        here = ((row == i // 2) & (lane // WIN == i % 2)) | ((row == chunks) & (lane == i))
        reward = reward_of[i].astype(jnp.float32) / reward_unit
        reward_info = jnp.where(here, reward, reward_info)
        group_info = jnp.where(here, group_of[i].astype(jnp.float32), group_info)
        length_info = jnp.where(here, length_of[i], length_info)
        own_reward = jnp.where(lane % SUBLANES == i, reward, own_reward)
        own_group = jnp.where(lane % SUBLANES == i, group_of[i], own_group)
    mask8 = jnp.concatenate([mask_rows[...], mask_rows[...]], axis=0)
    live = jnp.where((row < chunks) & (mask8 > 0) & (lane % WIN < length_info), 1.0, 0.0)
    token_info[0] = live
    token_info[1] = reward_info
    token_info[2] = group_info
    slot = lane // SUBLANES
    field = slot // GROUPS
    values = jnp.where(
        field == 0, own_reward, jnp.where(field == 1, rollout_sums(live), 1.0)
    )
    mine = own_group == slot % GROUPS
    own_info[0] = jnp.where(mine & (field != 2), values, 0.0)
    own_info[1] = jnp.where(mine & (field == 2), 1.0, 0.0)

    segments = width // LANES
    step_shape = (STEP, LANES)
    lane_value = lane_of(step_shape).astype(jnp.float32)
    lane_values = [lane_value + float(LANES * k) for k in range(segments)]
    pick_shape = (4 * chunks, 6 * LANES)
    pick_row, pick_lane = row_of(pick_shape), lane_of(pick_shape)
    pick_slot = pick_lane // LANES
    pick_kind = jnp.where(pick_slot < 2, pick_slot, pick_slot // 2 + 1)

    def find_peaks(c):
        for r in range(LANES * c, LANES * (c + 1), STEP):
            best = tiles[r : r + STEP, :LANES]
            for k in range(1, segments):
                best = jnp.maximum(best, tiles[r : r + STEP, LANES * k : LANES * (k + 1)])
            peak_rows[r : r + STEP, :] = jnp.broadcast_to(
                jnp.max(best.astype(jnp.float32), axis=1, keepdims=True), step_shape
            )

    def add_sums(c):
        lines = []
        for r in range(LANES * c, LANES * (c + 1), STEP):
            peak = peak_rows[r : r + STEP, :]
            column = columns[r : r + STEP, :]
            total = moment = picked = 0.0
            for k in range(segments):
                segment = tiles[r : r + STEP, LANES * k : LANES * (k + 1)].astype(jnp.float32)
                shifted = segment - peak
                weight = jnp.exp(shifted)
                product = weight * shifted
                total = weight if k == 0 else total + weight
                moment = product if k == 0 else moment + product
                picked = jnp.where(column == lane_values[k], segment, picked)
            total_high = total.astype(jnp.bfloat16)
            moment_high = moment.astype(jnp.bfloat16)
            lines.append(
                jnp.concatenate(
                    [
                        peak.astype(jnp.bfloat16),
                        picked.astype(jnp.bfloat16),
                        total_high,
                        (total - total_high.astype(jnp.float32)).astype(jnp.bfloat16),
                        moment_high,
                        (moment - moment_high.astype(jnp.float32)).astype(jnp.bfloat16),
                    ],
                    axis=1,
                )
            )
        pick = (pick_row == chunks * pick_kind + c) & ((pick_slot > 0) | (pick_lane == 0))
        return lines_to_lanes(
            jnp.where(pick, 1.0, 0.0).astype(jnp.bfloat16), jnp.concatenate(lines, axis=0)
        )

    logits_copy.wait()
    find_peaks(0)
    gathered = jnp.zeros((4 * chunks, LANES), jnp.float32)
    for c in range(chunks):
        if c + 1 < chunks:
            find_peaks(c + 1)
        gathered += add_sums(c)
    total = gathered[2 * chunks : 3 * chunks]
    log_total = jnp.log(total)
    log_sum = gathered[:chunks] + log_total
    entropy = log_total - gathered[3 * chunks :] / total
    picked = gathered[chunks : 2 * chunks]
    for n in range(send.shape[0]):
        send[n, 0] = log_sum
        send[n, 1] = entropy
        send[n, 2] = picked


def rollout_sums(values):
    shape = values.shape
    row, lane = row_of(shape), lane_of(shape)
    even = jnp.sum(jnp.where(lane < WIN, values, 0.0), axis=1, keepdims=True)
    odd = jnp.sum(jnp.where(lane >= WIN, values, 0.0), axis=1, keepdims=True)
    spread = jnp.where(
        row == lane % SUBLANES // 2, jnp.where(lane % 2 == 0, even, odd), 0.0
    )
    return jnp.broadcast_to(jnp.sum(spread, axis=0, keepdims=True), shape)


def merged(received):
    count = received.shape[0]
    joint = received[0, 0]
    picked = received[0, 2]
    for n in range(1, count):
        joint = jnp.maximum(joint, received[n, 0])
        picked += received[n, 2]
    total = jnp.zeros_like(joint)
    mixed = jnp.zeros_like(joint)
    for n in range(count):
        shift = received[n, 0] - joint
        factor = jnp.exp(shift)
        total += factor
        mixed += factor * (received[n, 1] - shift)
    log_total = jnp.log(total)
    return joint + log_total, mixed / total + log_total, picked


def merge_kernel(received, send):
    log_sum, entropy, picked = merged(received)
    for n in range(send.shape[0]):
        send[n, 0] = log_sum
        send[n, 1] = entropy
        send[n, 2] = picked


def token_kernel(received, token_info, own_info, send, token_values):
    log_sum, entropy, picked = merged(received)
    chunks = log_sum.shape[0]
    live = token_info[0][:chunks]
    logprob = live * (picked - log_sum)
    token_values[:chunks] = logprob
    token_values[chunks:] = live * entropy
    padded = jnp.concatenate([logprob, jnp.zeros_like(logprob)], axis=0)
    send[...] = own_info[0] + own_info[1] * rollout_sums(padded)


def final_kernel(
    received, token_info, token_values,
    advantage, token_weight, token_logprob, token_entropy, objective,
    advantage_row, weight_rows, objective_row, sems,
):
    chunks = token_weight.shape[0]
    copies = [
        pltpu.make_async_copy(token_values.at[pl.ds(0, chunks)], token_logprob, sems.at[0]),
        pltpu.make_async_copy(token_values.at[pl.ds(chunks, chunks)], token_entropy, sems.at[1]),
        pltpu.make_async_copy(weight_rows, token_weight, sems.at[2]),
        pltpu.make_async_copy(advantage_row, advantage, sems.at[3]),
        pltpu.make_async_copy(objective_row, objective, sems.at[4]),
    ]
    copies[0].start()
    copies[1].start()
    shape = (SUBLANES, LANES)
    row, lane = row_of(shape), lane_of(shape)
    slot = lane // SUBLANES
    first = row < GROUPS
    own_slot = slot == row
    rewards = received[...]
    logprob_sums = pltpu.roll(rewards, LANES // 2, 1)
    member = pltpu.roll(rewards, LANES // 4, 1)

    def row_sums(upper, lower):
        upper = jnp.sum(upper, axis=0, keepdims=True)
        lower = jnp.sum(lower, axis=0, keepdims=True)
        chosen = jnp.where(
            first, jnp.where(own_slot, upper, 0.0), jnp.where(slot == row - GROUPS, lower, 0.0)
        )
        return jnp.sum(chosen, axis=1, keepdims=True)

    total = jnp.sum(rewards, axis=0, keepdims=True)
    sums = jnp.sum(jnp.where(own_slot, total, 0.0), axis=1, keepdims=True)
    group_mean = sums / GROUP
    mean_row = jnp.sum(jnp.where(own_slot & first, group_mean, 0.0), axis=0, keepdims=True)
    centred = rewards - member * mean_row
    spreads = row_sums(centred * centred, centred * logprob_sums)
    group_spread = jnp.maximum(jnp.sqrt(spreads / GROUP), spread_floor)
    info_reward, info_group = token_info[1], token_info[2]
    mean, spread, tokens = group_mean[0:1], group_spread[0:1], sums[GROUPS : GROUPS + 1]
    terms = spreads[GROUPS : GROUPS + 1] * (GROUP * WIN / tokens) / spread
    for g in range(1, GROUPS):
        chosen = info_group == float(g)
        one_tokens = sums[GROUPS + g : GROUPS + g + 1]
        one_spread = group_spread[g : g + 1]
        terms += spreads[GROUPS + g : GROUPS + g + 1] * (GROUP * WIN / one_tokens) / one_spread
        mean = jnp.where(chosen, group_mean[g : g + 1], mean)
        spread = jnp.where(chosen, one_spread, spread)
        tokens = jnp.where(chosen, one_tokens, tokens)
    total_rows = GROUPS * GROUP * WIN
    objective_row[...] = -terms / total_rows
    copies[4].start()
    info_advantage = (info_reward - mean) / spread
    weight = token_info[0] * (info_advantage * (GROUP * WIN / tokens))
    advantage_row[...] = info_advantage[chunks : chunks + 1, :SUBLANES]
    copies[3].start()
    weight_rows[...] = weight[:chunks]
    copies[2].start()
    for copy in copies:
        copy.wait()


def shards(rewards, group_ids, lengths, token_mask, targets, logits):
    rows = logits.shape[0]
    chunks = rows // LANES
    f32, i32 = jnp.float32, jnp.int32
    any_spec = pl.BlockSpec(memory_space=pl.ANY)
    vmem = pl.BlockSpec(memory_space=pltpu.VMEM)

    def kept(*shape):
        return pltpu.VMEM(shape, f32)

    def near(array):
        return pltpu.with_memory_space_constraint(array, pltpu.VMEM)

    sent, token_info, own_info = pl.pallas_call(
        local_kernel,
        name="local_stats",
        in_specs=[any_spec] * 6,
        out_specs=[vmem] * 3,
        out_shape=[
            kept(2 ** len(FIRST), 3, chunks, LANES),
            kept(3, SUBLANES, LANES),
            kept(2, SUBLANES, LANES),
        ],
        scratch_shapes=[
            pltpu.VMEM(logits.shape, logits.dtype),
            pltpu.VMEM((chunks, LANES), i32),
            pltpu.VMEM((chunks, LANES), i32),
            pltpu.SMEM(rewards.shape, i32),
            pltpu.SMEM(rewards.shape, i32),
            pltpu.SMEM(rewards.shape, i32),
            pltpu.VMEM((rows, LANES), f32),
            pltpu.VMEM((rows, LANES), f32),
            pltpu.SemaphoreType.DMA((6,)),
        ],
    )(
        rewards,
        group_ids,
        lengths,
        token_mask.reshape(chunks, LANES),
        targets.reshape(chunks, LANES),
        logits,
    )
    received = lax.all_to_all(sent, FIRST, 0, 0, tiled=True)
    sent = pl.pallas_call(
        merge_kernel,
        name="merge_stats",
        in_specs=[vmem],
        out_specs=vmem,
        out_shape=kept(2 ** len(Y_AXES), 3, chunks, LANES),
    )(near(received))
    received = lax.all_to_all(
        sent, X_AXES + MP, 0, 0, axis_index_groups=y_groups(), tiled=True
    )
    shard_count = 2 ** len(X_AXES)
    sent, token_values = pl.pallas_call(
        token_kernel,
        name="token_values",
        in_specs=[vmem] * 3,
        out_specs=[vmem] * 2,
        out_shape=[kept(SUBLANES, LANES), kept(2 * chunks, LANES)],
    )(near(received), near(token_info), near(own_info))
    received = lax.all_to_all(
        sent.reshape(shard_count, 1, LANES),
        X_AXES + MP,
        0,
        0,
        axis_index_groups=x_groups(),
        tiled=True,
    )
    advantage, token_weight, token_logprob, token_entropy, objective = pl.pallas_call(
        final_kernel,
        name="group_values",
        in_specs=[vmem] * 3,
        out_specs=[any_spec] * 5,
        out_shape=[
            jax.ShapeDtypeStruct((1, SUBLANES), f32),
            jax.ShapeDtypeStruct((chunks, LANES), f32),
            jax.ShapeDtypeStruct((chunks, LANES), f32),
            jax.ShapeDtypeStruct((chunks, LANES), f32),
            jax.ShapeDtypeStruct((1, 1), f32),
        ],
        scratch_shapes=[
            pltpu.VMEM((1, SUBLANES), f32),
            pltpu.VMEM((chunks, LANES), f32),
            pltpu.VMEM((1, 1), f32),
            pltpu.SemaphoreType.DMA((5,)),
        ],
    )(near(received.reshape(shard_count, LANES)), near(token_info), near(token_values))
    return (
        advantage.reshape(-1),
        token_weight.reshape(-1),
        token_logprob.reshape(-1),
        token_entropy.reshape(-1),
        objective.reshape(()),
    )


def solution(mesh):
    names = X_AXES + MP
    split = Mesh(mesh.devices.reshape((2,) * len(names)), names)
    rows = P(X_AXES)
    in_specs = (rows, rows, rows, rows, rows, P(X_AXES, MP))
    out_specs = (rows, rows, rows, rows, P())
    return jax.shard_map(
        shards, mesh=split, in_specs=in_specs, out_specs=out_specs, check_vma=False
    )
```

```python
import jax
import jax.numpy as jnp
from jax import lax
from jax.experimental import pallas as pl
from jax.experimental.pallas import tpu as pltpu
from jax.sharding import Mesh
from jax.sharding import PartitionSpec as P

GROUP = 16
WIN = 64
LANES = 128
SUBLANES = 8
GROUPS = 4
STEP = 16
X_AXES = ("x2", "x1", "x0")
Z_AXES = ("z2", "z1", "z0")
Y_AXES = ("y2", "y1", "y0")
MP = Z_AXES + Y_AXES + ("core",)
FIRST = ("core",) + Z_AXES

spread_floor = 0.25
reward_unit = 1024.0


def position(x, z, y, core):
    return ((x * 8 + z) * 8 + y) * 2 + core


def y_groups():
    return [
        [position(x, z, y, core if y < 4 or z == 0 else 1 - core) for y in range(8)]
        for x in range(8)
        for z in range(8)
        for core in range(2)
    ]


def x_groups():
    groups = {}
    for z in range(8):
        for y in range(8):
            swapped = (4, 5, 6, 7) if z else (4,) if y else ()
            for core in range(2):
                groups[z, y, core] = [
                    position(x, z, y, 1 - core if x in swapped else core) for x in range(8)
                ]
    here, there = groups[0, 0, 0], groups[1, 0, 0]
    for x in (3, 4, 5):
        here[x], there[x] = there[x], here[x]
    return list(groups.values())


def lane_of(shape):
    return lax.broadcasted_iota(jnp.int32, shape, 1)


def row_of(shape):
    return lax.broadcasted_iota(jnp.int32, shape, 0)


def lines_to_lanes(pick, block):
    return lax.dot_general(
        pick, block, (((1,), (1,)), ((), ())), preferred_element_type=jnp.float32
    )


def local_kernel(
    rewards, group_ids, lengths, token_mask, targets, logits,
    send, token_info, own_info,
    tiles, target_rows, mask_rows, reward_of, group_of, length_of, peak_rows, columns, sems,
):
    chunks = logits.shape[0] // LANES
    width = logits.shape[1]
    targets_copy = pltpu.make_async_copy(targets, target_rows, sems.at[0])
    small = [
        pltpu.make_async_copy(token_mask, mask_rows, sems.at[1]),
        pltpu.make_async_copy(rewards, reward_of, sems.at[2]),
        pltpu.make_async_copy(group_ids, group_of, sems.at[3]),
        pltpu.make_async_copy(lengths, length_of, sems.at[4]),
    ]
    logits_copy = pltpu.make_async_copy(logits, tiles, sems.at[5])
    targets_copy.start()
    for copy in small:
        copy.start()
    logits_copy.start()
    shard = 0
    for name in MP:
        shard = shard * 2 + lax.axis_index(name)
    targets_copy.wait()

    block = (LANES, LANES)
    diagonal = row_of(block) == lane_of(block)
    digit_row = row_of((2 * LANES, LANES))
    digits = jnp.where(digit_row < LANES, 1.0, float(LANES)).astype(jnp.bfloat16)
    local = target_rows[...] - shard * width
    inside = (local >= 0) & (local < width)
    low_digit = jnp.where(inside, local % LANES, -1).astype(jnp.float32)
    high_digit = jnp.where(inside, local // LANES, 0).astype(jnp.float32)
    for c in range(chunks):
        spread = jnp.concatenate(
            [
                jnp.where(diagonal, low_digit[c : c + 1], 0.0),
                jnp.where(diagonal, high_digit[c : c + 1], 0.0),
            ],
            axis=1,
        ).astype(jnp.bfloat16)
        columns[LANES * c : LANES * (c + 1), :] = jnp.dot(
            spread, digits, preferred_element_type=jnp.float32
        )

    for copy in small:
        copy.wait()
    shape = (SUBLANES, LANES)
    row, lane = row_of(shape), lane_of(shape)
    reward_info = jnp.zeros(shape, jnp.float32)
    group_info = jnp.zeros(shape, jnp.float32)
    length_info = jnp.zeros(shape, jnp.int32)
    own_reward = jnp.zeros(shape, jnp.float32)
    own_group = jnp.zeros(shape, jnp.int32)
    for i in range(2 * chunks):
        here = ((row == i // 2) & (lane // WIN == i % 2)) | ((row == chunks) & (lane == i))
        reward = reward_of[i].astype(jnp.float32) / reward_unit
        reward_info = jnp.where(here, reward, reward_info)
        group_info = jnp.where(here, group_of[i].astype(jnp.float32), group_info)
        length_info = jnp.where(here, length_of[i], length_info)
        own_reward = jnp.where(lane % SUBLANES == i, reward, own_reward)
        own_group = jnp.where(lane % SUBLANES == i, group_of[i], own_group)
    mask8 = jnp.concatenate([mask_rows[...], mask_rows[...]], axis=0)
    live = jnp.where((row < chunks) & (mask8 > 0) & (lane % WIN < length_info), 1.0, 0.0)
    token_info[0] = live
    token_info[1] = reward_info
    token_info[2] = group_info
    slot = lane // SUBLANES
    field = slot // GROUPS
    values = jnp.where(
        field == 0, own_reward, jnp.where(field == 1, rollout_sums(live), 1.0)
    )
    mine = own_group == slot % GROUPS
    own_info[0] = jnp.where(mine & (field != 2), values, 0.0)
    own_info[1] = jnp.where(mine & (field == 2), 1.0, 0.0)

    segments = width // LANES
    step_shape = (STEP, LANES)
    lane_value = lane_of(step_shape).astype(jnp.float32)
    lane_values = [lane_value + float(LANES * k) for k in range(segments)]
    pick_shape = (4 * chunks, 6 * LANES)
    pick_row, pick_lane = row_of(pick_shape), lane_of(pick_shape)
    pick_slot = pick_lane // LANES
    pick_kind = jnp.where(pick_slot < 2, pick_slot, pick_slot // 2 + 1)

    def find_peaks(c):
        for r in range(LANES * c, LANES * (c + 1), STEP):
            best = tiles[r : r + STEP, :LANES]
            for k in range(1, segments):
                best = jnp.maximum(best, tiles[r : r + STEP, LANES * k : LANES * (k + 1)])
            peak_rows[r : r + STEP, :] = jnp.broadcast_to(
                jnp.max(best.astype(jnp.float32), axis=1, keepdims=True), step_shape
            )

    def add_sums(c):
        lines = []
        for r in range(LANES * c, LANES * (c + 1), STEP):
            peak = peak_rows[r : r + STEP, :]
            column = columns[r : r + STEP, :]
            total = moment = picked = 0.0
            for k in range(segments):
                segment = tiles[r : r + STEP, LANES * k : LANES * (k + 1)].astype(jnp.float32)
                shifted = segment - peak
                weight = jnp.exp(shifted)
                product = weight * shifted
                total = weight if k == 0 else total + weight
                moment = product if k == 0 else moment + product
                picked = jnp.where(column == lane_values[k], segment, picked)
            total_high = total.astype(jnp.bfloat16)
            moment_high = moment.astype(jnp.bfloat16)
            lines.append(
                jnp.concatenate(
                    [
                        peak.astype(jnp.bfloat16),
                        picked.astype(jnp.bfloat16),
                        total_high,
                        (total - total_high.astype(jnp.float32)).astype(jnp.bfloat16),
                        moment_high,
                        (moment - moment_high.astype(jnp.float32)).astype(jnp.bfloat16),
                    ],
                    axis=1,
                )
            )
        pick = (pick_row == chunks * pick_kind + c) & ((pick_slot > 0) | (pick_lane == 0))
        return lines_to_lanes(
            jnp.where(pick, 1.0, 0.0).astype(jnp.bfloat16), jnp.concatenate(lines, axis=0)
        )

    logits_copy.wait()
    find_peaks(0)
    gathered = jnp.zeros((4 * chunks, LANES), jnp.float32)
    for c in range(chunks):
        if c + 1 < chunks:
            find_peaks(c + 1)
        gathered += add_sums(c)
    total = gathered[2 * chunks : 3 * chunks]
    log_total = jnp.log(total)
    log_sum = gathered[:chunks] + log_total
    entropy = log_total - gathered[3 * chunks :] / total
    picked = gathered[chunks : 2 * chunks]
    for n in range(send.shape[0]):
        send[n, 0] = log_sum
        send[n, 1] = entropy
        send[n, 2] = picked


def rollout_sums(values):
    shape = values.shape
    row, lane = row_of(shape), lane_of(shape)
    even = jnp.sum(jnp.where(lane < WIN, values, 0.0), axis=1, keepdims=True)
    odd = jnp.sum(jnp.where(lane >= WIN, values, 0.0), axis=1, keepdims=True)
    spread = jnp.where(
        row == lane % SUBLANES // 2, jnp.where(lane % 2 == 0, even, odd), 0.0
    )
    return jnp.broadcast_to(jnp.sum(spread, axis=0, keepdims=True), shape)


def merged(received):
    count = received.shape[0]
    joint = received[0, 0]
    picked = received[0, 2]
    for n in range(1, count):
        joint = jnp.maximum(joint, received[n, 0])
        picked += received[n, 2]
    total = jnp.zeros_like(joint)
    mixed = jnp.zeros_like(joint)
    for n in range(count):
        shift = received[n, 0] - joint
        factor = jnp.exp(shift)
        total += factor
        mixed += factor * (received[n, 1] - shift)
    log_total = jnp.log(total)
    return joint + log_total, mixed / total + log_total, picked


def merge_kernel(received, send):
    log_sum, entropy, picked = merged(received)
    for n in range(send.shape[0]):
        send[n, 0] = log_sum
        send[n, 1] = entropy
        send[n, 2] = picked


def token_kernel(received, token_info, own_info, send, token_values):
    log_sum, entropy, picked = merged(received)
    chunks = log_sum.shape[0]
    live = token_info[0][:chunks]
    logprob = live * (picked - log_sum)
    token_values[:chunks] = logprob
    token_values[chunks:] = live * entropy
    padded = jnp.concatenate([logprob, jnp.zeros_like(logprob)], axis=0)
    send[...] = own_info[0] + own_info[1] * rollout_sums(padded)


def final_kernel(
    received, token_info, token_values,
    advantage, token_weight, token_logprob, token_entropy, objective,
    advantage_row, weight_rows, objective_row, sems,
):
    chunks = token_weight.shape[0]
    copies = [
        pltpu.make_async_copy(token_values.at[pl.ds(0, chunks)], token_logprob, sems.at[0]),
        pltpu.make_async_copy(token_values.at[pl.ds(chunks, chunks)], token_entropy, sems.at[1]),
        pltpu.make_async_copy(weight_rows, token_weight, sems.at[2]),
        pltpu.make_async_copy(advantage_row, advantage, sems.at[3]),
        pltpu.make_async_copy(objective_row, objective, sems.at[4]),
    ]
    copies[0].start()
    copies[1].start()
    shape = (SUBLANES, LANES)
    row, lane = row_of(shape), lane_of(shape)
    slot = lane // SUBLANES
    first = row < GROUPS
    own_slot = slot == row
    rewards = received[...]
    logprob_sums = pltpu.roll(rewards, LANES // 2, 1)
    member = pltpu.roll(rewards, LANES // 4, 1)

    def row_sums(upper, lower):
        upper = jnp.sum(upper, axis=0, keepdims=True)
        lower = jnp.sum(lower, axis=0, keepdims=True)
        chosen = jnp.where(
            first, jnp.where(own_slot, upper, 0.0), jnp.where(slot == row - GROUPS, lower, 0.0)
        )
        return jnp.sum(chosen, axis=1, keepdims=True)

    total = jnp.sum(rewards, axis=0, keepdims=True)
    sums = jnp.sum(jnp.where(own_slot, total, 0.0), axis=1, keepdims=True)
    group_mean = sums / GROUP
    mean_row = jnp.sum(jnp.where(own_slot & first, group_mean, 0.0), axis=0, keepdims=True)
    centred = rewards - member * mean_row
    spreads = row_sums(centred * centred, centred * logprob_sums)
    group_spread = jnp.maximum(jnp.sqrt(spreads / GROUP), spread_floor)
    info_reward, info_group = token_info[1], token_info[2]
    mean, spread, tokens = group_mean[0:1], group_spread[0:1], sums[GROUPS : GROUPS + 1]
    terms = spreads[GROUPS : GROUPS + 1] * (GROUP * WIN / tokens) / spread
    for g in range(1, GROUPS):
        chosen = info_group == float(g)
        one_tokens = sums[GROUPS + g : GROUPS + g + 1]
        one_spread = group_spread[g : g + 1]
        terms += spreads[GROUPS + g : GROUPS + g + 1] * (GROUP * WIN / one_tokens) / one_spread
        mean = jnp.where(chosen, group_mean[g : g + 1], mean)
        spread = jnp.where(chosen, one_spread, spread)
        tokens = jnp.where(chosen, one_tokens, tokens)
    total_rows = GROUPS * GROUP * WIN
    objective_row[...] = -terms / total_rows
    copies[4].start()
    info_advantage = (info_reward - mean) / spread
    weight = token_info[0] * (info_advantage * (GROUP * WIN / tokens))
    advantage_row[...] = info_advantage[chunks : chunks + 1, :SUBLANES]
    copies[3].start()
    weight_rows[...] = weight[:chunks]
    copies[2].start()
    for copy in copies:
        copy.wait()


def shards(rewards, group_ids, lengths, token_mask, targets, logits):
    rows = logits.shape[0]
    chunks = rows // LANES
    f32, i32 = jnp.float32, jnp.int32
    any_spec = pl.BlockSpec(memory_space=pl.ANY)
    vmem = pl.BlockSpec(memory_space=pltpu.VMEM)

    def kept(*shape):
        return pltpu.VMEM(shape, f32)

    def near(array):
        return pltpu.with_memory_space_constraint(array, pltpu.VMEM)

    sent, token_info, own_info = pl.pallas_call(
        local_kernel,
        name="local_stats",
        in_specs=[any_spec] * 6,
        out_specs=[vmem] * 3,
        out_shape=[
            kept(2 ** len(FIRST), 3, chunks, LANES),
            kept(3, SUBLANES, LANES),
            kept(2, SUBLANES, LANES),
        ],
        scratch_shapes=[
            pltpu.VMEM(logits.shape, logits.dtype),
            pltpu.VMEM((chunks, LANES), i32),
            pltpu.VMEM((chunks, LANES), i32),
            pltpu.SMEM(rewards.shape, i32),
            pltpu.SMEM(rewards.shape, i32),
            pltpu.SMEM(rewards.shape, i32),
            pltpu.VMEM((rows, LANES), f32),
            pltpu.VMEM((rows, LANES), f32),
            pltpu.SemaphoreType.DMA((6,)),
        ],
    )(
        rewards,
        group_ids,
        lengths,
        token_mask.reshape(chunks, LANES),
        targets.reshape(chunks, LANES),
        logits,
    )
    received = lax.all_to_all(sent, FIRST, 0, 0, tiled=True)
    sent = pl.pallas_call(
        merge_kernel,
        name="merge_stats",
        in_specs=[vmem],
        out_specs=vmem,
        out_shape=kept(2 ** len(Y_AXES), 3, chunks, LANES),
    )(near(received))
    received = lax.all_to_all(
        sent, X_AXES + MP, 0, 0, axis_index_groups=y_groups(), tiled=True
    )
    shard_count = 2 ** len(X_AXES)
    sent, token_values = pl.pallas_call(
        token_kernel,
        name="token_values",
        in_specs=[vmem] * 3,
        out_specs=[vmem] * 2,
        out_shape=[kept(SUBLANES, LANES), kept(2 * chunks, LANES)],
    )(near(received), near(token_info), near(own_info))
    received = lax.all_to_all(
        sent.reshape(shard_count, 1, LANES),
        X_AXES + MP,
        0,
        0,
        axis_index_groups=x_groups(),
        tiled=True,
    )
    advantage, token_weight, token_logprob, token_entropy, objective = pl.pallas_call(
        final_kernel,
        name="group_values",
        in_specs=[vmem] * 3,
        out_specs=[any_spec] * 5,
        out_shape=[
            jax.ShapeDtypeStruct((1, SUBLANES), f32),
            jax.ShapeDtypeStruct((chunks, LANES), f32),
            jax.ShapeDtypeStruct((chunks, LANES), f32),
            jax.ShapeDtypeStruct((chunks, LANES), f32),
            jax.ShapeDtypeStruct((1, 1), f32),
        ],
        scratch_shapes=[
            pltpu.VMEM((1, SUBLANES), f32),
            pltpu.VMEM((chunks, LANES), f32),
            pltpu.VMEM((1, 1), f32),
            pltpu.SemaphoreType.DMA((5,)),
        ],
    )(near(received.reshape(shard_count, LANES)), near(token_info), near(token_values))
    return (
        advantage.reshape(-1),
        token_weight.reshape(-1),
        token_logprob.reshape(-1),
        token_entropy.reshape(-1),
        objective.reshape(()),
    )


def solution(mesh):
    names = X_AXES + MP
    split = Mesh(mesh.devices.reshape((2,) * len(names)), names)
    rows = P(X_AXES)
    in_specs = (rows, rows, rows, rows, rows, P(X_AXES, MP))
    out_specs = (rows, rows, rows, rows, P())
    return jax.shard_map(
        shards, mesh=split, in_specs=in_specs, out_specs=out_specs, check_vma=False
    )
```

```python
import jax
import jax.numpy as jnp
from jax import lax
from jax.experimental import pallas as pl
from jax.experimental.pallas import tpu as pltpu
from jax.sharding import Mesh
from jax.sharding import PartitionSpec as P

GROUP = 16
WIN = 64
LANES = 128
SUBLANES = 8
GROUPS = 4
STEP = 16
X_AXES = ("x2", "x1", "x0")
Z_AXES = ("z2", "z1", "z0")
Y_AXES = ("y2", "y1", "y0")
MP = Z_AXES + Y_AXES + ("core",)
FIRST = ("core",) + Z_AXES

spread_floor = 0.25
reward_unit = 1024.0


def position(x, z, y, core):
    return ((x * 8 + z) * 8 + y) * 2 + core


def y_groups():
    return [
        [position(x, z, y, 1 - core if y in ((4, 5, 6, 7) if z else (4,)) else core) for y in range(8)]
        for x in range(8)
        for z in range(8)
        for core in range(2)
    ]


def x_groups():
    groups = []
    for z in range(8):
        for y in range(8):
            swapped = () if y == z == 0 else (4, 5, 6, 7)
            for core in range(2):
                groups.append(
                    [position(x, z, y, 1 - core if x in swapped else core) for x in range(8)]
                )
    return groups


def lane_of(shape):
    return lax.broadcasted_iota(jnp.int32, shape, 1)


def row_of(shape):
    return lax.broadcasted_iota(jnp.int32, shape, 0)


def lines_to_lanes(pick, block):
    return lax.dot_general(
        pick, block, (((1,), (1,)), ((), ())), preferred_element_type=jnp.float32
    )


def local_kernel(
    rewards, group_ids, lengths, token_mask, targets, logits,
    send, token_info, own_info,
    tiles, target_rows, mask_rows, reward_of, group_of, length_of, peak_rows, columns, sems,
):
    chunks = logits.shape[0] // LANES
    width = logits.shape[1]
    targets_copy = pltpu.make_async_copy(targets, target_rows, sems.at[0])
    small = [
        pltpu.make_async_copy(token_mask, mask_rows, sems.at[1]),
        pltpu.make_async_copy(rewards, reward_of, sems.at[2]),
        pltpu.make_async_copy(group_ids, group_of, sems.at[3]),
        pltpu.make_async_copy(lengths, length_of, sems.at[4]),
    ]
    logits_copy = pltpu.make_async_copy(logits, tiles, sems.at[5])
    targets_copy.start()
    for copy in small:
        copy.start()
    logits_copy.start()
    shard = 0
    for name in MP:
        shard = shard * 2 + lax.axis_index(name)
    targets_copy.wait()

    block = (LANES, LANES)
    diagonal = row_of(block) == lane_of(block)
    digit_row = row_of((2 * LANES, LANES))
    digits = jnp.where(digit_row < LANES, 1.0, float(LANES)).astype(jnp.bfloat16)
    local = target_rows[...] - shard * width
    inside = (local >= 0) & (local < width)
    low_digit = jnp.where(inside, local % LANES, -1).astype(jnp.float32)
    high_digit = jnp.where(inside, local // LANES, 0).astype(jnp.float32)
    for c in range(chunks):
        spread = jnp.concatenate(
            [
                jnp.where(diagonal, low_digit[c : c + 1], 0.0),
                jnp.where(diagonal, high_digit[c : c + 1], 0.0),
            ],
            axis=1,
        ).astype(jnp.bfloat16)
        columns[LANES * c : LANES * (c + 1), :] = jnp.dot(
            spread, digits, preferred_element_type=jnp.float32
        )

    for copy in small:
        copy.wait()
    shape = (SUBLANES, LANES)
    row, lane = row_of(shape), lane_of(shape)
    reward_info = jnp.zeros(shape, jnp.float32)
    group_info = jnp.zeros(shape, jnp.float32)
    length_info = jnp.zeros(shape, jnp.int32)
    own_reward = jnp.zeros(shape, jnp.float32)
    own_group = jnp.zeros(shape, jnp.int32)
    for i in range(2 * chunks):
        here = ((row == i // 2) & (lane // WIN == i % 2)) | ((row == chunks) & (lane == i))
        reward = reward_of[i].astype(jnp.float32) / reward_unit
        reward_info = jnp.where(here, reward, reward_info)
        group_info = jnp.where(here, group_of[i].astype(jnp.float32), group_info)
        length_info = jnp.where(here, length_of[i], length_info)
        own_reward = jnp.where(lane % SUBLANES == i, reward, own_reward)
        own_group = jnp.where(lane % SUBLANES == i, group_of[i], own_group)
    mask8 = jnp.concatenate([mask_rows[...], mask_rows[...]], axis=0)
    live = jnp.where((row < chunks) & (mask8 > 0) & (lane % WIN < length_info), 1.0, 0.0)
    token_info[0] = live
    token_info[1] = reward_info
    token_info[2] = group_info
    slot = lane // SUBLANES
    field = slot // GROUPS
    values = jnp.where(
        field == 0, own_reward, jnp.where(field == 1, rollout_sums(live), 1.0)
    )
    mine = own_group == slot % GROUPS
    own_info[0] = jnp.where(mine & (field != 2), values, 0.0)
    own_info[1] = jnp.where(mine & (field == 2), 1.0, 0.0)

    segments = width // LANES
    step_shape = (STEP, LANES)
    lane_value = lane_of(step_shape).astype(jnp.float32)
    lane_values = [lane_value + float(LANES * k) for k in range(segments)]
    pick_shape = (4 * chunks, 6 * LANES)
    pick_row, pick_lane = row_of(pick_shape), lane_of(pick_shape)
    pick_slot = pick_lane // LANES
    pick_kind = jnp.where(pick_slot < 2, pick_slot, pick_slot // 2 + 1)

    def find_peaks(c):
        for r in range(LANES * c, LANES * (c + 1), STEP):
            best = tiles[r : r + STEP, :LANES]
            for k in range(1, segments):
                best = jnp.maximum(best, tiles[r : r + STEP, LANES * k : LANES * (k + 1)])
            peak_rows[r : r + STEP, :] = jnp.broadcast_to(
                jnp.max(best.astype(jnp.float32), axis=1, keepdims=True), step_shape
            )

    def add_sums(c):
        lines = []
        for r in range(LANES * c, LANES * (c + 1), STEP):
            peak = peak_rows[r : r + STEP, :]
            column = columns[r : r + STEP, :]
            total = moment = picked = 0.0
            for k in range(segments):
                segment = tiles[r : r + STEP, LANES * k : LANES * (k + 1)].astype(jnp.float32)
                shifted = segment - peak
                weight = jnp.exp(shifted)
                product = weight * shifted
                total = weight if k == 0 else total + weight
                moment = product if k == 0 else moment + product
                picked = jnp.where(column == lane_values[k], segment, picked)
            total_high = total.astype(jnp.bfloat16)
            moment_high = moment.astype(jnp.bfloat16)
            lines.append(
                jnp.concatenate(
                    [
                        peak.astype(jnp.bfloat16),
                        picked.astype(jnp.bfloat16),
                        total_high,
                        (total - total_high.astype(jnp.float32)).astype(jnp.bfloat16),
                        moment_high,
                        (moment - moment_high.astype(jnp.float32)).astype(jnp.bfloat16),
                    ],
                    axis=1,
                )
            )
        pick = (pick_row == chunks * pick_kind + c) & ((pick_slot > 0) | (pick_lane == 0))
        return lines_to_lanes(
            jnp.where(pick, 1.0, 0.0).astype(jnp.bfloat16), jnp.concatenate(lines, axis=0)
        )

    logits_copy.wait()
    find_peaks(0)
    gathered = jnp.zeros((4 * chunks, LANES), jnp.float32)
    for c in range(chunks):
        if c + 1 < chunks:
            find_peaks(c + 1)
        gathered += add_sums(c)
    total = gathered[2 * chunks : 3 * chunks]
    log_total = jnp.log(total)
    log_sum = gathered[:chunks] + log_total
    entropy = log_total - gathered[3 * chunks :] / total
    picked = gathered[chunks : 2 * chunks]
    for n in range(send.shape[0]):
        send[n, 0] = log_sum
        send[n, 1] = entropy
        send[n, 2] = picked


def rollout_sums(values):
    shape = values.shape
    row, lane = row_of(shape), lane_of(shape)
    even = jnp.sum(jnp.where(lane < WIN, values, 0.0), axis=1, keepdims=True)
    odd = jnp.sum(jnp.where(lane >= WIN, values, 0.0), axis=1, keepdims=True)
    spread = jnp.where(
        row == lane % SUBLANES // 2, jnp.where(lane % 2 == 0, even, odd), 0.0
    )
    return jnp.broadcast_to(jnp.sum(spread, axis=0, keepdims=True), shape)


def merged(received):
    count = received.shape[0]
    joint = received[0, 0]
    picked = received[0, 2]
    for n in range(1, count):
        joint = jnp.maximum(joint, received[n, 0])
        picked += received[n, 2]
    total = jnp.zeros_like(joint)
    mixed = jnp.zeros_like(joint)
    for n in range(count):
        shift = received[n, 0] - joint
        factor = jnp.exp(shift)
        total += factor
        mixed += factor * (received[n, 1] - shift)
    log_total = jnp.log(total)
    return joint + log_total, mixed / total + log_total, picked


def merge_kernel(received, send):
    log_sum, entropy, picked = merged(received)
    for n in range(send.shape[0]):
        send[n, 0] = log_sum
        send[n, 1] = entropy
        send[n, 2] = picked


def token_kernel(received, token_info, own_info, send, token_values):
    log_sum, entropy, picked = merged(received)
    chunks = log_sum.shape[0]
    live = token_info[0][:chunks]
    logprob = live * (picked - log_sum)
    token_values[:chunks] = logprob
    token_values[chunks:] = live * entropy
    padded = jnp.concatenate([logprob, jnp.zeros_like(logprob)], axis=0)
    send[...] = own_info[0] + own_info[1] * rollout_sums(padded)


def final_kernel(
    received, token_info, token_values,
    advantage, token_weight, token_logprob, token_entropy, objective,
    advantage_row, weight_rows, objective_row, sems,
):
    chunks = token_weight.shape[0]
    copies = [
        pltpu.make_async_copy(token_values.at[pl.ds(0, chunks)], token_logprob, sems.at[0]),
        pltpu.make_async_copy(token_values.at[pl.ds(chunks, chunks)], token_entropy, sems.at[1]),
        pltpu.make_async_copy(weight_rows, token_weight, sems.at[2]),
        pltpu.make_async_copy(advantage_row, advantage, sems.at[3]),
        pltpu.make_async_copy(objective_row, objective, sems.at[4]),
    ]
    copies[0].start()
    copies[1].start()
    shape = (SUBLANES, LANES)
    row, lane = row_of(shape), lane_of(shape)
    slot = lane // SUBLANES
    first = row < GROUPS
    own_slot = slot == row
    rewards = received[...]
    logprob_sums = pltpu.roll(rewards, LANES // 2, 1)
    member = pltpu.roll(rewards, LANES // 4, 1)

    def row_sums(upper, lower):
        upper = jnp.sum(upper, axis=0, keepdims=True)
        lower = jnp.sum(lower, axis=0, keepdims=True)
        chosen = jnp.where(
            first, jnp.where(own_slot, upper, 0.0), jnp.where(slot == row - GROUPS, lower, 0.0)
        )
        return jnp.sum(chosen, axis=1, keepdims=True)

    total = jnp.sum(rewards, axis=0, keepdims=True)
    sums = jnp.sum(jnp.where(own_slot, total, 0.0), axis=1, keepdims=True)
    group_mean = sums / GROUP
    mean_row = jnp.sum(jnp.where(own_slot & first, group_mean, 0.0), axis=0, keepdims=True)
    centred = rewards - member * mean_row
    spreads = row_sums(centred * centred, centred * logprob_sums)
    group_spread = jnp.maximum(jnp.sqrt(spreads / GROUP), spread_floor)
    info_reward, info_group = token_info[1], token_info[2]
    mean, spread, tokens = group_mean[0:1], group_spread[0:1], sums[GROUPS : GROUPS + 1]
    terms = spreads[GROUPS : GROUPS + 1] * (GROUP * WIN / tokens) / spread
    for g in range(1, GROUPS):
        chosen = info_group == float(g)
        one_tokens = sums[GROUPS + g : GROUPS + g + 1]
        one_spread = group_spread[g : g + 1]
        terms += spreads[GROUPS + g : GROUPS + g + 1] * (GROUP * WIN / one_tokens) / one_spread
        mean = jnp.where(chosen, group_mean[g : g + 1], mean)
        spread = jnp.where(chosen, one_spread, spread)
        tokens = jnp.where(chosen, one_tokens, tokens)
    total_rows = GROUPS * GROUP * WIN
    objective_row[...] = -terms / total_rows
    copies[4].start()
    info_advantage = (info_reward - mean) / spread
    weight = token_info[0] * (info_advantage * (GROUP * WIN / tokens))
    advantage_row[...] = info_advantage[chunks : chunks + 1, :SUBLANES]
    copies[3].start()
    weight_rows[...] = weight[:chunks]
    copies[2].start()
    for copy in copies:
        copy.wait()


def shards(rewards, group_ids, lengths, token_mask, targets, logits):
    rows = logits.shape[0]
    chunks = rows // LANES
    f32, i32 = jnp.float32, jnp.int32
    any_spec = pl.BlockSpec(memory_space=pl.ANY)
    vmem = pl.BlockSpec(memory_space=pltpu.VMEM)

    def kept(*shape):
        return pltpu.VMEM(shape, f32)

    def near(array):
        return pltpu.with_memory_space_constraint(array, pltpu.VMEM)

    sent, token_info, own_info = pl.pallas_call(
        local_kernel,
        name="local_stats",
        in_specs=[any_spec] * 6,
        out_specs=[vmem] * 3,
        out_shape=[
            kept(2 ** len(FIRST), 3, chunks, LANES),
            kept(3, SUBLANES, LANES),
            kept(2, SUBLANES, LANES),
        ],
        scratch_shapes=[
            pltpu.VMEM(logits.shape, logits.dtype),
            pltpu.VMEM((chunks, LANES), i32),
            pltpu.VMEM((chunks, LANES), i32),
            pltpu.SMEM(rewards.shape, i32),
            pltpu.SMEM(rewards.shape, i32),
            pltpu.SMEM(rewards.shape, i32),
            pltpu.VMEM((rows, LANES), f32),
            pltpu.VMEM((rows, LANES), f32),
            pltpu.SemaphoreType.DMA((6,)),
        ],
    )(
        rewards,
        group_ids,
        lengths,
        token_mask.reshape(chunks, LANES),
        targets.reshape(chunks, LANES),
        logits,
    )
    received = lax.all_to_all(sent, FIRST, 0, 0, tiled=True)
    sent = pl.pallas_call(
        merge_kernel,
        name="merge_stats",
        in_specs=[vmem],
        out_specs=vmem,
        out_shape=kept(2 ** len(Y_AXES), 3, chunks, LANES),
    )(near(received))
    received = lax.all_to_all(
        sent, X_AXES + MP, 0, 0, axis_index_groups=y_groups(), tiled=True
    )
    shard_count = 2 ** len(X_AXES)
    sent, token_values = pl.pallas_call(
        token_kernel,
        name="token_values",
        in_specs=[vmem] * 3,
        out_specs=[vmem] * 2,
        out_shape=[kept(SUBLANES, LANES), kept(2 * chunks, LANES)],
    )(near(received), near(token_info), near(own_info))
    received = lax.all_to_all(
        sent.reshape(shard_count, 1, LANES),
        X_AXES + MP,
        0,
        0,
        axis_index_groups=x_groups(),
        tiled=True,
    )
    advantage, token_weight, token_logprob, token_entropy, objective = pl.pallas_call(
        final_kernel,
        name="group_values",
        in_specs=[vmem] * 3,
        out_specs=[any_spec] * 5,
        out_shape=[
            jax.ShapeDtypeStruct((1, SUBLANES), f32),
            jax.ShapeDtypeStruct((chunks, LANES), f32),
            jax.ShapeDtypeStruct((chunks, LANES), f32),
            jax.ShapeDtypeStruct((chunks, LANES), f32),
            jax.ShapeDtypeStruct((1, 1), f32),
        ],
        scratch_shapes=[
            pltpu.VMEM((1, SUBLANES), f32),
            pltpu.VMEM((chunks, LANES), f32),
            pltpu.VMEM((1, 1), f32),
            pltpu.SemaphoreType.DMA((5,)),
        ],
    )(near(received.reshape(shard_count, LANES)), near(token_info), near(token_values))
    return (
        advantage.reshape(-1),
        token_weight.reshape(-1),
        token_logprob.reshape(-1),
        token_entropy.reshape(-1),
        objective.reshape(()),
    )


def solution(mesh):
    names = X_AXES + MP
    split = Mesh(mesh.devices.reshape((2,) * len(names)), names)
    rows = P(X_AXES)
    in_specs = (rows, rows, rows, rows, rows, P(X_AXES, MP))
    out_specs = (rows, rows, rows, rows, P())
    return jax.shard_map(
        shards, mesh=split, in_specs=in_specs, out_specs=out_specs, check_vma=False
    )
```

```python
import jax
import jax.numpy as jnp
from jax import lax
from jax.experimental import pallas as pl
from jax.experimental.pallas import tpu as pltpu
from jax.sharding import Mesh
from jax.sharding import PartitionSpec as P

GROUP = 16
WIN = 64
LANES = 128
SUBLANES = 8
GROUPS = 4
STEP = 16
X_AXES = ("x2", "x1", "x0")
Z_AXES = ("z2", "z1", "z0")
Y_AXES = ("y2", "y1", "y0")
MP = Z_AXES + Y_AXES + ("core",)
FIRST = Z_AXES + ("core",)
SECOND = Y_AXES
THIRD = X_AXES

spread_floor = 0.25
reward_unit = 1024.0


def lane_of(shape):
    return lax.broadcasted_iota(jnp.int32, shape, 1)


def row_of(shape):
    return lax.broadcasted_iota(jnp.int32, shape, 0)


def lines_to_lanes(pick, block):
    return lax.dot_general(
        pick, block, (((1,), (1,)), ((), ())), preferred_element_type=jnp.float32
    )


def local_kernel(
    rewards, group_ids, lengths, token_mask, targets, logits,
    send, token_info, own_info,
    tiles, target_rows, mask_rows, reward_of, group_of, length_of, peak_rows, columns, sems,
):
    chunks = logits.shape[0] // LANES
    width = logits.shape[1]
    targets_copy = pltpu.make_async_copy(targets, target_rows, sems.at[0])
    small = [
        pltpu.make_async_copy(token_mask, mask_rows, sems.at[1]),
        pltpu.make_async_copy(rewards, reward_of, sems.at[2]),
        pltpu.make_async_copy(group_ids, group_of, sems.at[3]),
        pltpu.make_async_copy(lengths, length_of, sems.at[4]),
    ]
    logits_copy = pltpu.make_async_copy(logits, tiles, sems.at[5])
    targets_copy.start()
    for copy in small:
        copy.start()
    logits_copy.start()
    shard = 0
    for name in MP:
        shard = shard * 2 + lax.axis_index(name)
    targets_copy.wait()

    block = (LANES, LANES)
    diagonal = row_of(block) == lane_of(block)
    digit_row = row_of((2 * LANES, LANES))
    digits = jnp.where(digit_row < LANES, 1.0, float(LANES)).astype(jnp.bfloat16)
    local = target_rows[...] - shard * width
    inside = (local >= 0) & (local < width)
    low_digit = jnp.where(inside, local % LANES, -1).astype(jnp.float32)
    high_digit = jnp.where(inside, local // LANES, 0).astype(jnp.float32)
    for c in range(chunks):
        spread = jnp.concatenate(
            [
                jnp.where(diagonal, low_digit[c : c + 1], 0.0),
                jnp.where(diagonal, high_digit[c : c + 1], 0.0),
            ],
            axis=1,
        ).astype(jnp.bfloat16)
        columns[LANES * c : LANES * (c + 1), :] = jnp.dot(
            spread, digits, preferred_element_type=jnp.float32
        )

    for copy in small:
        copy.wait()
    shape = (SUBLANES, LANES)
    row, lane = row_of(shape), lane_of(shape)
    reward_info = jnp.zeros(shape, jnp.float32)
    group_info = jnp.zeros(shape, jnp.float32)
    length_info = jnp.zeros(shape, jnp.int32)
    own_reward = jnp.zeros(shape, jnp.float32)
    own_group = jnp.zeros(shape, jnp.int32)
    for i in range(2 * chunks):
        here = ((row == i // 2) & (lane // WIN == i % 2)) | ((row == chunks) & (lane == i))
        reward = reward_of[i].astype(jnp.float32) / reward_unit
        reward_info = jnp.where(here, reward, reward_info)
        group_info = jnp.where(here, group_of[i].astype(jnp.float32), group_info)
        length_info = jnp.where(here, length_of[i], length_info)
        own_reward = jnp.where(lane % SUBLANES == i, reward, own_reward)
        own_group = jnp.where(lane % SUBLANES == i, group_of[i], own_group)
    mask8 = jnp.concatenate([mask_rows[...], mask_rows[...]], axis=0)
    live = jnp.where((row < chunks) & (mask8 > 0) & (lane % WIN < length_info), 1.0, 0.0)
    token_info[0] = live
    token_info[1] = reward_info
    token_info[2] = group_info
    slot = lane // SUBLANES
    field = slot // GROUPS
    values = jnp.where(
        field == 0, own_reward, jnp.where(field == 1, rollout_sums(live), 1.0)
    )
    mine = own_group == slot % GROUPS
    own_info[0] = jnp.where(mine & (field != 2), values, 0.0)
    own_info[1] = jnp.where(mine & (field == 2), 1.0, 0.0)

    segments = width // LANES
    step_shape = (STEP, LANES)
    lane_value = lane_of(step_shape).astype(jnp.float32)
    lane_values = [lane_value + float(LANES * k) for k in range(segments)]
    pick_shape = (4 * chunks, 6 * LANES)
    pick_row, pick_lane = row_of(pick_shape), lane_of(pick_shape)
    pick_slot = pick_lane // LANES
    pick_kind = jnp.where(pick_slot < 2, pick_slot, pick_slot // 2 + 1)

    def find_peaks(c):
        for r in range(LANES * c, LANES * (c + 1), STEP):
            best = tiles[r : r + STEP, :LANES]
            for k in range(1, segments):
                best = jnp.maximum(best, tiles[r : r + STEP, LANES * k : LANES * (k + 1)])
            peak_rows[r : r + STEP, :] = jnp.broadcast_to(
                jnp.max(best.astype(jnp.float32), axis=1, keepdims=True), step_shape
            )

    def add_sums(c):
        lines = []
        for r in range(LANES * c, LANES * (c + 1), STEP):
            peak = peak_rows[r : r + STEP, :]
            column = columns[r : r + STEP, :]
            total = moment = picked = 0.0
            for k in range(segments):
                segment = tiles[r : r + STEP, LANES * k : LANES * (k + 1)].astype(jnp.float32)
                shifted = segment - peak
                weight = jnp.exp(shifted)
                product = weight * shifted
                total = weight if k == 0 else total + weight
                moment = product if k == 0 else moment + product
                picked = jnp.where(column == lane_values[k], segment, picked)
            total_high = total.astype(jnp.bfloat16)
            moment_high = moment.astype(jnp.bfloat16)
            lines.append(
                jnp.concatenate(
                    [
                        peak.astype(jnp.bfloat16),
                        picked.astype(jnp.bfloat16),
                        total_high,
                        (total - total_high.astype(jnp.float32)).astype(jnp.bfloat16),
                        moment_high,
                        (moment - moment_high.astype(jnp.float32)).astype(jnp.bfloat16),
                    ],
                    axis=1,
                )
            )
        pick = (pick_row == chunks * pick_kind + c) & ((pick_slot > 0) | (pick_lane == 0))
        return lines_to_lanes(
            jnp.where(pick, 1.0, 0.0).astype(jnp.bfloat16), jnp.concatenate(lines, axis=0)
        )

    logits_copy.wait()
    find_peaks(0)
    gathered = jnp.zeros((4 * chunks, LANES), jnp.float32)
    for c in range(chunks):
        if c + 1 < chunks:
            find_peaks(c + 1)
        gathered += add_sums(c)
    total = gathered[2 * chunks : 3 * chunks]
    log_total = jnp.log(total)
    log_sum = gathered[:chunks] + log_total
    entropy = log_total - gathered[3 * chunks :] / total
    picked = gathered[chunks : 2 * chunks]
    for n in range(send.shape[0]):
        send[n, 0] = log_sum
        send[n, 1] = entropy
        send[n, 2] = picked


def rollout_sums(values):
    shape = values.shape
    row, lane = row_of(shape), lane_of(shape)
    even = jnp.sum(jnp.where(lane < WIN, values, 0.0), axis=1, keepdims=True)
    odd = jnp.sum(jnp.where(lane >= WIN, values, 0.0), axis=1, keepdims=True)
    spread = jnp.where(
        row == lane % SUBLANES // 2, jnp.where(lane % 2 == 0, even, odd), 0.0
    )
    return jnp.broadcast_to(jnp.sum(spread, axis=0, keepdims=True), shape)


def merged(received):
    count = received.shape[0]
    joint = received[0, 0]
    picked = received[0, 2]
    for n in range(1, count):
        joint = jnp.maximum(joint, received[n, 0])
        picked += received[n, 2]
    total = jnp.zeros_like(joint)
    mixed = jnp.zeros_like(joint)
    for n in range(count):
        shift = received[n, 0] - joint
        factor = jnp.exp(shift)
        total += factor
        mixed += factor * (received[n, 1] - shift)
    log_total = jnp.log(total)
    return joint + log_total, mixed / total + log_total, picked


def merge_kernel(received, send):
    log_sum, entropy, picked = merged(received)
    for n in range(send.shape[0]):
        send[n, 0] = log_sum
        send[n, 1] = entropy
        send[n, 2] = picked


def token_kernel(received, token_info, own_info, send, token_values):
    log_sum, entropy, picked = merged(received)
    chunks = log_sum.shape[0]
    live = token_info[0][:chunks]
    logprob = live * (picked - log_sum)
    token_values[:chunks] = logprob
    token_values[chunks:] = live * entropy
    padded = jnp.concatenate([logprob, jnp.zeros_like(logprob)], axis=0)
    send[...] = own_info[0] + own_info[1] * rollout_sums(padded)


def final_kernel(
    received, token_info, token_values,
    advantage, token_weight, token_logprob, token_entropy, objective,
    advantage_row, weight_rows, objective_row, sems,
):
    chunks = token_weight.shape[0]
    copies = [
        pltpu.make_async_copy(token_values.at[pl.ds(0, chunks)], token_logprob, sems.at[0]),
        pltpu.make_async_copy(token_values.at[pl.ds(chunks, chunks)], token_entropy, sems.at[1]),
        pltpu.make_async_copy(weight_rows, token_weight, sems.at[2]),
        pltpu.make_async_copy(advantage_row, advantage, sems.at[3]),
        pltpu.make_async_copy(objective_row, objective, sems.at[4]),
    ]
    copies[0].start()
    copies[1].start()
    shape = (SUBLANES, LANES)
    row, lane = row_of(shape), lane_of(shape)
    slot = lane // SUBLANES
    first = row < GROUPS
    own_slot = slot == row
    rewards = received[...]
    logprob_sums = pltpu.roll(rewards, LANES // 2, 1)
    member = pltpu.roll(rewards, LANES // 4, 1)

    def row_sums(upper, lower):
        upper = jnp.sum(upper, axis=0, keepdims=True)
        lower = jnp.sum(lower, axis=0, keepdims=True)
        chosen = jnp.where(
            first, jnp.where(own_slot, upper, 0.0), jnp.where(slot == row - GROUPS, lower, 0.0)
        )
        return jnp.sum(chosen, axis=1, keepdims=True)

    total = jnp.sum(rewards, axis=0, keepdims=True)
    sums = jnp.sum(jnp.where(own_slot, total, 0.0), axis=1, keepdims=True)
    group_mean = sums / GROUP
    mean_row = jnp.sum(jnp.where(own_slot & first, group_mean, 0.0), axis=0, keepdims=True)
    centred = rewards - member * mean_row
    spreads = row_sums(centred * centred, centred * logprob_sums)
    group_spread = jnp.maximum(jnp.sqrt(spreads / GROUP), spread_floor)
    info_reward, info_group = token_info[1], token_info[2]
    mean, spread, tokens = group_mean[0:1], group_spread[0:1], sums[GROUPS : GROUPS + 1]
    terms = spreads[GROUPS : GROUPS + 1] * (GROUP * WIN / tokens) / spread
    for g in range(1, GROUPS):
        chosen = info_group == float(g)
        one_tokens = sums[GROUPS + g : GROUPS + g + 1]
        one_spread = group_spread[g : g + 1]
        terms += spreads[GROUPS + g : GROUPS + g + 1] * (GROUP * WIN / one_tokens) / one_spread
        mean = jnp.where(chosen, group_mean[g : g + 1], mean)
        spread = jnp.where(chosen, one_spread, spread)
        tokens = jnp.where(chosen, one_tokens, tokens)
    total_rows = GROUPS * GROUP * WIN
    objective_row[...] = -terms / total_rows
    copies[4].start()
    info_advantage = (info_reward - mean) / spread
    weight = token_info[0] * (info_advantage * (GROUP * WIN / tokens))
    advantage_row[...] = info_advantage[chunks : chunks + 1, :SUBLANES]
    copies[3].start()
    weight_rows[...] = weight[:chunks]
    copies[2].start()
    for copy in copies:
        copy.wait()


def shards(rewards, group_ids, lengths, token_mask, targets, logits):
    rows = logits.shape[0]
    chunks = rows // LANES
    f32, i32 = jnp.float32, jnp.int32
    any_spec = pl.BlockSpec(memory_space=pl.ANY)
    vmem = pl.BlockSpec(memory_space=pltpu.VMEM)

    def kept(*shape):
        return pltpu.VMEM(shape, f32)

    def near(array):
        return pltpu.with_memory_space_constraint(array, pltpu.VMEM)

    sent, token_info, own_info = pl.pallas_call(
        local_kernel,
        name="local_stats",
        in_specs=[any_spec] * 6,
        out_specs=[vmem] * 3,
        out_shape=[
            kept(2 ** len(FIRST), 3, chunks, LANES),
            kept(3, SUBLANES, LANES),
            kept(2, SUBLANES, LANES),
        ],
        scratch_shapes=[
            pltpu.VMEM(logits.shape, logits.dtype),
            pltpu.VMEM((chunks, LANES), i32),
            pltpu.VMEM((chunks, LANES), i32),
            pltpu.SMEM(rewards.shape, i32),
            pltpu.SMEM(rewards.shape, i32),
            pltpu.SMEM(rewards.shape, i32),
            pltpu.VMEM((rows, LANES), f32),
            pltpu.VMEM((rows, LANES), f32),
            pltpu.SemaphoreType.DMA((6,)),
        ],
    )(
        rewards,
        group_ids,
        lengths,
        token_mask.reshape(chunks, LANES),
        targets.reshape(chunks, LANES),
        logits,
    )
    received = lax.all_to_all(sent, FIRST, 0, 0, tiled=True)
    sent = pl.pallas_call(
        merge_kernel,
        name="merge_stats",
        in_specs=[vmem],
        out_specs=vmem,
        out_shape=kept(2 ** len(SECOND), 3, chunks, LANES),
    )(near(received))
    received = lax.all_to_all(sent, SECOND, 0, 0, tiled=True)
    shard_count = 2 ** len(THIRD)
    sent, token_values = pl.pallas_call(
        token_kernel,
        name="token_values",
        in_specs=[vmem] * 3,
        out_specs=[vmem] * 2,
        out_shape=[kept(SUBLANES, LANES), kept(2 * chunks, LANES)],
    )(near(received), near(token_info), near(own_info))
    received = lax.all_to_all(sent.reshape(shard_count, 1, LANES), THIRD, 0, 0, tiled=True)
    advantage, token_weight, token_logprob, token_entropy, objective = pl.pallas_call(
        final_kernel,
        name="group_values",
        in_specs=[vmem] * 3,
        out_specs=[any_spec] * 5,
        out_shape=[
            jax.ShapeDtypeStruct((1, SUBLANES), f32),
            jax.ShapeDtypeStruct((chunks, LANES), f32),
            jax.ShapeDtypeStruct((chunks, LANES), f32),
            jax.ShapeDtypeStruct((chunks, LANES), f32),
            jax.ShapeDtypeStruct((1, 1), f32),
        ],
        scratch_shapes=[
            pltpu.VMEM((1, SUBLANES), f32),
            pltpu.VMEM((chunks, LANES), f32),
            pltpu.VMEM((1, 1), f32),
            pltpu.SemaphoreType.DMA((5,)),
        ],
    )(near(received.reshape(shard_count, LANES)), near(token_info), near(token_values))
    return (
        advantage.reshape(-1),
        token_weight.reshape(-1),
        token_logprob.reshape(-1),
        token_entropy.reshape(-1),
        objective.reshape(()),
    )


def solution(mesh):
    names = X_AXES + MP
    split = Mesh(mesh.devices.reshape((2,) * len(names)), names)
    rows = P(X_AXES)
    in_specs = (rows, rows, rows, rows, rows, P(X_AXES, MP))
    out_specs = (rows, rows, rows, rows, P())
    return jax.shard_map(
        shards, mesh=split, in_specs=in_specs, out_specs=out_specs, check_vma=False
    )
```

```python
import jax
import jax.numpy as jnp
from jax import lax
from jax.experimental import pallas as pl
from jax.experimental.pallas import tpu as pltpu
from jax.sharding import Mesh
from jax.sharding import PartitionSpec as P

GROUP = 16
WIN = 64
LANES = 128
SUBLANES = 8
GROUPS = 4
STEP = 16
X_AXES = ("x2", "x1", "x0")
Z_AXES = ("z2", "z1", "z0")
Y_AXES = ("y2", "y1", "y0")
MP = Z_AXES + Y_AXES + ("core",)
FIRST = Z_AXES + ("core",)
SECOND = Y_AXES
THIRD = X_AXES

spread_floor = 0.25
reward_unit = 1024.0


def lane_of(shape):
    return lax.broadcasted_iota(jnp.int32, shape, 1)


def row_of(shape):
    return lax.broadcasted_iota(jnp.int32, shape, 0)


def lines_to_lanes(pick, block):
    return lax.dot_general(
        pick, block, (((1,), (1,)), ((), ())), preferred_element_type=jnp.float32
    )


def local_kernel(
    rewards, group_ids, lengths, token_mask, targets, logits,
    send, token_info, own_info,
    tiles, target_rows, mask_rows, reward_of, group_of, length_of, peak_rows, columns, sems,
):
    chunks = logits.shape[0] // LANES
    width = logits.shape[1]
    targets_copy = pltpu.make_async_copy(targets, target_rows, sems.at[0])
    small = [
        pltpu.make_async_copy(token_mask, mask_rows, sems.at[1]),
        pltpu.make_async_copy(rewards, reward_of, sems.at[2]),
        pltpu.make_async_copy(group_ids, group_of, sems.at[3]),
        pltpu.make_async_copy(lengths, length_of, sems.at[4]),
    ]
    logits_copy = pltpu.make_async_copy(logits, tiles, sems.at[5])
    targets_copy.start()
    for copy in small:
        copy.start()
    logits_copy.start()
    shard = 0
    for name in MP:
        shard = shard * 2 + lax.axis_index(name)
    targets_copy.wait()

    block = (LANES, LANES)
    diagonal = row_of(block) == lane_of(block)
    digit_row = row_of((2 * LANES, LANES))
    digits = jnp.where(digit_row < LANES, 1.0, float(LANES)).astype(jnp.bfloat16)
    local = target_rows[...] - shard * width
    inside = (local >= 0) & (local < width)
    low_digit = jnp.where(inside, local % LANES, -1).astype(jnp.float32)
    high_digit = jnp.where(inside, local // LANES, 0).astype(jnp.float32)
    for c in range(chunks):
        spread = jnp.concatenate(
            [
                jnp.where(diagonal, low_digit[c : c + 1], 0.0),
                jnp.where(diagonal, high_digit[c : c + 1], 0.0),
            ],
            axis=1,
        ).astype(jnp.bfloat16)
        columns[LANES * c : LANES * (c + 1), :] = jnp.dot(
            spread, digits, preferred_element_type=jnp.float32
        )

    for copy in small:
        copy.wait()
    shape = (SUBLANES, LANES)
    row, lane = row_of(shape), lane_of(shape)
    reward_info = jnp.zeros(shape, jnp.float32)
    group_info = jnp.zeros(shape, jnp.float32)
    length_info = jnp.zeros(shape, jnp.int32)
    own_reward = jnp.zeros(shape, jnp.float32)
    own_group = jnp.zeros(shape, jnp.int32)
    for i in range(2 * chunks):
        here = ((row == i // 2) & (lane // WIN == i % 2)) | ((row == chunks) & (lane == i))
        reward = reward_of[i].astype(jnp.float32) / reward_unit
        reward_info = jnp.where(here, reward, reward_info)
        group_info = jnp.where(here, group_of[i].astype(jnp.float32), group_info)
        length_info = jnp.where(here, length_of[i], length_info)
        own_reward = jnp.where(lane % SUBLANES == i, reward, own_reward)
        own_group = jnp.where(lane % SUBLANES == i, group_of[i], own_group)
    mask8 = jnp.concatenate([mask_rows[...], mask_rows[...]], axis=0)
    live = jnp.where((row < chunks) & (mask8 > 0) & (lane % WIN < length_info), 1.0, 0.0)
    token_info[0] = live
    token_info[1] = reward_info
    token_info[2] = group_info
    slot = lane // SUBLANES
    field = slot // GROUPS
    values = jnp.where(
        field == 0, own_reward, jnp.where(field == 1, rollout_sums(live), 1.0)
    )
    mine = own_group == slot % GROUPS
    own_info[0] = jnp.where(mine & (field != 2), values, 0.0)
    own_info[1] = jnp.where(mine & (field == 2), 1.0, 0.0)

    segments = width // LANES
    step_shape = (STEP, LANES)
    lane_value = lane_of(step_shape).astype(jnp.float32)
    lane_values = [lane_value + float(LANES * k) for k in range(segments)]
    pick_shape = (4 * chunks, 6 * LANES)
    pick_row, pick_lane = row_of(pick_shape), lane_of(pick_shape)
    pick_slot = pick_lane // LANES
    pick_kind = jnp.where(pick_slot < 2, pick_slot, pick_slot // 2 + 1)

    def find_peaks(c):
        for r in range(LANES * c, LANES * (c + 1), STEP):
            best = tiles[r : r + STEP, :LANES]
            for k in range(1, segments):
                best = jnp.maximum(best, tiles[r : r + STEP, LANES * k : LANES * (k + 1)])
            peak_rows[r : r + STEP, :] = jnp.broadcast_to(
                jnp.max(best.astype(jnp.float32), axis=1, keepdims=True), step_shape
            )

    def add_sums(c):
        lines = []
        for r in range(LANES * c, LANES * (c + 1), STEP):
            peak = peak_rows[r : r + STEP, :]
            column = columns[r : r + STEP, :]
            total = moment = picked = 0.0
            for k in range(segments):
                segment = tiles[r : r + STEP, LANES * k : LANES * (k + 1)].astype(jnp.float32)
                shifted = segment - peak
                weight = jnp.exp(shifted)
                product = weight * shifted
                total = weight if k == 0 else total + weight
                moment = product if k == 0 else moment + product
                picked = jnp.where(column == lane_values[k], segment, picked)
            total_high = total.astype(jnp.bfloat16)
            moment_high = moment.astype(jnp.bfloat16)
            lines.append(
                jnp.concatenate(
                    [
                        peak.astype(jnp.bfloat16),
                        picked.astype(jnp.bfloat16),
                        total_high,
                        (total - total_high.astype(jnp.float32)).astype(jnp.bfloat16),
                        moment_high,
                        (moment - moment_high.astype(jnp.float32)).astype(jnp.bfloat16),
                    ],
                    axis=1,
                )
            )
        pick = (pick_row == chunks * pick_kind + c) & ((pick_slot > 0) | (pick_lane == 0))
        return lines_to_lanes(
            jnp.where(pick, 1.0, 0.0).astype(jnp.bfloat16), jnp.concatenate(lines, axis=0)
        )

    logits_copy.wait()
    find_peaks(0)
    gathered = jnp.zeros((4 * chunks, LANES), jnp.float32)
    for c in range(chunks):
        if c + 1 < chunks:
            find_peaks(c + 1)
        gathered += add_sums(c)
    total = gathered[2 * chunks : 3 * chunks]
    log_total = jnp.log(total)
    log_sum = gathered[:chunks] + log_total
    entropy = log_total - gathered[3 * chunks :] / total
    picked = gathered[chunks : 2 * chunks]
    for n in range(send.shape[0]):
        send[n, 0] = log_sum
        send[n, 1] = entropy
        send[n, 2] = picked


def rollout_sums(values):
    shape = values.shape
    row, lane = row_of(shape), lane_of(shape)
    even = jnp.sum(jnp.where(lane < WIN, values, 0.0), axis=1, keepdims=True)
    odd = jnp.sum(jnp.where(lane >= WIN, values, 0.0), axis=1, keepdims=True)
    spread = jnp.where(
        row == lane % SUBLANES // 2, jnp.where(lane % 2 == 0, even, odd), 0.0
    )
    return jnp.broadcast_to(jnp.sum(spread, axis=0, keepdims=True), shape)


def merged(received):
    count = received.shape[0]
    joint = received[0, 0]
    picked = received[0, 2]
    for n in range(1, count):
        joint = jnp.maximum(joint, received[n, 0])
        picked += received[n, 2]
    total = jnp.zeros_like(joint)
    mixed = jnp.zeros_like(joint)
    for n in range(count):
        shift = received[n, 0] - joint
        factor = jnp.exp(shift)
        total += factor
        mixed += factor * (received[n, 1] - shift)
    log_total = jnp.log(total)
    return joint + log_total, mixed / total + log_total, picked


def merge_kernel(received, send):
    log_sum, entropy, picked = merged(received)
    for n in range(send.shape[0]):
        send[n, 0] = log_sum
        send[n, 1] = entropy
        send[n, 2] = picked


def token_kernel(received, token_info, own_info, send, token_values):
    log_sum, entropy, picked = merged(received)
    chunks = log_sum.shape[0]
    live = token_info[0][:chunks]
    logprob = live * (picked - log_sum)
    token_values[:chunks] = logprob
    token_values[chunks:] = live * entropy
    padded = jnp.concatenate([logprob, jnp.zeros_like(logprob)], axis=0)
    send[...] = own_info[0] + own_info[1] * rollout_sums(padded)


def final_kernel(
    received, token_info, token_values,
    advantage, token_weight, token_logprob, token_entropy, objective,
    advantage_row, weight_rows, objective_row, sems,
):
    chunks = token_weight.shape[0]
    copies = [
        pltpu.make_async_copy(token_values.at[pl.ds(0, chunks)], token_logprob, sems.at[0]),
        pltpu.make_async_copy(token_values.at[pl.ds(chunks, chunks)], token_entropy, sems.at[1]),
        pltpu.make_async_copy(weight_rows, token_weight, sems.at[2]),
        pltpu.make_async_copy(advantage_row, advantage, sems.at[3]),
        pltpu.make_async_copy(objective_row, objective, sems.at[4]),
    ]
    copies[0].start()
    copies[1].start()
    shape = (SUBLANES, LANES)
    row, lane = row_of(shape), lane_of(shape)
    slot = lane // SUBLANES
    first = row < GROUPS
    own_slot = slot == row
    rewards = received[...]
    logprob_sums = pltpu.roll(rewards, LANES // 2, 1)
    member = pltpu.roll(rewards, LANES // 4, 1)

    def row_sums(upper, lower):
        upper = jnp.sum(upper, axis=0, keepdims=True)
        lower = jnp.sum(lower, axis=0, keepdims=True)
        chosen = jnp.where(
            first, jnp.where(own_slot, upper, 0.0), jnp.where(slot == row - GROUPS, lower, 0.0)
        )
        return jnp.sum(chosen, axis=1, keepdims=True)

    total = jnp.sum(rewards, axis=0, keepdims=True)
    sums = jnp.sum(jnp.where(own_slot, total, 0.0), axis=1, keepdims=True)
    group_mean = sums / GROUP
    mean_row = jnp.sum(jnp.where(own_slot & first, group_mean, 0.0), axis=0, keepdims=True)
    centred = rewards - member * mean_row
    spreads = row_sums(centred * centred, centred * logprob_sums)
    group_spread = jnp.maximum(jnp.sqrt(spreads / GROUP), spread_floor)
    info_reward, info_group = token_info[1], token_info[2]
    mean, spread, tokens = group_mean[0:1], group_spread[0:1], sums[GROUPS : GROUPS + 1]
    terms = spreads[GROUPS : GROUPS + 1] * (GROUP * WIN / tokens) / spread
    for g in range(1, GROUPS):
        chosen = info_group == float(g)
        one_tokens = sums[GROUPS + g : GROUPS + g + 1]
        one_spread = group_spread[g : g + 1]
        terms += spreads[GROUPS + g : GROUPS + g + 1] * (GROUP * WIN / one_tokens) / one_spread
        mean = jnp.where(chosen, group_mean[g : g + 1], mean)
        spread = jnp.where(chosen, one_spread, spread)
        tokens = jnp.where(chosen, one_tokens, tokens)
    info_advantage = (info_reward - mean) / spread
    weight = token_info[0] * (info_advantage * (GROUP * WIN / tokens))
    advantage_row[...] = info_advantage[chunks : chunks + 1, :SUBLANES]
    copies[3].start()
    weight_rows[...] = weight[:chunks]
    copies[2].start()
    total_rows = GROUPS * GROUP * WIN
    objective_row[...] = -terms / total_rows
    copies[4].start()
    for copy in copies:
        copy.wait()


def shards(rewards, group_ids, lengths, token_mask, targets, logits):
    rows = logits.shape[0]
    chunks = rows // LANES
    f32, i32 = jnp.float32, jnp.int32
    any_spec = pl.BlockSpec(memory_space=pl.ANY)
    vmem = pl.BlockSpec(memory_space=pltpu.VMEM)

    def kept(*shape):
        return pltpu.VMEM(shape, f32)

    def near(array):
        return pltpu.with_memory_space_constraint(array, pltpu.VMEM)

    sent, token_info, own_info = pl.pallas_call(
        local_kernel,
        name="local_stats",
        in_specs=[any_spec] * 6,
        out_specs=[vmem] * 3,
        out_shape=[
            kept(2 ** len(FIRST), 3, chunks, LANES),
            kept(3, SUBLANES, LANES),
            kept(2, SUBLANES, LANES),
        ],
        scratch_shapes=[
            pltpu.VMEM(logits.shape, logits.dtype),
            pltpu.VMEM((chunks, LANES), i32),
            pltpu.VMEM((chunks, LANES), i32),
            pltpu.SMEM(rewards.shape, i32),
            pltpu.SMEM(rewards.shape, i32),
            pltpu.SMEM(rewards.shape, i32),
            pltpu.VMEM((rows, LANES), f32),
            pltpu.VMEM((rows, LANES), f32),
            pltpu.SemaphoreType.DMA((6,)),
        ],
    )(
        rewards,
        group_ids,
        lengths,
        token_mask.reshape(chunks, LANES),
        targets.reshape(chunks, LANES),
        logits,
    )
    received = lax.all_to_all(sent, FIRST, 0, 0, tiled=True)
    sent = pl.pallas_call(
        merge_kernel,
        name="merge_stats",
        in_specs=[vmem],
        out_specs=vmem,
        out_shape=kept(2 ** len(SECOND), 3, chunks, LANES),
    )(near(received))
    received = lax.all_to_all(sent, SECOND, 0, 0, tiled=True)
    shard_count = 2 ** len(THIRD)
    sent, token_values = pl.pallas_call(
        token_kernel,
        name="token_values",
        in_specs=[vmem] * 3,
        out_specs=[vmem] * 2,
        out_shape=[kept(SUBLANES, LANES), kept(2 * chunks, LANES)],
    )(near(received), near(token_info), near(own_info))
    received = lax.all_to_all(sent.reshape(shard_count, 1, LANES), THIRD, 0, 0, tiled=True)
    advantage, token_weight, token_logprob, token_entropy, objective = pl.pallas_call(
        final_kernel,
        name="group_values",
        in_specs=[vmem] * 3,
        out_specs=[any_spec] * 5,
        out_shape=[
            jax.ShapeDtypeStruct((1, SUBLANES), f32),
            jax.ShapeDtypeStruct((chunks, LANES), f32),
            jax.ShapeDtypeStruct((chunks, LANES), f32),
            jax.ShapeDtypeStruct((chunks, LANES), f32),
            jax.ShapeDtypeStruct((1, 1), f32),
        ],
        scratch_shapes=[
            pltpu.VMEM((1, SUBLANES), f32),
            pltpu.VMEM((chunks, LANES), f32),
            pltpu.VMEM((1, 1), f32),
            pltpu.SemaphoreType.DMA((5,)),
        ],
    )(near(received.reshape(shard_count, LANES)), near(token_info), near(token_values))
    return (
        advantage.reshape(-1),
        token_weight.reshape(-1),
        token_logprob.reshape(-1),
        token_entropy.reshape(-1),
        objective.reshape(()),
    )


def solution(mesh):
    names = X_AXES + MP
    split = Mesh(mesh.devices.reshape((2,) * len(names)), names)
    rows = P(X_AXES)
    in_specs = (rows, rows, rows, rows, rows, P(X_AXES, MP))
    out_specs = (rows, rows, rows, rows, P())
    return jax.shard_map(
        shards, mesh=split, in_specs=in_specs, out_specs=out_specs, check_vma=False
    )
```
